16 devices in a mesh: dpy: 2 (over z), dpx: 2 (over y), tp: 4 (over x, core).
Axes of the slice: x: 2, y: 2, z: 2, core: 2. Of those that a mesh axis runs over, the one named last changes fastest.
Arguments:
- x_saved: bfloat16 [2, 64, 512, 768], P(None, ('dpy', 'dpx'))
- y_saved: bfloat16 [2, 64, 512, 768], P(None, ('dpy', 'dpx'))
- dz_top: bfloat16 [64, 512, 768], P(('dpy', 'dpx'))
- w_qkv: bfloat16 [2, 768, 3, 12, 64], P(None, None, None, 'tp')
- w_out: bfloat16 [2, 12, 64, 768], P(None, 'tp')
- w_up: bfloat16 [2, 768, 3072], P(None, None, 'tp')
- w_down: bfloat16 [2, 3072, 768], P(None, 'tp')
Outputs:
- output 1: bfloat16 [64, 512, 768], P(('dpy', 'dpx'))
- output 2: float32 [2, 768, 3, 12, 64], P(None, ('dpy', 'dpx'), None, 'tp')
- output 3: float32 [2, 12, 64, 768], P(None, 'tp', None, ('dpy', 'dpx'))
- output 4: float32 [2, 768, 3072], P(None, ('dpy', 'dpx'), 'tp')
- output 5: float32 [2, 3072, 768], P(None, ('tp', 'dpy', 'dpx'))
All inputs are finite; a program needn't handle non-finite values.
Results may differ from the reference program's by a relative error of at most 0.0179834.
Values are sent between devices in bfloat16 or wider.
A program may use at most 1 GiB of HBM per device.

```python
import jax
import jax.numpy as jnp
from jax import lax

D = 768
FF = 3072
HEADS = 12
HEAD = 64
SEQ = 512
BATCH = 64
REPLICAS = 4
LAYERS = 2


def setup_inputs(seed: int = 0) -> dict:
    rng_keys = jax.random.split(jax.random.key(seed), 8)
    attn_gain = SEQ ** 0.25
    act_shape = (LAYERS, BATCH, SEQ, D)
    x_saved = jax.random.normal(rng_keys[0], act_shape, jnp.float32)
    y_saved = jax.random.normal(rng_keys[1], act_shape, jnp.float32)
    dz_top = jax.random.normal(rng_keys[2], (BATCH, SEQ, D), jnp.float32)
    qk_weight = jax.random.normal(rng_keys[3], (LAYERS, D, 2, HEADS, HEAD), jnp.float32) * D ** -0.5
    v_weight = jax.random.normal(rng_keys[4], (LAYERS, D, 1, HEADS, HEAD), jnp.float32) * (attn_gain * D ** -0.5)
    w_qkv = jnp.concatenate([qk_weight, v_weight], axis=2)
    w_out = jax.random.normal(rng_keys[5], (LAYERS, HEADS, HEAD, D), jnp.float32) * (attn_gain * D ** -0.5)
    w_up = jax.random.normal(rng_keys[6], (LAYERS, D, FF), jnp.float32) * D ** -0.5
    w_down = jax.random.normal(rng_keys[7], (LAYERS, FF, D), jnp.float32) * FF ** -0.5
    return {'x_saved': x_saved.astype(jnp.bfloat16), 'y_saved': y_saved.astype(jnp.bfloat16), 'dz_top': dz_top.astype(jnp.bfloat16), 'w_qkv': w_qkv.astype(jnp.bfloat16), 'w_out': w_out.astype(jnp.bfloat16), 'w_up': w_up.astype(jnp.bfloat16), 'w_down': w_down.astype(jnp.bfloat16)}


def layer_backward(x_seq, y_seq, d_out, w_qkv, w_out, w_up, w_down):
    h_pre = jnp.dot(y_seq, w_up, preferred_element_type=jnp.float32)
    gelu_out, gelu_pull = jax.vjp(jax.nn.gelu, h_pre)
    gelu_bf = gelu_out.astype(jnp.bfloat16)
    g_down = jnp.dot(gelu_bf.T, d_out, preferred_element_type=jnp.float32)
    d_gelu = jnp.dot(d_out, w_down.T, preferred_element_type=jnp.float32)
    d_pre = gelu_pull(d_gelu)[0].astype(jnp.bfloat16)
    g_up = jnp.dot(y_seq.T, d_pre, preferred_element_type=jnp.float32)
    d_mid = (d_out.astype(jnp.float32) + jnp.dot(d_pre, w_up.T, preferred_element_type=jnp.float32)).astype(jnp.bfloat16)
    qkv_flat = w_qkv.reshape(D, 3 * D)
    qkv_act = jnp.dot(x_seq, qkv_flat, preferred_element_type=jnp.float32).astype(jnp.bfloat16).reshape(SEQ, 3, HEADS, HEAD)
    q_heads = qkv_act[:, 0].astype(jnp.float32)
    k_heads = qkv_act[:, 1].astype(jnp.float32)
    v_heads = qkv_act[:, 2].astype(jnp.float32)
    attn_scale = HEAD ** -0.5
    scores = jnp.einsum('qhe,khe->hqk', q_heads, k_heads) * attn_scale
    attn_prob = jax.nn.softmax(scores, axis=-1)
    prob_bf = attn_prob.astype(jnp.bfloat16).astype(jnp.float32)
    context = jnp.einsum('hqk,khe->qhe', prob_bf, v_heads).astype(jnp.bfloat16).reshape(SEQ, D)
    out_flat = w_out.reshape(D, D)
    g_out = jnp.dot(context.T, d_mid, preferred_element_type=jnp.float32).reshape(HEADS, HEAD, D)
    d_ctx = jnp.dot(d_mid, out_flat.T, preferred_element_type=jnp.float32).astype(jnp.bfloat16).reshape(SEQ, HEADS, HEAD).astype(jnp.float32)
    d_prob = jnp.einsum('qhe,khe->hqk', d_ctx, v_heads)
    d_val = jnp.einsum('hqk,qhe->khe', prob_bf, d_ctx).astype(jnp.bfloat16)
    row_dot = jnp.sum(d_prob * attn_prob, axis=-1, keepdims=True)
    d_scores = (attn_prob * (d_prob - row_dot) * attn_scale).astype(jnp.bfloat16).astype(jnp.float32)
    d_query = jnp.einsum('hqk,khe->qhe', d_scores, k_heads).astype(jnp.bfloat16)
    d_key = jnp.einsum('hqk,qhe->khe', d_scores, q_heads).astype(jnp.bfloat16)
    d_qkv = jnp.stack([d_query, d_key, d_val], axis=1).reshape(SEQ, 3 * D)
    g_qkv = jnp.dot(x_seq.T, d_qkv, preferred_element_type=jnp.float32).reshape(D, 3, HEADS, HEAD)
    d_input = (d_mid.astype(jnp.float32) + jnp.dot(d_qkv, qkv_flat.T, preferred_element_type=jnp.float32)).astype(jnp.bfloat16)
    return d_input, (g_qkv, g_out, g_up, g_down)


def reference(x_saved, y_saved, dz_top, w_qkv, w_out, w_up, w_down):
    def seq_step(grad_acc, seq_inputs):
        x_seq, y_seq, grad_in = seq_inputs
        layer_grads = [None] * LAYERS
        for layer_idx in reversed(range(LAYERS)):
            grad_in, layer_grads[layer_idx] = layer_backward(x_seq[layer_idx], y_seq[layer_idx], grad_in, w_qkv[layer_idx], w_out[layer_idx], w_up[layer_idx], w_down[layer_idx])
        summed = tuple(grad_acc[slot_idx] + jnp.stack([layer_grad[slot_idx] for layer_grad in layer_grads]) for slot_idx in range(4))
        return summed, grad_in
    zero_acc = (jnp.zeros(w_qkv.shape, jnp.float32), jnp.zeros(w_out.shape, jnp.float32), jnp.zeros(w_up.shape, jnp.float32), jnp.zeros(w_down.shape, jnp.float32))
    totals, d_input = lax.scan(seq_step, zero_acc, (jnp.swapaxes(x_saved, 0, 1), jnp.swapaxes(y_saved, 0, 1), dz_top))
    return (d_input, totals[0] / REPLICAS, totals[1] / REPLICAS, totals[2] / REPLICAS, totals[3] / REPLICAS)
```

```python
import jax
import jax.numpy as jnp
from jax import lax
from jax.sharding import PartitionSpec as P

DATA_AXES = ('dpy', 'dpx')
ALL_AXES = ('dpy', 'dpx', 'tp')
F32 = jnp.float32
BF16 = jnp.bfloat16


def layer_backward(x_in, y_mid, d_out, w_qkv, w_out, w_up, w_down):
    head_dim = w_qkv.shape[-1]
    attn_scale = head_dim ** -0.5
    h_pre = jnp.einsum('bsd,df->bsf', y_mid, w_up, preferred_element_type=F32)
    gelu_out, gelu_pull = jax.vjp(jax.nn.gelu, h_pre)
    gelu_bf = gelu_out.astype(BF16)
    g_down = jnp.einsum('bsf,bsd->fd', gelu_bf, d_out, preferred_element_type=F32)
    d_gelu = jnp.einsum('bsd,fd->bsf', d_out, w_down, preferred_element_type=F32)
    d_pre = gelu_pull(d_gelu)[0].astype(BF16)
    g_up = jnp.einsum('bsd,bsf->df', y_mid, d_pre, preferred_element_type=F32)
    mlp = jnp.einsum('bsf,df->bsd', d_pre, w_up, preferred_element_type=F32)
    d_mid = (d_out.astype(F32) + mlp).astype(BF16)
    qkv_act = jnp.einsum('bsd,dche->bsche', x_in, w_qkv, preferred_element_type=F32).astype(BF16)
    q_heads = qkv_act[:, :, 0]
    k_heads = qkv_act[:, :, 1]
    v_heads = qkv_act[:, :, 2]
    scores = jnp.einsum('bqhe,bkhe->bhqk', q_heads, k_heads, preferred_element_type=F32) * attn_scale
    attn_prob = jax.nn.softmax(scores, axis=-1)
    prob_bf = attn_prob.astype(BF16)
    context = jnp.einsum('bhqk,bkhe->bqhe', prob_bf, v_heads, preferred_element_type=F32).astype(BF16)
    g_out = jnp.einsum('crif,cre->ife', context, d_mid, preferred_element_type=F32)
    d_ctx = jnp.einsum('cre,ife->crif', d_mid, w_out, preferred_element_type=F32).astype(BF16)
    d_prob = jnp.einsum('bqhe,bkhe->bhqk', d_ctx, v_heads, preferred_element_type=F32)
    d_val = jnp.einsum('bhqk,bqhe->bkhe', prob_bf, d_ctx, preferred_element_type=F32).astype(BF16)
    row_dot = jnp.sum(d_prob * attn_prob, axis=-1, keepdims=True)
    d_scores = (attn_prob * (d_prob - row_dot) * attn_scale).astype(BF16)
    d_query = jnp.einsum('bhqk,bkhe->bqhe', d_scores, k_heads, preferred_element_type=F32).astype(BF16)
    d_key = jnp.einsum('bhqk,bqhe->bkhe', d_scores, q_heads, preferred_element_type=F32).astype(BF16)
    d_qkv = jnp.stack([d_query, d_key, d_val], axis=2)
    g_qkv = jnp.einsum('bsd,bsche->dche', x_in, d_qkv, preferred_element_type=F32)
    attn = jnp.einsum('bsche,dche->bsd', d_qkv, w_qkv, preferred_element_type=F32)
    d_input = (d_mid.astype(F32) + attn).astype(BF16)
    return d_input, (g_qkv, g_out, g_up, g_down)


def solution(mesh):
    dp = mesh.shape['dpy'] * mesh.shape['dpx']
    tp = mesh.shape['tp']
    act_spec = P(None, DATA_AXES, None, None)

    def reduce_grads(grads):
        g_qkv, g_out, g_up, g_down = grads
        d = g_up.shape[0]
        f = g_up.shape[1]
        nh, hd = g_out.shape[0], g_out.shape[1]

        def rs(g):
            return lax.psum_scatter(g.reshape((dp * tp,) + g.shape[2:]), ALL_AXES, scatter_dimension=0, tiled=True)[0] / dp
        a = rs(g_qkv.reshape(dp, d // dp, 3, tp, nh // tp, hd).transpose(0, 3, 1, 2, 4, 5).reshape(dp, tp, d // dp, -1))
        a = a.reshape(d // dp, 3, nh // tp, hd)
        b = rs(g_out.reshape(tp, nh // tp * hd, dp, d // dp).transpose(2, 0, 1, 3))
        b = b.reshape(nh // tp, hd, d // dp)
        c = rs(g_up.reshape(dp, d // dp, tp, f // tp).transpose(0, 2, 1, 3))
        e = rs(g_down.reshape(tp, dp, f // tp // dp, d).transpose(1, 0, 2, 3))
        return a, b, c, e

    def device_backward(x_saved, y_saved, dz_top, w_qkv, w_out, w_up, w_down):
        t = lax.axis_index('tp')
        nb = dz_top.shape[0] // tp
        layers = range(x_saved.shape[0])
        w_up, w_down, w_qkv, w_out = [list(w) for w in (w_up, w_down, w_qkv, w_out)]
        for l in reversed(layers):
            w_up[l] = lax.all_gather(w_up[l], 'tp', axis=1, tiled=True)
            w_down[l] = lax.all_gather(w_down[l], 'tp', axis=0, tiled=True)
            w_qkv[l] = lax.all_gather(w_qkv[l], 'tp', axis=2, tiled=True)
            w_out[l] = lax.all_gather(w_out[l], 'tp', axis=0, tiled=True)
        x = lax.dynamic_slice_in_dim(x_saved, t * nb, nb, axis=1)
        y = lax.dynamic_slice_in_dim(y_saved, t * nb, nb, axis=1)
        grad_in = lax.dynamic_slice_in_dim(dz_top, t * nb, nb, axis=0)
        reduced = []
        for l in reversed(layers):
            grad_in, grads = layer_backward(x[l], y[l], grad_in, w_qkv[l], w_out[l], w_up[l], w_down[l])
            reduced.insert(0, reduce_grads(grads))
        stacked = tuple(jnp.stack([g[i] for g in reduced]) for i in range(4))
        grad_in = lax.all_gather(grad_in, 'tp', axis=0, tiled=True)
        return (grad_in,) + stacked

    return jax.shard_map(device_backward, mesh=mesh,
                         in_specs=(act_spec, act_spec, P(DATA_AXES, None, None), P(None, None, None, 'tp', None), P(None, 'tp', None, None), P(None, None, 'tp'), P(None, 'tp', None)),
                         out_specs=(P(DATA_AXES, None, None), P(None, DATA_AXES, None, 'tp', None), P(None, 'tp', None, DATA_AXES), P(None, DATA_AXES, 'tp'), P(None, ('tp', 'dpy', 'dpx'), None)),
                         check_vma=False)
```

```python
import functools
import math

import jax
import jax.numpy as jnp
from jax import lax
from jax.experimental import pallas as pl
from jax.experimental.pallas import tpu as pltpu
from jax.sharding import PartitionSpec as P

DATA_AXES = ('dpy', 'dpx')
ALL_AXES = ('dpy', 'dpx', 'tp')
F32 = jnp.float32
BF16 = jnp.bfloat16
HEAD = 64
NN = (((1,), (0,)), ((), ()))
NT = (((1,), (1,)), ((), ()))
TN = (((0,), (0,)), ((), ()))
VMEM_LIMIT = 60 * 1024 * 1024


def dot(a, b, dims):
    return lax.dot_general(a, b, dims, preferred_element_type=F32)


def mlp_kernel(natural_dz, pos_ref, y_ref, dz_ref, w1_ref, w2_ref, dy_ref, g_ref, yt, dzt, acc, w1t, gt, dht):
    slot = pl.program_id(0)
    seqs, seq = y_ref.shape[-3], y_ref.shape[-2]
    dp, rows = g_ref.shape[0], g_ref.shape[3]

    @pl.when(slot == 0)
    def _():
        acc[...] = jnp.zeros_like(acc)
        for s in range(seqs):
            cols = slice(s * seq, (s + 1) * seq)
            yt[:, cols] = y_ref[0, s].T
            if natural_dz:
                dzt[:, cols] = dz_ref[s].T
    dz = dzt if natural_dz else dz_ref
    w1t[...] = w1_ref[0].T

    def block(i, carry):
        cols = pl.ds(pl.multiple_of(i * seq, seq), seq)
        h = dot(w1t[...], yt[:, cols], NN)
        dg = dot(w2_ref[0], dz[:, cols], NN)
        c0 = math.sqrt(2 / math.pi)
        c1 = 0.044715 * c0
        h2 = h * h
        t = jnp.tanh(h * (c0 + c1 * h2))
        q = 0.5 * t + 0.5
        g = h * q
        dh = dg * (q + (g * (1.0 - t)) * (c0 + (3 * c1) * h2))
        gt[:, cols] = g.astype(BF16)
        dh = dh.astype(BF16)
        dht[:, cols] = dh
        acc[:, cols] += dot(w1_ref[0], dh, NN)
        return carry
    lax.fori_loop(0, seqs, block, 0)
    g_down = dot(gt[...], dz[...], NT)
    for d in range(dp):
        g_ref[d, 0, 0] = g_down[d * rows:(d + 1) * rows]
    g_up = dot(yt[...], dht[...], NT)
    for d in range(dp):
        g_ref[d, 0, 1] = g_up[d * rows:(d + 1) * rows]

    @pl.when(slot == pl.num_programs(0) - 1)
    def _():
        dy_ref[...] = (dz[...].astype(F32) + acc[...]).astype(BF16)


def mlp_backward(pos, layer, y, dz, w1, w2, dp):
    slots, d, f = w1.shape
    natural = dz.ndim == 3
    seq = y.shape[2]
    seqs = y.shape[1] // slots
    tok = seqs * seq
    once = pl.Buffered(1)
    dz_spec = (pl.BlockSpec((seqs, seq, d), lambda j, p: (p[0], 0, 0), pipeline_mode=once) if natural
               else pl.BlockSpec((d, tok), lambda j, p: (0, 0), pipeline_mode=once))
    return pl.pallas_call(
        functools.partial(mlp_kernel, natural),
        out_shape=(jax.ShapeDtypeStruct((d, tok), BF16), jax.ShapeDtypeStruct((dp, slots, 2, d // dp, f), F32)),
        grid_spec=pltpu.PrefetchScalarGridSpec(
            num_scalar_prefetch=1, grid=(slots,),
            in_specs=[pl.BlockSpec((1, seqs, seq, d), lambda j, p: (layer, p[0], 0, 0), pipeline_mode=once), dz_spec,
                      pl.BlockSpec((1, d, f), lambda j, p: (j, 0, 0)), pl.BlockSpec((1, f, d), lambda j, p: (j, 0, 0))],
            out_specs=[pl.BlockSpec((d, tok), lambda j, p: (0, 0), pipeline_mode=once),
                       pl.BlockSpec((dp, 1, 2, d // dp, f), lambda j, p: (0, j, 0, 0, 0))],
            scratch_shapes=[pltpu.VMEM((d, tok), BF16), pltpu.VMEM((d, tok), BF16), pltpu.VMEM((d, tok), F32),
                            pltpu.VMEM((f, d), BF16), pltpu.VMEM((f, tok), BF16), pltpu.VMEM((f, tok), BF16)]),
        compiler_params=pltpu.CompilerParams(vmem_limit_bytes=VMEM_LIMIT, dimension_semantics=('arbitrary',)),
        cost_estimate=pl.CostEstimate(flops=10 * tok * d * f * slots, bytes_accessed=4 * d * f * 3 * slots, transcendentals=tok * f * slots),
        name='mlp_backward',
    )(pos, y, dz, w1, w2)


def attn_kernel(natural_out, pos_ref, x_ref, dy_ref, w_ref, dx_ref, g_ref, xt, acc, gacc, wt, qkv, do, b1, b2):
    slot, s = pl.program_id(0), pl.program_id(1)
    seq, d = x_ref.shape[-2:]
    dp, rows = g_ref.shape[0], g_ref.shape[2]
    nqkv = qkv.shape[0]
    third = nqkv // 3
    cols = pl.ds(pl.multiple_of(s * seq, seq), seq)

    @pl.when(slot == 0)
    def _():
        xt[:, cols] = x_ref[0, 0].T
        acc[:, cols] = jnp.zeros((d, seq), F32)

    @pl.when(s == 0)
    def _():
        wt[...] = w_ref[0].T
        gacc[...] = jnp.zeros_like(gacc)
        b1[pl.ds(nqkv, d - nqkv), :] = jnp.zeros((d - nqkv, seq), BF16)
        b2[pl.ds(0, b2.shape[0] - third), :] = jnp.zeros((b2.shape[0] - third, seq), BF16)
    x_t = xt[:, cols]
    dy_t = dy_ref[:, cols]
    qkv[...] = dot(w_ref[0, pl.ds(0, nqkv), :], x_t, NN).astype(BF16)
    do[...] = dot(w_ref[0, pl.ds(nqkv, d - nqkv), :], dy_t, NN).astype(BF16)
    scale = HEAD ** -0.5
    exp_scale = scale * math.log2(math.e)
    for h in range(third // HEAD):
        r = slice(h * HEAD, (h + 1) * HEAD)
        q_t = qkv[r, :]
        k_t = qkv[slice(third + h * HEAD, third + (h + 1) * HEAD), :]
        v_t = qkv[slice(2 * third + h * HEAD, 2 * third + (h + 1) * HEAD), :]
        do_t = do[r, :]
        do_s = do_t * scale
        k_n = k_t.T
        v_n = v_t.T
        dv = jnp.zeros((HEAD, seq), F32)
        dk = jnp.zeros((HEAD, seq), F32)
        qb = 256
        for c in range(seq // qb):
            qc = slice(c * qb, (c + 1) * qb)
            sc = dot(k_n, q_t[:, qc], NN)
            m = jnp.max(sc, axis=0, keepdims=True)
            e = jnp.exp2((sc - m) * exp_scale)
            p = e * (1.0 / jnp.sum(e, axis=0, keepdims=True))
            p_bf = p.astype(BF16)
            dp_t = dot(v_n, do_s[:, qc], NN)
            rd = jnp.sum(p * dp_t, axis=0, keepdims=True)
            ds = (p * (dp_t - rd)).astype(BF16)
            b2[pl.ds(b2.shape[0] - third + h * HEAD, HEAD), qc] = dot(v_t, p_bf, NN).astype(BF16)
            b1[pl.ds(h * HEAD, HEAD), qc] = dot(k_t, ds, NN).astype(BF16)
            dv += dot(do_t[:, qc], p_bf, NT)
            dk += dot(q_t[:, qc], ds, NT)
        b1[pl.ds(third + h * HEAD, HEAD), :] = dk.astype(BF16)
        b1[pl.ds(2 * third + h * HEAD, HEAD), :] = dv.astype(BF16)
    split = d - b2.shape[0]
    gacc[:, :split] += dot(x_t, b1[pl.ds(0, split), :], NT)
    gacc[:, split:] += dot(x_t, b1[pl.ds(split, d - split), :], NT) + dot(dy_t, b2[...], NT)
    acc[:, cols] += dot(wt[...], b1[...], NN)

    @pl.when(s == pl.num_programs(1) - 1)
    def _():
        for i in range(dp):
            g_ref[i, 0] = gacc[pl.ds(i * rows, rows), :]

    @pl.when(slot == pl.num_programs(0) - 1)
    def _():
        dx = dy_t.astype(F32) + acc[:, cols]
        if natural_out:
            dx_ref[0] = dx.T.astype(BF16)
        else:
            dx_ref[...] = dx.astype(BF16)


def attn_backward(pos, layer, x, dy, w, dp, natural_out):
    slots, nw, d = w.shape
    seq = x.shape[2]
    seqs = x.shape[1] // slots
    tok = seqs * seq
    nqkv = nw * 3 // 4
    last = slots - 1
    if natural_out:
        dx_shape, dx_spec = (seqs, seq, d), pl.BlockSpec((1, seq, d), lambda j, s, p: (jnp.where(j == last, s, 0), 0, 0))
    else:
        dx_shape, dx_spec = (d, tok), pl.BlockSpec((d, seq), lambda j, s, p: (0, jnp.where(j == last, s, 0)))
    return pl.pallas_call(
        functools.partial(attn_kernel, natural_out),
        out_shape=(jax.ShapeDtypeStruct(dx_shape, BF16), jax.ShapeDtypeStruct((dp, slots, d // dp, nw), F32)),
        grid_spec=pltpu.PrefetchScalarGridSpec(
            num_scalar_prefetch=1, grid=(slots, seqs),
            in_specs=[pl.BlockSpec((1, 1, seq, d), lambda j, s, p: (layer, p[0] * seqs + jnp.where(j == 0, s, seqs - 1), 0, 0)),
                      pl.BlockSpec((d, tok), lambda j, s, p: (0, 0), pipeline_mode=pl.Buffered(1)),
                      pl.BlockSpec((1, nw, d), lambda j, s, p: (j, 0, 0))],
            out_specs=[dx_spec, pl.BlockSpec((dp, 1, d // dp, nw), lambda j, s, p: (0, j, 0, 0))],
            scratch_shapes=[pltpu.VMEM((d, tok), BF16), pltpu.VMEM((d, tok), F32), pltpu.VMEM((d, nw), F32),
                            pltpu.VMEM((d, nw), BF16), pltpu.VMEM((nqkv, seq), BF16), pltpu.VMEM((nw - nqkv, seq), BF16),
                            pltpu.VMEM((nw, seq), BF16), pltpu.VMEM((256, seq), BF16)]),
        compiler_params=pltpu.CompilerParams(vmem_limit_bytes=VMEM_LIMIT, dimension_semantics=('arbitrary', 'arbitrary')),
        cost_estimate=pl.CostEstimate(flops=tok * slots * (6 * nw * d + 24 * nqkv // 3 * seq), bytes_accessed=8 * nw * d * slots, transcendentals=tok * seq * 12),
        name='attn_backward',
    )(pos, x, dy, w)


def solution(mesh):
    dp = mesh.shape['dpy'] * mesh.shape['dpx']
    act_spec = P(None, DATA_AXES, None, None)

    def scatter(g):
        n = g.shape[0] * g.shape[1]
        return lax.psum_scatter(g.reshape(n, -1, g.shape[-1]), ALL_AXES, scatter_dimension=0, tiled=True).reshape(g.shape[2:]) / dp

    def device_backward(x_saved, y_saved, dz_top, w_qkv, w_out, w_up, w_down):
        layers, d = w_up.shape[:2]
        f = w_up.shape[2]
        heads, hd = w_out.shape[1:3]
        w_a = jnp.concatenate([w_qkv.transpose(0, 2, 3, 4, 1).reshape(layers, 3 * heads * hd, d), w_out.reshape(layers, heads * hd, d)], axis=1)
        pos = lax.axis_index('tp')[None]
        w1, w2, wa = {}, {}, {}
        for l in reversed(range(layers)):
            both = lax.all_gather(jnp.stack([w_up[l], w_down[l]]), 'tp', axis=0)
            w1[l], w2[l] = both[:, 0], both[:, 1]
            wa[l] = lax.all_gather(w_a[l], 'tp', axis=0)
        grad = dz_top
        outs = {}
        for l in reversed(range(layers)):
            dy, gm = mlp_backward(pos, l, y_saved, grad, w1[l], w2[l], dp)
            outs[l, 'm'] = scatter(gm)
            grad, ga = attn_backward(pos, l, x_saved, dy, wa[l], dp, l == 0)
            outs[l, 'a'] = scatter(ga)
        d_input = lax.all_gather(grad, 'tp', axis=0, tiled=True)
        n = 3 * heads * hd
        g_a = jnp.stack([outs[l, 'a'] for l in range(layers)])
        g_m = jnp.stack([outs[l, 'm'] for l in range(layers)])
        g_qkv = g_a[:, :, :n].reshape(layers, d // dp, 3, heads, hd)
        g_out = g_a[:, :, n:].transpose(0, 2, 1).reshape(layers, heads, hd, d // dp)
        return d_input, g_qkv, g_out, g_m[:, 1], g_m[:, 0]

    return jax.shard_map(device_backward, mesh=mesh,
                         in_specs=(act_spec, act_spec, P(DATA_AXES, None, None), P(None, None, None, 'tp', None), P(None, 'tp', None, None), P(None, None, 'tp'), P(None, 'tp', None)),
                         out_specs=(P(DATA_AXES, None, None), P(None, DATA_AXES, None, 'tp', None), P(None, 'tp', None, DATA_AXES), P(None, DATA_AXES, 'tp'), P(None, ('tp', 'dpy', 'dpx'), None)),
                         check_vma=False)
```

```python
import functools
import math

import jax
import jax.numpy as jnp
from jax import lax
from jax.experimental import pallas as pl
from jax.experimental.pallas import tpu as pltpu
from jax.sharding import PartitionSpec as P

DATA_AXES = ('dpy', 'dpx')
F32 = jnp.float32
BF16 = jnp.bfloat16
HEAD = 64
SLOTS = 4
NN = (((1,), (0,)), ((), ()))
NT = (((1,), (1,)), ((), ()))
VMEM_LIMIT = 63 * 1024 * 1024
MESH = pl.DeviceIdType.MESH
ANY = pl.BlockSpec(memory_space=pl.ANY)


def dot(a, b, dims):
    return lax.dot_general(a, b, dims, preferred_element_type=F32)


class Peers:
    def __init__(self):
        z, y, t = lax.axis_index('dpy'), lax.axis_index('dpx'), lax.axis_index('tp')
        self.z, self.y, self.t = z, y, t
        self.sib = (z, y, t + 1 - 2 * (t % 2))
        self.xp = (z, y, (t + 2) % 4)
        self.yp = (z, 1 - y, t)
        self.zp = (1 - z, y, t)

    def barrier(self):
        sem = pltpu.get_barrier_semaphore()
        for peer in (self.sib, self.xp, self.yp, self.zp):
            pl.semaphore_signal(sem, inc=1, device_id=peer, device_id_type=MESH)
        pl.semaphore_wait(sem, 4)

    def rel(self, d):
        zr = self.z if d // 2 == 0 else 1 - self.z
        yr = self.y if d % 2 == 0 else 1 - self.y
        return zr * 2 + yr


class Sems:
    def __init__(self, send, recv, local):
        self.send, self.recv, self.local = send, recv, local
        self.n = self.m = 0

    def remote(self, src, dst, peer):
        i = self.n
        self.n += 1
        return lambda: pltpu.make_async_remote_copy(src_ref=src(), dst_ref=dst(), send_sem=self.send.at[i], recv_sem=self.recv.at[i],
                                                    device_id=peer, device_id_type=MESH)

    def copy(self, src, dst):
        i = self.m
        self.m += 1
        return lambda: pltpu.make_async_copy(src(), dst(), self.local.at[i])


def at_ticks(actions, tick, position=0, points=1):
    for k in sorted(actions):
        if k % points == position:
            @pl.when(tick == k)
            def _(k=k):
                for action in actions[k]:
                    action()


class Scatter:
    def __init__(self, sems, peers, partial, mine, bufs, out, rows, load=True):
        r0, r1, r2, r3 = self.bufs = bufs
        first, count = rows
        h = count // 2
        self.mine, self.all, self.lo, self.hi = mine, pl.ds(first, count), pl.ds(first, h), pl.ds(first + h, h)
        self.half = half = pl.ds(first // 2, h)
        every, lo, hi = self.all, self.lo, self.hi
        self.load, self.c0, self.c1, self.c2 = [], [], [], []
        for x in range(2):
            def near(k, part, x=x):
                return lambda: mine(x).at[k, part]

            def place(buf, *index):
                return lambda: buf.at[index]
            if load:
                self.load.append(sems.copy(lambda x=x: partial(2 * x).at[:, every], near(slice(None), every)))
            self.c0.append(sems.remote(lambda x=x: partial(2 * x + 1).at[:, every], place(r0, x, slice(None), every), peers.sib))
            self.c1.append([sems.remote(near(2 * k + 1, lo), place(r1, 0, x, k, half), peers.yp) for k in range(2)]
                           + [sems.remote(near(2 + k, hi), place(r1, 1, x, k, half), peers.zp) for k in range(2)])
            self.c2.append([sems.remote(near(2, lo), place(r2, 0, x, half), peers.zp), sems.remote(near(1, hi), place(r2, 1, x, half), peers.yp)])
        self.c3 = sems.remote(lambda: mine(1).at[0, every], place(r3, every), peers.xp)
        self.store = sems.copy(lambda: mine(0).at[0, every], out)

    def start(self, x):
        self.c0[x]().start()
        if self.load:
            self.load[x]().start()

    def add0(self, x):
        if self.load:
            self.load[x]().wait()
        self.c0[x]().wait_recv()
        mine, r0 = self.mine(x), self.bufs[0].at[x]

        def body(k, carry):
            mine[k, self.all] = mine[k, self.all] + r0[k, self.all]
            return carry
        lax.fori_loop(0, 4, body, 0)

    def send1(self, x):
        for c in self.c1[x]:
            c().start()

    def add1(self, x):
        for c in self.c1[x]:
            c().wait_recv()
        mine, r1 = self.mine(x), self.bufs[1]

        def body(k, carry):
            mine[2 * k, self.lo] = mine[2 * k, self.lo] + r1[0, x, k, self.half]
            mine[k, self.hi] = mine[k, self.hi] + r1[1, x, k, self.half]
            return carry
        lax.fori_loop(0, 2, body, 0)

    def send2(self, x):
        for c in self.c2[x]:
            c().start()

    def add2(self, x):
        for c in self.c2[x]:
            c().wait_recv()
        mine, r2 = self.mine(x), self.bufs[2]
        mine[0, self.lo] = mine[0, self.lo] + r2[0, x, self.half]
        mine[0, self.hi] = mine[0, self.hi] + r2[1, x, self.half]

    def send3(self):
        self.c3().start()

    def add3(self):
        self.c3().wait_recv()
        mine = self.mine(0)
        mine[0, self.all] = (mine[0, self.all] + self.bufs[3][self.all]) * (1 / SLOTS)

    def out(self):
        self.store().start()

    def finish(self):
        for c in self.c0 + sum(self.c1, []) + sum(self.c2, []) + [self.c3]:
            c().wait_send()
        self.store().wait()

    def both(self, name):
        for x in range(2):
            getattr(self, name)(x)


def scatter_bufs(rows, d):
    return [pltpu.VMEM((2, 4, rows, d), F32), pltpu.VMEM((2, 2, 2, rows // 2, d), F32), pltpu.VMEM((2, 2, rows // 2, d), F32), pltpu.VMEM((rows, d), F32)]


def steps(job, plan):
    out = []
    for k, name in plan:
        out.append((k, functools.partial(job.both, name) if name[-1] in '012' or name == 'start' else getattr(job, name)))
    return out


class Gather:
    def __init__(self, sems, peers, blocks):
        self.sib = [sems.remote(own, lambda dst=dst: dst(1), peers.sib) for own, dst in blocks]
        self.xp = [sems.remote(own, lambda dst=dst: dst(2), peers.xp) for own, dst in blocks]
        self.fwd = [sems.remote(lambda dst=dst: dst(2), lambda dst=dst: dst(3), peers.sib) for own, dst in blocks]

    def start(self, blocks):
        for i in blocks:
            self.sib[i]().start()
            self.xp[i]().start()

    def forward(self, i):
        self.xp[i]().wait_recv()
        self.fwd[i]().start()

    def finish(self, sib=True):
        for i in range(len(self.sib)):
            if sib:
                self.sib[i]().wait_recv()
                self.fwd[i]().wait_recv()
            self.sib[i]().wait_send()
            self.xp[i]().wait_send()
            self.fwd[i]().wait_send()


class Bounce:
    def __init__(self, sems, items, buf):
        self.steps = []
        prev = None
        for own, dst, rows in items:
            ld = sems.copy(own, lambda rows=rows: buf.at[pl.ds(0, rows)])
            st = sems.copy(lambda rows=rows: buf.at[pl.ds(0, rows)], lambda dst=dst: dst(0))
            self.steps.append(functools.partial(self.load, prev, ld))
            self.steps.append(functools.partial(self.flip, ld, st))
            prev = st
        self.steps.append(lambda prev=prev: prev().wait())

    @staticmethod
    def load(prev, ld):
        if prev is not None:
            prev().wait()
        ld().start()

    @staticmethod
    def flip(ld, st):
        ld().wait()
        st().start()


def merge(*lists):
    actions = {}
    for pairs in lists:
        for k, action in pairs:
            actions.setdefault(k, []).append(action)
    return actions


SEMS = [pltpu.SemaphoreType.DMA((96,)), pltpu.SemaphoreType.DMA((96,)), pltpu.SemaphoreType.DMA((24,))]


def whole(*shape):
    return pl.BlockSpec(shape, lambda *_: (0,) * len(shape), pipeline_mode=pl.Buffered(1))


def leading(*shape):
    return pl.BlockSpec((1,) + shape, lambda j, *_: (j,) + (0,) * len(shape))


def params(collective_id, axes):
    return pltpu.CompilerParams(vmem_limit_bytes=VMEM_LIMIT, dimension_semantics=('arbitrary',) * axes, collective_id=collective_id, has_side_effects=True)


def mlp_slot(seqs, seq, w1, w2, w1t, yt, dz, acc, gt, dht, tick):
    w1t[...] = w1[...].T

    def block(i, carry):
        tick(i)
        cols = pl.ds(pl.multiple_of(i * seq, seq), seq)
        h = dot(w1t[...], yt[:, cols], NN)
        dg = dot(w2[...], dz[:, cols], NN)
        c0 = math.sqrt(2 / math.pi)
        c1 = 0.044715 * c0
        h2 = h * h
        t = jnp.tanh(h * (c0 + c1 * h2))
        q = 0.5 * t + 0.5
        g = h * q
        dh = dg * (q + (g * (1.0 - t)) * (c0 + (3 * c1) * h2))
        gt[:, cols] = g.astype(BF16)
        dh = dh.astype(BF16)
        dht[:, cols] = dh
        acc[:, cols] += dot(w1[...], dh, NN)
        return carry
    lax.fori_loop(0, seqs, block, 0)


def store_shards(peers, g_ref, j, g):
    rows = g_ref.shape[-2]
    for d in range(4):
        g_ref[0, j, peers.rel(d)] = g[d * rows:(d + 1) * rows]


def mlp_rest(slot, actions, peers, seqs, seq, w1, w2, dz, dy_ref, g_ref, w1t, yt, acc, gt, dht):
    points = seqs + 2
    first = slot * points

    def tick(i):
        at_ticks({k: v for k, v in actions.items() if k % points < seqs}, first + i)
    mlp_slot(seqs, seq, w1, w2, w1t, yt, dz, acc, gt, dht, tick)
    at_ticks(actions, first + seqs, seqs, points)
    store_shards(peers, g_ref, 0, dot(gt[...], dz[...], NT))
    at_ticks(actions, first + seqs + 1, seqs + 1, points)
    store_shards(peers, g_ref, 1, dot(yt[...], dht[...], NT))

    @pl.when(slot == SLOTS - 1)
    def _():
        dy_ref[...] = (dz[...].astype(F32) + acc[...]).astype(BF16)


def attn_weights(layer, wq, wo, wa_g):
    nq, d = wq.shape[1:]
    return [(lambda: wq.at[layer], lambda j: wa_g.at[j, pl.ds(0, nq)], nq), (lambda: wo.at[layer], lambda j: wa_g.at[j, pl.ds(nq, d - nq)], d - nq)]


class Spread:
    def __init__(self, sems, peers, wb, pieces):
        rows = wb.shape[2] // pieces
        y = peers.y

        def piece(slot, m, k):
            return lambda: wb.at[slot, m, pl.ds(k * rows, rows)]
        every = range(pieces)
        self.sib = sems.remote(lambda: wb.at[0], lambda: wb.at[1], peers.sib)
        self.xp = [sems.remote(piece(0, y, k), piece(2, y, k), peers.xp) for k in every]
        self.fy, self.wy = [], []
        for k in every:
            self.fy.append(sems.remote(piece(2, y, k), piece(2, y, k), peers.yp))
            sems.n -= 1
            self.wy.append(sems.remote(piece(2, 1 - y, k), piece(2, 1 - y, k), peers.yp))
        self.fs = [sems.remote(piece(2, y, k), piece(3, y, k), peers.sib) for k in every]
        self.fs2 = [sems.remote(piece(2, 1 - y, k), piece(3, 1 - y, k), peers.sib) for k in every]

    def start(self):
        for c in self.xp + [self.sib]:
            c().start()

    def forward(self, k):
        self.xp[k]().wait_recv()
        self.fy[k]().start()
        self.fs[k]().start()

    def forward2(self, k):
        self.wy[k]().wait_recv()
        self.fs2[k]().start()

    def arrived(self):
        for c in self.fs + self.fs2:
            c().wait_recv()

    def finish(self):
        for c in [self.sib] + self.xp + self.fy + self.fs + self.fs2:
            c().wait_send()


def mlp_first_kernel(layer, y_ref, dz_ref, wup, wdn, wq, wo, dy_ref, g_ref, wa_g, yt, dzt, acc, w1t, gt, dht, wb, bounce, *rest):
    slot = pl.program_id(0)
    seqs, seq = y_ref.shape[1:3]
    peers, sems = Peers(), Sems(*rest)
    own = [sems.copy(lambda w=w: w.at[layer], lambda m=m: wb.at[0, m]) for m, w in enumerate((wup, wdn))]
    blocks = attn_weights(layer, wq, wo, wa_g)
    gather = Gather(sems, peers, [r[:2] for r in blocks])
    hop = Bounce(sems, blocks, bounce)
    spread = Spread(sems, peers, wb, SLOTS)

    @pl.when(slot == 0)
    def _():
        for c in own:
            c().start()
        peers.barrier()
        for c in own:
            c().wait()
        spread.start()
        gather.start(range(2))
        acc[...] = jnp.zeros_like(acc)
        for s in range(seqs):
            cols = slice(s * seq, (s + 1) * seq)
            yt[:, cols] = y_ref[0, s].T
            dzt[:, cols] = dz_ref[s].T

    @pl.when(slot == 1)
    def _():
        spread.sib().wait_recv()

    @pl.when(slot == 2)
    def _():
        spread.forward2(2)
        spread.forward2(3)

    @pl.when(slot == 3)
    def _():
        spread.arrived()
    ahead = [(4, 0), (6, 1), (8, 2), (11, 3)]
    actions = merge([(14 + k, s) for k, s in enumerate(hop.steps)], [(t, functools.partial(spread.forward, k)) for t, k in ahead],
                    [(7, functools.partial(spread.forward2, 0)), (10, functools.partial(spread.forward2, 1)), (21, functools.partial(gather.forward, 0))])
    mlp_rest(slot, actions, peers, seqs, seq, wb.at[slot, 0], wb.at[slot, 1], dzt, dy_ref, g_ref, w1t, yt, acc, gt, dht)

    @pl.when(slot == SLOTS - 1)
    def _():
        gather.forward(1)
        spread.finish()
        gather.finish()


def mlp_first(layer, y, dz, wup, wdn, wq, wo):
    d, f = wup.shape[1:]
    seq = y.shape[2]
    seqs = y.shape[1] // SLOTS
    tok = seqs * seq
    once = pl.Buffered(1)
    return pl.pallas_call(
        functools.partial(mlp_first_kernel, layer),
        out_shape=(jax.ShapeDtypeStruct((d, tok), BF16), jax.ShapeDtypeStruct((SLOTS, 2, 4, d // 4, f), F32), jax.ShapeDtypeStruct((SLOTS, d, d), BF16)),
        grid=(SLOTS,),
        in_specs=[pl.BlockSpec((1, seqs, seq, d), lambda j: (layer, lax.axis_index('tp'), 0, 0), pipeline_mode=once),
                  pl.BlockSpec((seqs, seq, d), lambda j: (lax.axis_index('tp'), 0, 0), pipeline_mode=once), ANY, ANY, ANY, ANY],
        out_specs=[whole(d, tok), leading(2, 4, d // 4, f), ANY],
        scratch_shapes=[pltpu.VMEM((d, tok), BF16), pltpu.VMEM((d, tok), BF16), pltpu.VMEM((d, tok), F32), pltpu.VMEM((f, d), BF16),
                        pltpu.VMEM((f, tok), BF16), pltpu.VMEM((f, tok), BF16), pltpu.VMEM((SLOTS, 2, d, f), BF16), pltpu.VMEM((d, d), BF16)] + SEMS,
        compiler_params=params(0, 1),
        name='mlp_first',
    )(y, dz, wup, wdn, wq, wo)


def mlp_second_kernel(layer, y_ref, dz_ref, w1_ref, w2_ref, partial, wq, wo, dy_ref, g_ref, wa_g, red, yt, acc, w1t, gt, dht, bounce, mine, *rest):
    slot = pl.program_id(0)
    seqs, seq = y_ref.shape[1:3]
    bufs, rest = rest[:4], rest[4:]
    peers, sems = Peers(), Sems(*rest)
    blocks = attn_weights(layer, wq, wo, wa_g)
    gather = Gather(sems, peers, [r[:2] for r in blocks])
    hop = Bounce(sems, blocks, bounce)
    rows = mine.shape[2] // 2
    a, b = jobs = [Scatter(sems, peers, lambda s: partial.at[s], lambda x: mine.at[x], bufs, lambda j=j: red.at[pl.ds(j * rows, rows)], (j * rows, rows)) for j in range(2)]

    @pl.when(slot == 0)
    def _():
        peers.barrier()
        for job in jobs:
            job.both('start')
        gather.start(range(2))
        acc[...] = jnp.zeros_like(acc)
        for s in range(seqs):
            yt[:, slice(s * seq, (s + 1) * seq)] = y_ref[0, s].T
    actions = merge([(4 + k, s) for k, s in enumerate(hop.steps)], [(11, functools.partial(gather.forward, 0)), (12, functools.partial(gather.forward, 1))],
                    steps(a, [(3, 'add0'), (4, 'send1'), (10, 'add1'), (11, 'send2'), (17, 'add2'), (18, 'send3'), (22, 'add3'), (23, 'out')]),
                    steps(b, [(4, 'add0'), (5, 'send1'), (15, 'add1'), (16, 'send2'), (20, 'add2'), (21, 'send3')]))
    mlp_rest(slot, actions, peers, seqs, seq, w1_ref.at[0], w2_ref.at[0], dz_ref, dy_ref, g_ref, w1t, yt, acc, gt, dht)

    @pl.when(slot == SLOTS - 1)
    def _():
        b.add3()
        gather.finish()
        b.out()
        a.finish()
        b.finish()


def mlp_second(layer, y, dz, w1, w2, partial, wq, wo):
    d, f = w1.shape[1:]
    seq = y.shape[2]
    seqs = y.shape[1] // SLOTS
    tok = seqs * seq
    return pl.pallas_call(
        functools.partial(mlp_second_kernel, layer),
        out_shape=(jax.ShapeDtypeStruct((d, tok), BF16), jax.ShapeDtypeStruct((SLOTS, 2, 4, d // 4, f), F32), jax.ShapeDtypeStruct((SLOTS, d, d), BF16),
                   jax.ShapeDtypeStruct((d // 4, d), F32)),
        grid=(SLOTS,),
        in_specs=[pl.BlockSpec((1, seqs, seq, d), lambda j: (layer, lax.axis_index('tp'), 0, 0), pipeline_mode=pl.Buffered(1)),
                  whole(d, tok), leading(d, f), leading(f, d), ANY, ANY, ANY],
        out_specs=[whole(d, tok), leading(2, 4, d // 4, f), ANY, ANY],
        scratch_shapes=[pltpu.VMEM((d, tok), BF16), pltpu.VMEM((d, tok), F32), pltpu.VMEM((f, d), BF16),
                        pltpu.VMEM((f, tok), BF16), pltpu.VMEM((f, tok), BF16), pltpu.VMEM((d, d), BF16), pltpu.VMEM((2, 4, d // 4, d), F32)]
        + scatter_bufs(d // 4, d) + SEMS,
        compiler_params=params(1, 1),
        name='mlp_second',
    )(y, dz, w1, w2, partial, wq, wo)


def attn_step(peers, x_ref, dy_ref, w_ref, xt, acc, gacc, qkv, do, b1, b2, emit):
    s, slot = pl.program_id(0), pl.program_id(1)
    step = s * SLOTS + slot
    last = SLOTS * SLOTS - 1
    before = (step + last) % (last + 1)
    seq, d = x_ref.shape[-2:]
    nqkv = qkv.shape[0]
    third = nqkv // 3
    split = d - b2.shape[1]
    rows = d // 4

    def tokens(n):
        return pl.ds(pl.multiple_of(n * seq, seq), seq)

    @pl.when(step == 0)
    def _():
        xt[1] = jnp.zeros((d, seq), BF16)
        for j in range(SLOTS):
            gacc[j] = jnp.zeros(gacc.shape[1:], F32)
        for j in range(2):
            b1[j] = jnp.zeros(b1.shape[1:], BF16)
            b2[j] = jnp.zeros(b2.shape[1:], BF16)

    @pl.when(slot == 0)
    def _():
        xt[s % 2] = x_ref[0, 0].T

    def grads(n):
        ps, pj, par = n // SLOTS, n % SLOTS, n % 2
        third_d = d // 3

        def weights(c):
            cols = slice(c * third_d, (c + 1) * third_d)
            g = dot(xt[ps % 2], b1[par, cols], NT)
            if c == 2:
                g = g + dot(dy_ref[:, tokens(ps)], b2[par], NT)
            for k in range(4):
                r = peers.rel(k)
                gacc[pj, r, :, cols] = gacc[pj, r, :, cols] + g[k * rows:(k + 1) * rows]

        def inputs(c):
            part = slice(c * third_d, (c + 1) * third_d)
            acc[part] += dot(w_ref[pj, :, part].T, b1[par], NN)
        return [functools.partial(f, c) for c in range(3) for f in (weights, inputs)]
    x_t = xt[s % 2]
    dy_t = dy_ref[:, tokens(s)]
    now = step % 2
    qkv[...] = dot(w_ref[slot, pl.ds(0, nqkv), :], x_t, NN).astype(BF16)
    do[...] = dot(w_ref[slot, pl.ds(nqkv, d - nqkv), :], dy_t, NN).astype(BF16)
    scale = HEAD ** -0.5
    exp_scale = scale * math.log2(math.e)
    qb = seq // 2
    units = [(h, slice(c * qb, (c + 1) * qb)) for h in range(third // HEAD) for c in range(2)]

    def scores(h, qc):
        q_rows, k_rows, v_rows = head_rows(h)
        return dot(qkv[k_rows, :].T, qkv[q_rows, qc], NN), dot(qkv[v_rows, :].T, do[q_rows, qc] * scale, NN)

    def head_rows(h):
        return [slice(i * third + h * HEAD, i * third + (h + 1) * HEAD) for i in range(3)]
    ahead = scores(*units[0])
    pieces = grads(before)
    for n, (h, qc) in enumerate(units):
        sc, dp_t = ahead
        if n + 1 < len(units):
            ahead = scores(*units[n + 1])
        pieces[n]()
        q_rows, k_rows, v_rows = head_rows(h)
        m = jnp.max(sc, axis=0, keepdims=True)
        e = jnp.exp2((sc - m) * exp_scale)
        inv = 1.0 / jnp.sum(e, axis=0, keepdims=True)
        rd = jnp.sum(e * dp_t, axis=0, keepdims=True) * inv
        p = e * inv
        p_bf = p.astype(BF16)
        ds = (p * (dp_t - rd)).astype(BF16)
        b2[now, pl.ds(b2.shape[1] - third + h * HEAD, HEAD), qc] = dot(qkv[v_rows, :], p_bf, NN).astype(BF16)
        b1[now, q_rows, qc] = dot(qkv[k_rows, :], ds, NN).astype(BF16)
        dv_c = dot(do[q_rows, qc], p_bf, NT)
        dk_c = dot(qkv[q_rows, qc], ds, NT)
        if n % 2 == 0:
            dv, dk = dv_c, dk_c
        else:
            b1[now, k_rows] = (dk + dk_c).astype(BF16)
            b1[now, v_rows] = (dv + dv_c).astype(BF16)

    @pl.when(slot == 0)
    def _():
        @pl.when(s > 0)
        def _():
            emit(s - 1)
        acc[...] = dy_ref[:, tokens(s)].astype(F32)

    @pl.when(step == last)
    def _():
        for piece in grads(last):
            piece()
        emit(s)


ATTN_IN = 3
ATTN_SCRATCH = 7
JOB_PLAN = [(2, 'add0'), (3, 'send1'), (9, 'add1'), (10, 'send2')], [(3, 'add0'), (4, 'send1'), (14, 'add1'), (15, 'send2')]


def attn_first_kernel(layer, x_ref, dy_ref, w_ref, partial, wup, wdn, dx_ref, g_hbm, w1_g, w2_g, red, *rest):
    body, rest = rest[:ATTN_SCRATCH], rest[ATTN_SCRATCH:]
    gacc, mine, bounce = body[2], rest[:2], rest[-4]
    seq = x_ref.shape[-2]
    step = pl.program_id(0) * SLOTS + pl.program_id(1)
    peers, sems = Peers(), Sems(*rest[-3:])
    a, b = jobs = [Scatter(sems, peers, lambda s, j=j: partial.at[s, j], lambda x, j=j: mine[j].at[x], rest[2 + 4 * j:6 + 4 * j], lambda j=j: red.at[j],
                           (0, red.shape[1])) for j in range(2)]
    blocks = [(lambda w=w: w.at[layer - 1], lambda j, g=g: g.at[j], wup.shape[1]) for w, g in ((wup, w1_g), (wdn, w2_g))]
    gather = Gather(sems, peers, [r[:2] for r in blocks])
    hop = Bounce(sems, blocks, bounce)
    stores = [sems.copy(lambda j=j: gacc.at[j], lambda j=j: g_hbm.at[j]) for j in range(SLOTS)]
    actions = merge(steps(a, JOB_PLAN[0]), steps(b, JOB_PLAN[1]), [(5 + k, s) for k, s in enumerate(hop.steps)],
                    [(7, functools.partial(gather.forward, 0)), (13, functools.partial(gather.forward, 1))])

    @pl.when(step == 0)
    def _():
        peers.barrier()
        for job in jobs:
            job.both('start')
        gather.start(range(2))
    at_ticks(actions, step)

    def emit(s):
        dx_ref[:, pl.ds(pl.multiple_of(s * seq, seq), seq)] = acc[...].astype(BF16)
    acc = body[1]
    attn_step(peers, x_ref, dy_ref, w_ref, *body, emit)

    @pl.when(step == SLOTS * SLOTS - 1)
    def _():
        for job in jobs:
            job.both('add2')
            job.send3()
        for c in stores:
            c().start()
        gather.finish()
        for job in jobs:
            job.add3()
        for job in jobs:
            job.out()
        for c in stores:
            c().wait()
        for job in jobs:
            job.finish()


def attn_last_kernel(x_ref, dy_ref, w_ref, partial, dxg, red, red_last, *rest):
    body, rest = rest[:ATTN_SCRATCH], rest[ATTN_SCRATCH:]
    acc, gacc, mine, dxb, free = body[1], body[2], rest[:2], rest[-5], rest[-4]
    step = pl.program_id(0) * SLOTS + pl.program_id(1)
    seqs = pl.num_programs(0)
    peers, sems = Peers(), Sems(*rest[-3:])
    nred = red.shape[1]
    a, b = jobs = [Scatter(sems, peers, lambda s, j=j: partial.at[s, j], lambda x, j=j: mine[j].at[x], rest[2 + 4 * j:6 + 4 * j], lambda j=j: red.at[j],
                           (0, nred)) for j in range(2)]
    h = nred // 2
    ends = [Scatter(sems, peers, lambda s: gacc.at[s], lambda x: gacc.at[2 * x], rest[2:6], lambda j=j: red_last.at[pl.ds(j * h, h)], (j * h, h), load=False)
            for j in range(2)]
    t = peers.t
    t2 = (t + 2) % SLOTS
    sib, xp, fwd, mine_dx = [], [], [], []
    for s in range(SLOTS):
        def src(s=s):
            return dxb.at[s]

        def dst(s=s):
            return dxg.at[t * SLOTS + s]

        def other(s=s):
            return dxg.at[t2 * SLOTS + s]
        mine_dx.append(sems.copy(src, dst))
        sib.append(sems.remote(src, dst, peers.sib))
        xp.append(sems.remote(src, dst, peers.xp))
        fwd.append(sems.remote(other, other, peers.sib))

    def freed(i, who):
        for peer in who:
            pl.semaphore_signal(free.at[i], inc=1, device_id=peer, device_id_type=MESH)

    def forward(s):
        xp[s]().wait_recv()
        fwd[s]().start()
    actions = merge(steps(a, JOB_PLAN[0]), steps(b, JOB_PLAN[1]), [(3, lambda: freed(0, [peers.sib])), (10, lambda: freed(1, [peers.yp, peers.zp])),
                                                                  (10, functools.partial(forward, 0)), (14, functools.partial(forward, 1))])

    @pl.when(step == 0)
    def _():
        peers.barrier()
        for job in jobs:
            job.both('start')
    at_ticks(actions, step)

    def emit(s):
        dxb[s] = acc[...].T.astype(BF16)
        for k in range(SLOTS):
            @pl.when(s == k)
            def _(k=k):
                for c in (xp, sib, mine_dx):
                    c[k]().start()
    attn_step(peers, x_ref, dy_ref, w_ref, *body, emit)

    @pl.when(step == SLOTS * SLOTS - 1)
    def _():
        pl.semaphore_wait(free.at[0], 1)
        for job in ends:
            job.both('start')
        a.both('add2')
        a.send3()
        freed(2, [peers.yp, peers.zp])
        pl.semaphore_wait(free.at[1], 2)
        for job in ends:
            job.both('add0')
        for job in ends:
            job.both('send1')
        forward(2)
        b.both('add2')
        b.send3()
        a.add3()
        freed(3, [peers.xp])
        pl.semaphore_wait(free.at[2], 2)
        for job in ends:
            job.both('add1')
            job.both('send2')
        pl.semaphore_wait(free.at[3], 1)
        forward(3)
        a.out()
        b.add3()
        b.out()
        for job in ends:
            job.both('add2')
            job.send3()
        for s in range(SLOTS):
            mine_dx[s]().wait()
            sib[s]().wait()
            xp[s]().wait_send()
        for job in ends:
            job.add3()
        for job in ends:
            job.out()
        for s in range(SLOTS):
            fwd[s]().wait()
        for job in jobs + ends:
            job.finish()


def attn_specs(layer, x, w):
    slots, nw, d = w.shape
    seq = x.shape[2]
    seqs = x.shape[1] // slots
    tok = seqs * seq
    nqkv = nw * 3 // 4
    in_specs = [pl.BlockSpec((1, 1, seq, d), lambda s, j: (layer, lax.axis_index('tp') * seqs + s, 0, 0)), whole(d, tok), whole(slots, nw, d), ANY]
    scratch = [pltpu.VMEM((2, d, seq), BF16), pltpu.VMEM((d, seq), F32), pltpu.VMEM((slots, 4, d // 4, nw), F32), pltpu.VMEM((nqkv, seq), BF16),
               pltpu.VMEM((nw - nqkv, seq), BF16), pltpu.VMEM((2, nw, seq), BF16), pltpu.VMEM((2, d // 3, seq), BF16)]
    scratch += [pltpu.VMEM((2, 4, d // 4, d), F32)] * 2 + scatter_bufs(d // 4, d) * 2
    red = jax.ShapeDtypeStruct((2, d // 4, d), F32)
    return (slots, seqs), in_specs, scratch, red, tok


def attn_first(layer, x, dy, w, partial, wup, wdn):
    grid, in_specs, scratch, red, tok = attn_specs(layer, x, w)
    slots, nw, d = w.shape
    gathered = [jax.ShapeDtypeStruct((slots, d, d), BF16)] * 2
    return pl.pallas_call(
        functools.partial(attn_first_kernel, layer),
        out_shape=[jax.ShapeDtypeStruct((d, tok), BF16), jax.ShapeDtypeStruct((slots, 4, d // 4, nw), F32)] + gathered + [red],
        grid=grid,
        in_specs=in_specs + [ANY, ANY],
        out_specs=[whole(d, tok)] + [ANY] * 4,
        scratch_shapes=scratch + [pltpu.VMEM((d, d), BF16)] + SEMS,
        compiler_params=params(2, 2),
        name='attn_first',
    )(x, dy, w, partial, wup, wdn)


def attn_last(layer, x, dy, w, partial):
    grid, in_specs, scratch, red, tok = attn_specs(layer, x, w)
    slots, nw, d = w.shape
    seq = x.shape[2]
    return pl.pallas_call(
        attn_last_kernel,
        out_shape=[jax.ShapeDtypeStruct((x.shape[1], seq, d), BF16), red, jax.ShapeDtypeStruct(red.shape[1:], F32)],
        grid=grid,
        in_specs=in_specs,
        out_specs=[ANY] * 3,
        scratch_shapes=scratch + [pltpu.VMEM((slots, seq, d), BF16), pltpu.SemaphoreType.REGULAR((4,))] + SEMS,
        compiler_params=params(3, 2),
        name='attn_last',
    )(x, dy, w, partial)


def solution(mesh):
    assert dict(mesh.shape) == {'dpy': 2, 'dpx': 2, 'tp': SLOTS}
    act_spec = P(None, DATA_AXES, None, None)

    def device_backward(x_saved, y_saved, dz_top, w_qkv, w_out, w_up, w_down):
        layers, d = w_up.shape[:2]
        assert layers == 2
        heads, hd = w_out.shape[1:3]
        n = 3 * heads * hd
        wq = w_qkv.transpose(0, 2, 3, 4, 1).reshape(layers, n, d)
        wo = w_out.reshape(layers, heads * hd, d)
        dy1, gm1, wa1 = mlp_first(1, y_saved, dz_top, w_up, w_down, wq, wo)
        dx1, ga1, w1_0, w2_0, rm1 = attn_first(1, x_saved, dy1, wa1, gm1, w_up, w_down)
        dy0, gm0, wa0, ra1 = mlp_second(0, y_saved, dx1, w1_0, w2_0, ga1, wq, wo)
        d_input, rm0, ra0 = attn_last(0, x_saved, dy0, wa0, gm0)
        g_a = jnp.stack([ra0, ra1])
        g_qkv = g_a[:, :, :n].reshape(layers, d // 4, 3, heads, hd)
        g_out = g_a[:, :, n:].transpose(0, 2, 1).reshape(layers, heads, hd, d // 4)
        return d_input, g_qkv, g_out, jnp.stack([rm0[1], rm1[1]]), jnp.stack([rm0[0], rm1[0]])

    tp_last = P(None, None, None, 'tp', None), P(None, 'tp', None, None), P(None, None, 'tp'), P(None, 'tp', None)
    return jax.shard_map(device_backward, mesh=mesh,
                         in_specs=(act_spec, act_spec, P(DATA_AXES, None, None)) + tp_last,
                         out_specs=(P(DATA_AXES, None, None), P(None, DATA_AXES, None, 'tp', None), P(None, 'tp', None, DATA_AXES), P(None, DATA_AXES, 'tp'), P(None, ('tp', 'dpy', 'dpx'), None)),
                         check_vma=False)
```

```python
import functools
import math
import re

import jax
import jax.numpy as jnp
from jax import lax
from jax.experimental import pallas as pl
from jax.experimental.pallas import tpu as pltpu
from jax.sharding import PartitionSpec as P

DATA_AXES = ('dpy', 'dpx')
F32 = jnp.float32
BF16 = jnp.bfloat16
HEAD = 64
SLOTS = 4
LOOK_AHEAD = 3
NN = (((1,), (0,)), ((), ()))
NT = (((1,), (1,)), ((), ()))
VMEM_LIMIT = 63 * 1024 * 1024
MESH = pl.DeviceIdType.MESH
ANY = pl.BlockSpec(memory_space=pl.ANY)


def dot(a, b, dims):
    return lax.dot_general(a, b, dims, preferred_element_type=F32)


class Peers:
    def __init__(self):
        z, y, t = lax.axis_index('dpy'), lax.axis_index('dpx'), lax.axis_index('tp')
        self.z, self.y, self.t = z, y, t
        self.sib = (z, y, t + 1 - 2 * (t % 2))
        self.xp = (z, y, (t + 2) % 4)
        self.yp = (z, 1 - y, t)
        self.zp = (1 - z, y, t)

    def barrier(self):
        sem = pltpu.get_barrier_semaphore()
        with jax.named_scope('entry'):
            for peer in (self.sib, self.xp, self.yp, self.zp):
                pl.semaphore_signal(sem, inc=1, device_id=peer, device_id_type=MESH)
            pl.semaphore_wait(sem, 4)

    def rel(self, d):
        zr = self.z if d // 2 == 0 else 1 - self.z
        yr = self.y if d % 2 == 0 else 1 - self.y
        return zr * 2 + yr


class Sems:
    def __init__(self, send, recv, local):
        self.send, self.recv, self.local = send, recv, local
        self.n = self.m = 0

    def remote(self, src, dst, peer):
        i = self.n
        self.n += 1
        return lambda: pltpu.make_async_remote_copy(src_ref=src(), dst_ref=dst(), send_sem=self.send.at[i], recv_sem=self.recv.at[i],
                                                    device_id=peer, device_id_type=MESH)

    def copy(self, src, dst):
        i = self.m
        self.m += 1
        return lambda: pltpu.make_async_copy(src(), dst(), self.local.at[i])


def at_ticks(actions, tick, position=0, points=1):
    for k in sorted(actions):
        if k % points == position:
            @pl.when(tick == k)
            def _(k=k):
                with jax.named_scope('t%d' % k):
                    for action in actions[k]:
                        action()


class Scatter:
    def __init__(self, sems, peers, partial, mine, bufs, out, rows, load=True, half_out=None):
        r0, r1, r2, r3 = self.bufs = bufs
        first, count = rows
        h = count // 2
        self.mine, self.all, self.lo, self.hi = mine, pl.ds(first, count), pl.ds(first, h), pl.ds(first + h, h)
        self.half = half = pl.ds(first // 2, h)
        every, lo, hi = self.all, self.lo, self.hi
        self.load, self.c0, self.c1, self.c2 = [], [], [], []
        for x in range(2):
            def near(k, part, x=x):
                return lambda: mine(x).at[k, part]

            def place(buf, *index):
                return lambda: buf.at[index]
            if load:
                self.load.append(sems.copy(lambda x=x: partial(2 * x).at[:, every], near(slice(None), every)))
            self.c0.append(sems.remote(lambda x=x: partial(2 * x + 1).at[:, every], place(r0, x, slice(None), every), peers.sib))
            self.c1.append([sems.remote(near(2 * k + 1, lo), place(r1, 0, x, k, half), peers.yp) for k in range(2)]
                           + [sems.remote(near(2 + k, hi), place(r1, 1, x, k, half), peers.zp) for k in range(2)])
            self.c2.append([sems.remote(near(2, lo), place(r2, 0, x, half), peers.zp), sems.remote(near(1, hi), place(r2, 1, x, half), peers.yp)])
        if half_out is None:
            self.c3 = sems.remote(lambda: mine(1).at[0, every], place(r3, every), peers.xp)
            self.store = [sems.copy(lambda: mine(0).at[0, every], out)]
        else:
            self.c3 = None
            self.store = [sems.copy(lambda x=x: mine(x).at[0, every], lambda x=x: half_out(x)) for x in range(2)]

    def start(self, x):
        self.c0[x]().start()
        if self.load:
            self.load[x]().start()

    def add0(self, x):
        if self.load:
            self.load[x]().wait()
        self.c0[x]().wait_recv()
        mine, r0 = self.mine(x), self.bufs[0].at[x]

        def body(k, carry):
            mine[k, self.all] = mine[k, self.all] + r0[k, self.all]
            return carry
        lax.fori_loop(0, 4, body, 0)

    def send1(self, x):
        for c in self.c1[x]:
            c().start()

    def add1(self, x):
        for c in self.c1[x]:
            c().wait_recv()
        mine, r1 = self.mine(x), self.bufs[1]

        def body(k, carry):
            mine[2 * k, self.lo] = mine[2 * k, self.lo] + r1[0, x, k, self.half]
            mine[k, self.hi] = mine[k, self.hi] + r1[1, x, k, self.half]
            return carry
        lax.fori_loop(0, 2, body, 0)

    def send2(self, x):
        for c in self.c2[x]:
            c().start()

    def add2(self, x):
        for c in self.c2[x]:
            c().wait_recv()
        mine, r2 = self.mine(x), self.bufs[2]
        mine[0, self.lo] = mine[0, self.lo] + r2[0, x, self.half]
        mine[0, self.hi] = mine[0, self.hi] + r2[1, x, self.half]

    def send3(self):
        self.c3().start()

    def add3(self):
        self.c3().wait_recv()
        mine = self.mine(0)
        mine[0, self.all] = (mine[0, self.all] + self.bufs[3][self.all]) * (1 / SLOTS)

    def out(self):
        for c in self.store:
            c().start()

    def finish(self):
        for c in self.c0 + sum(self.c1, []) + sum(self.c2, []) + ([self.c3] if self.c3 else []):
            c().wait_send()
        for c in self.store:
            c().wait()

    def both(self, name):
        for x in range(2):
            getattr(self, name)(x)


def scatter_bufs(rows, d):
    return [pltpu.VMEM((2, 4, rows, d), F32), pltpu.VMEM((2, 2, 2, rows // 2, d), F32), pltpu.VMEM((2, 2, rows // 2, d), F32), pltpu.VMEM((rows, d), F32)]


def steps(job, plan):
    out = []
    for tick, name, half in re.findall('([0-9]+)([a-z]+[0-3]?)([xy]?)', plan):
        if half:
            action = functools.partial(getattr(job, name), int(half == 'y'))
        else:
            action = functools.partial(job.both, name) if name[-1] in '012' else getattr(job, name)
        out.append((int(tick), action))
    return out


def ticks(plan, actions):
    return list(zip(map(int, plan.split(',')), actions))


class Gather:
    def __init__(self, sems, peers, blocks):
        self.sib = [sems.remote(own, lambda dst=dst: dst(1), peers.sib) for own, dst in blocks]
        self.xp = [sems.remote(own, lambda dst=dst: dst(2), peers.xp) for own, dst in blocks]
        self.fwd = [sems.remote(lambda dst=dst: dst(2), lambda dst=dst: dst(3), peers.sib) for own, dst in blocks]

    def start(self, blocks):
        for i in blocks:
            self.sib[i]().start()
            self.xp[i]().start()

    def forward(self, i):
        self.xp[i]().wait_recv()
        self.fwd[i]().start()

    def forwards(self):
        return [functools.partial(self.forward, i) for i in range(len(self.fwd))]

    def finish(self):
        for i in range(len(self.sib)):
            self.sib[i]().wait_recv()
            self.fwd[i]().wait_recv()
            self.sib[i]().wait_send()
            self.xp[i]().wait_send()
            self.fwd[i]().wait_send()


class Bounce:
    def __init__(self, sems, items, buf):
        self.steps = []
        prev = None
        for own, dst, rows in items:
            ld = sems.copy(own, lambda rows=rows: buf.at[pl.ds(0, rows)])
            st = sems.copy(lambda rows=rows: buf.at[pl.ds(0, rows)], lambda dst=dst: dst(0))
            self.steps.append(functools.partial(self.load, prev, ld))
            self.steps.append(functools.partial(self.flip, ld, st))
            prev = st
        self.steps.append(lambda prev=prev: prev().wait())

    @staticmethod
    def load(prev, ld):
        if prev is not None:
            prev().wait()
        ld().start()

    @staticmethod
    def flip(ld, st):
        ld().wait()
        st().start()


def merge(*lists):
    actions = {}
    for pairs in lists:
        for k, action in pairs:
            actions.setdefault(k, []).append(action)
    return actions


SEMS = [pltpu.SemaphoreType.DMA((96,)), pltpu.SemaphoreType.DMA((96,)), pltpu.SemaphoreType.DMA((24,))]


def whole(*shape):
    return pl.BlockSpec(shape, lambda *_: (0,) * len(shape), pipeline_mode=pl.Buffered(1))


def leading(*shape):
    return pl.BlockSpec((1,) + shape, lambda j, *_: (j,) + (0,) * len(shape))


def params(collective_id, axes):
    return pltpu.CompilerParams(vmem_limit_bytes=VMEM_LIMIT, dimension_semantics=('arbitrary',) * axes, collective_id=collective_id, has_side_effects=True)


def mlp_slot(seqs, seq, w1, w2, w1t, yt, dz, acc, gt, dht, tick):
    w1t[...] = w1[...].T

    def block(i, carry):
        tick(i)
        with jax.named_scope('mblock'):
            inner(i)
        return carry

    def inner(i):
        cols = pl.ds(pl.multiple_of(i * seq, seq), seq)
        h = dot(w1t[...], yt[:, cols], NN)
        dg = dot(w2[...], dz[:, cols], NN)
        c0 = math.sqrt(2 / math.pi)
        c1 = 0.044715 * c0
        h2 = h * h
        t = jnp.tanh(h * (c0 + c1 * h2))
        q = 0.5 * t + 0.5
        g = h * q
        dh = dg * (q + (g * (1.0 - t)) * (c0 + (3 * c1) * h2))
        gt[:, cols] = g.astype(BF16)
        dh = dh.astype(BF16)
        dht[:, cols] = dh
        acc[:, cols] += dot(w1[...], dh, NN)
    lax.fori_loop(0, seqs, block, 0)


def prepare(seqs, seq, acc, *pairs):
    def body(s, carry):
        cols = pl.ds(pl.multiple_of(s * seq, seq), seq)
        acc[:, cols] = jnp.zeros((acc.shape[0], seq), F32)
        for src, dst in pairs:
            dst[:, cols] = src[s].T
        return carry
    lax.fori_loop(0, seqs, body, 0)


def store_shards(peers, g_ref, j, g):
    rows = g_ref.shape[-2]
    for d in range(4):
        g_ref[0, j, peers.rel(d)] = g[d * rows:(d + 1) * rows]


def mlp_rest(slot, actions, peers, seqs, seq, w1, w2, dz, dy_ref, g_ref, w1t, yt, acc, gt, dht):
    points = seqs + 2
    first = slot * points

    def tick(i):
        at_ticks({k: v for k, v in actions.items() if k % points < seqs}, first + i)
    mlp_slot(seqs, seq, w1, w2, w1t, yt, dz, acc, gt, dht, tick)
    at_ticks(actions, first + seqs, seqs, points)
    store_shards(peers, g_ref, 0, dot(gt[...], dz[...], NT))
    at_ticks(actions, first + seqs + 1, seqs + 1, points)
    store_shards(peers, g_ref, 1, dot(yt[...], dht[...], NT))

    @pl.when(slot == SLOTS - 1)
    def _():
        with jax.named_scope('e00_dy_ref_dz_astype_F32_acc_astype_BF'):
            dy_ref[...] = (dz[...].astype(F32) + acc[...]).astype(BF16)


def attn_weights(layer, wq, wo, wa_g):
    nq, d = wq.shape[1:]
    return [(lambda: wq.at[layer], lambda j: wa_g.at[j, pl.ds(0, nq)], nq), (lambda: wo.at[layer], lambda j: wa_g.at[j, pl.ds(nq, d - nq)], d - nq)]


class Spread:
    def __init__(self, sems, peers, wb, pieces):
        rows = wb.shape[2] // pieces
        y = peers.y

        def piece(slot, m, k):
            return lambda: wb.at[slot, m, pl.ds(k * rows, rows)]
        every = range(pieces)
        self.sib = sems.remote(lambda: wb.at[0], lambda: wb.at[1], peers.sib)
        self.xp = [sems.remote(piece(0, y, k), piece(2, y, k), peers.xp) for k in every]
        self.fy, self.wy = [], []
        for k in every:
            self.fy.append(sems.remote(piece(2, y, k), piece(2, y, k), peers.yp))
            sems.n -= 1
            self.wy.append(sems.remote(piece(2, 1 - y, k), piece(2, 1 - y, k), peers.yp))
        self.fs = [sems.remote(piece(2, y, k), piece(3, y, k), peers.sib) for k in every]
        self.fs2 = [sems.remote(piece(2, 1 - y, k), piece(3, 1 - y, k), peers.sib) for k in every]

    def start(self):
        for c in self.xp + [self.sib]:
            c().start()

    def forward(self, k):
        self.xp[k]().wait_recv()
        self.fy[k]().start()
        self.fs[k]().start()

    def forward2(self, k):
        self.wy[k]().wait_recv()
        self.fs2[k]().start()

    def arrived(self):
        for c in self.fs + self.fs2:
            c().wait_recv()

    def finish(self):
        for c in [self.sib] + self.xp + self.fy + self.fs + self.fs2:
            c().wait_send()


def mlp_first_kernel(layer, y_ref, dz_ref, wup, wdn, wq, wo, dy_ref, g_ref, wa_g, yt, dzt, acc, w1t, gt, dht, wb, bounce, *rest):
    slot = pl.program_id(0)
    seqs, seq = y_ref.shape[1:3]
    peers, sems = Peers(), Sems(*rest)
    own = [sems.copy(lambda w=w: w.at[layer], lambda m=m: wb.at[0, m]) for m, w in enumerate((wup, wdn))]
    blocks = attn_weights(layer, wq, wo, wa_g)
    gather = Gather(sems, peers, [r[:2] for r in blocks])
    hop = Bounce(sems, blocks, bounce)
    spread = Spread(sems, peers, wb, SLOTS)

    @pl.when(slot == 0)
    def _():
        with jax.named_scope('e00_for_c_in_own__c_start_'):
            for c in own:
                c().start()
        with jax.named_scope('e01_peers_barrier_'):
            peers.barrier()
        with jax.named_scope('e02_for_c_in_own__c_wait_'):
            for c in own:
                c().wait()
        with jax.named_scope('e03_spread_start_'):
            spread.start()
        with jax.named_scope('e04_gather_start_range_2_'):
            gather.start(range(2))
        with jax.named_scope('e05_prepare_seqs_seq_acc_y_ref_at_0_yt'):
            prepare(seqs, seq, acc, (y_ref.at[0], yt), (dz_ref, dzt))

    @pl.when(slot == 1)
    def _():
        with jax.named_scope('e00_spread_sib_wait_recv_'):
            spread.sib().wait_recv()

    @pl.when(slot == 2)
    def _():
        with jax.named_scope('e00_spread_forward2_2_'):
            spread.forward2(2)
        with jax.named_scope('e01_spread_forward2_3_'):
            spread.forward2(3)

    @pl.when(slot == 3)
    def _():
        with jax.named_scope('e00_spread_arrived_'):
            spread.arrived()
    every = range(SLOTS)
    actions = merge([(14 + k, s) for k, s in enumerate(hop.steps)], ticks('4,6,8,10', [functools.partial(spread.forward, k) for k in every]),
                    ticks('7,11', [functools.partial(spread.forward2, k) for k in every]), ticks('21', gather.forwards()))
    mlp_rest(slot, actions, peers, seqs, seq, wb.at[slot, 0], wb.at[slot, 1], dzt, dy_ref, g_ref, w1t, yt, acc, gt, dht)

    @pl.when(slot == SLOTS - 1)
    def _():
        with jax.named_scope('e00_gather_forward_1_'):
            gather.forward(1)
        with jax.named_scope('e01_spread_finish_'):
            spread.finish()
        with jax.named_scope('e02_gather_finish_'):
            gather.finish()


def mlp_first(layer, y, dz, wup, wdn, wq, wo):
    d, f = wup.shape[1:]
    seq = y.shape[2]
    seqs = y.shape[1] // SLOTS
    tok = seqs * seq
    once = pl.Buffered(1)
    return pl.pallas_call(
        functools.partial(mlp_first_kernel, layer),
        out_shape=(jax.ShapeDtypeStruct((d, tok), BF16), jax.ShapeDtypeStruct((SLOTS, 2, 4, d // 4, f), F32), jax.ShapeDtypeStruct((SLOTS, d, d), BF16)),
        grid=(SLOTS,),
        in_specs=[pl.BlockSpec((1, seqs, seq, d), lambda j: (layer, lax.axis_index('tp'), 0, 0), pipeline_mode=once),
                  pl.BlockSpec((seqs, seq, d), lambda j: (lax.axis_index('tp'), 0, 0), pipeline_mode=once), ANY, ANY, ANY, ANY],
        out_specs=[whole(d, tok), leading(2, 4, d // 4, f), ANY],
        scratch_shapes=[pltpu.VMEM((d, tok), BF16), pltpu.VMEM((d, tok), BF16), pltpu.VMEM((d, tok), F32), pltpu.VMEM((f, d), BF16),
                        pltpu.VMEM((f, tok), BF16), pltpu.VMEM((f, tok), BF16), pltpu.VMEM((SLOTS, 2, d, f), BF16), pltpu.VMEM((d, d), BF16)] + SEMS,
        compiler_params=params(0, 1),
        name='mlp_first',
    )(y, dz, wup, wdn, wq, wo)


def mlp_second_kernel(layer, y_ref, dz_ref, w1_ref, w2_ref, partial, half, wq, wo, dy_ref, g_ref, wa_g, red, red_half, yt, acc, w1t, gt, dht, bounce, mine, *rest):
    slot = pl.program_id(0)
    seqs, seq = y_ref.shape[1:3]
    bufs, rest = rest[:4], rest[4:]
    peers, sems = Peers(), Sems(*rest[2:])
    blocks = attn_weights(layer, wq, wo, wa_g)
    gather = Gather(sems, peers, [r[:2] for r in blocks])
    hop = Bounce(sems, blocks, bounce)
    rows = mine.shape[2] // 2
    a, b = jobs = [Scatter(sems, peers, lambda s: partial.at[s], lambda x: mine.at[x], bufs, lambda j=j: red.at[pl.ds(j * rows, rows)], (j * rows, rows)) for j in range(2)]

    h0, h1 = rest[:2]
    mine_half = sems.copy(lambda: half.at[0], lambda: h0)
    x_half = sems.remote(lambda: half.at[1], lambda: h1, peers.xp)
    store_half = sems.copy(lambda: h0, lambda: red_half)

    def add_half():
        mine_half().wait()
        x_half().wait_recv()
        h0[...] = (h0[...] + h1[...]) * (1 / SLOTS)

    @pl.when(slot == 0)
    def _():
        with jax.named_scope('e00_peers_barrier_'):
            peers.barrier()
        with jax.named_scope('e01_jobs__job_both_start_'):
            for job in jobs:
                job.both('start')
        with jax.named_scope('e02_x_half_start_'):
            x_half().start()
        with jax.named_scope('e03_mine_half_start_'):
            mine_half().start()
        with jax.named_scope('e04_gather_start_range_2_'):
            gather.start(range(2))
        with jax.named_scope('e05_prepare_seqs_seq_acc_y_ref_at_0_yt'):
            prepare(seqs, seq, acc, (y_ref.at[0], yt))
    actions = merge([(4 + k, s) for k, s in enumerate(hop.steps)], ticks('17,22,12,13', gather.forwards() + [add_half, lambda: store_half().start()]),
                    steps(a, '3add0,4send1,10add1,11send2,17add2,18send3,22add3,23out'),
                    steps(b, '4add0,5send1,15add1,16send2,20add2,21send3'))
    mlp_rest(slot, actions, peers, seqs, seq, w1_ref.at[0], w2_ref.at[0], dz_ref, dy_ref, g_ref, w1t, yt, acc, gt, dht)

    @pl.when(slot == SLOTS - 1)
    def _():
        with jax.named_scope('e00_b_add3_'):
            b.add3()
        with jax.named_scope('e01_gather_finish_'):
            gather.finish()
        with jax.named_scope('e02_x_half_wait_send_'):
            x_half().wait_send()
        with jax.named_scope('e03_store_half_wait_'):
            store_half().wait()
        with jax.named_scope('e04_b_out_'):
            b.out()
        with jax.named_scope('e05_a_finish_'):
            a.finish()
        with jax.named_scope('e06_b_finish_'):
            b.finish()


def mlp_second(layer, y, dz, w1, w2, partial, half, wq, wo):
    d, f = w1.shape[1:]
    seq = y.shape[2]
    seqs = y.shape[1] // SLOTS
    tok = seqs * seq
    return pl.pallas_call(
        functools.partial(mlp_second_kernel, layer),
        out_shape=(jax.ShapeDtypeStruct((d, tok), BF16), jax.ShapeDtypeStruct((SLOTS, 2, 4, d // 4, f), F32), jax.ShapeDtypeStruct((SLOTS, d, d), BF16),
                   jax.ShapeDtypeStruct((d // 4, d), F32), jax.ShapeDtypeStruct(half.shape[1:], F32)),
        grid=(SLOTS,),
        in_specs=[pl.BlockSpec((1, seqs, seq, d), lambda j: (layer, lax.axis_index('tp'), 0, 0), pipeline_mode=pl.Buffered(1)),
                  whole(d, tok), leading(d, f), leading(f, d)] + [ANY] * 4,
        out_specs=[whole(d, tok), leading(2, 4, d // 4, f)] + [ANY] * 3,
        scratch_shapes=[pltpu.VMEM((d, tok), BF16), pltpu.VMEM((d, tok), F32), pltpu.VMEM((f, d), BF16),
                        pltpu.VMEM((f, tok), BF16), pltpu.VMEM((f, tok), BF16), pltpu.VMEM((d, d), BF16), pltpu.VMEM((2, 4, d // 4, d), F32)]
        + scatter_bufs(d // 4, d) + [pltpu.VMEM(half.shape[1:], F32)] * 2 + SEMS,
        compiler_params=params(1, 1),
        name='mlp_second',
    )(y, dz, w1, w2, partial, half, wq, wo)


def attn_step(peers, x_ref, dy_ref, w_ref, xt, acc, gacc, qkv, do, b1, b2, emit):
    s, slot = pl.program_id(0), pl.program_id(1)
    step = s * SLOTS + slot
    last = SLOTS * SLOTS - 1
    before = (step + last) % (last + 1)
    seq, d = x_ref.shape[-2:]
    nqkv = qkv.shape[0]
    third = nqkv // 3
    split = d - b2.shape[1]
    rows = d // 4

    def tokens(n):
        return pl.ds(pl.multiple_of(n * seq, seq), seq)

    @pl.when(step == 0)
    def _():
        xt[1] = jnp.zeros((d, seq), BF16)

        def clear(j, carry):
            gacc[j // 4, j % 4] = jnp.zeros(gacc.shape[2:], F32)
            b1[j % 2] = jnp.zeros(b1.shape[1:], BF16)
            b2[j % 2] = jnp.zeros(b2.shape[1:], BF16)
            return carry
        lax.fori_loop(0, SLOTS * 4, clear, 0)

    @pl.when(slot == 0)
    def _():
        with jax.named_scope('e00_xt_s_2_x_ref_0_0_T'):
            xt[s % 2] = x_ref[0, 0].T

    def grads(n):
        ps, pj, par = n // SLOTS, n % SLOTS, n % 2
        third_d = d // 3

        def weights(c):
            cols = slice(c * third_d, (c + 1) * third_d)
            g = dot(xt[ps % 2], b1[par, cols], NT)
            if c == 2:
                g = g + dot(dy_ref[:, tokens(ps)], b2[par], NT)
            for k in range(4):
                r = peers.rel(k)
                gacc[pj, r, :, cols] = gacc[pj, r, :, cols] + g[k * rows:(k + 1) * rows]

        def inputs(c):
            part = slice(c * third_d, (c + 1) * third_d)
            acc[part] += dot(w_ref[pj, :, part].T, b1[par], NN)
        return [functools.partial(f, c) for c in range(3) for f in (weights, inputs)]
    with jax.named_scope("main"):
        x_t = xt[s % 2]
        dy_t = dy_ref[:, tokens(s)]
        now = step % 2
        qkv[...] = dot(w_ref[slot, pl.ds(0, nqkv), :], x_t, NN).astype(BF16)
        do[...] = dot(w_ref[slot, pl.ds(nqkv, d - nqkv), :], dy_t, NN).astype(BF16)
        scale = HEAD ** -0.5
        exp_scale = scale * math.log2(math.e)
        qb = seq // 2
        units = [(h, slice(c * qb, (c + 1) * qb)) for h in range(third // HEAD) for c in range(2)]

        def scores(h, qc):
            q_rows, k_rows, v_rows = head_rows(h)
            return dot(qkv[k_rows, :].T, qkv[q_rows, qc], NN), dot(qkv[v_rows, :].T, do[q_rows, qc] * scale, NN)

        def head_rows(h):
            return [slice(i * third + h * HEAD, i * third + (h + 1) * HEAD) for i in range(3)]
        for piece in grads(before):
            piece()
        ahead = [scores(*unit) for unit in units[:LOOK_AHEAD]]
        for n, (h, qc) in enumerate(units):
            sc, dp_t = ahead.pop(0)
            if n + LOOK_AHEAD < len(units):
                ahead.append(scores(*units[n + LOOK_AHEAD]))
            q_rows, k_rows, v_rows = head_rows(h)
            m = jnp.max(sc, axis=0, keepdims=True)
            e = jnp.exp2((sc - m) * exp_scale)
            inv = 1.0 / jnp.sum(e, axis=0, keepdims=True)
            rd = jnp.sum(e * dp_t, axis=0, keepdims=True) * inv
            p = e * inv
            p_bf = p.astype(BF16)
            ds = (p * (dp_t - rd)).astype(BF16)
            b2[now, pl.ds(b2.shape[1] - third + h * HEAD, HEAD), qc] = dot(qkv[v_rows, :], p_bf, NN).astype(BF16)
            b1[now, q_rows, qc] = dot(qkv[k_rows, :], ds, NN).astype(BF16)
            dv_c = dot(do[q_rows, qc], p_bf, NT)
            dk_c = dot(qkv[q_rows, qc], ds, NT)
            if n % 2 == 0:
                dv, dk = dv_c, dk_c
            else:
                b1[now, k_rows] = (dk + dk_c).astype(BF16)
                b1[now, v_rows] = (dv + dv_c).astype(BF16)

    @pl.when(slot == 0)
    def _():
        @pl.when(s > 0)
        def _():
            emit(s - 1)
        acc[...] = dy_ref[:, tokens(s)].astype(F32)

    @pl.when(step == last)
    def _():
        with jax.named_scope('e00_for_piece_in_grads_last__piece_'):
            for piece in grads(last):
                piece()
        with jax.named_scope('e01_emit_s_'):
            emit(s)


ATTN_IN = 3
ATTN_SCRATCH = 7
JOB_PLAN = '1add0,2send1,7add1,8send2,12add2', '2add0,3send1x,8send1y,10add1x,11send2x,14add1y,15send2y'


def attn_first_kernel(layer, x_ref, dy_ref, w_ref, partial, wup, wdn, dx_ref, g_hbm, w1_g, w2_g, half, *rest):
    body, rest = rest[:ATTN_SCRATCH], rest[ATTN_SCRATCH:]
    gacc, mine, bounce = body[2], rest[:2], rest[-4]
    seq = x_ref.shape[-2]
    step = pl.program_id(0) * SLOTS + pl.program_id(1)
    peers, sems = Peers(), Sems(*rest[-3:])
    a, b = jobs = [Scatter(sems, peers, lambda s, j=j: partial.at[s, j], lambda x, j=j: mine[j].at[x], rest[2 + 4 * j:6 + 4 * j], None,
                           (0, half.shape[2]), half_out=lambda x, j=j: half.at[x, j]) for j in range(2)]
    blocks = [(lambda w=w: w.at[layer - 1], lambda j, g=g: g.at[j], wup.shape[1]) for w, g in ((wup, w1_g), (wdn, w2_g))]
    gather = Gather(sems, peers, [r[:2] for r in blocks])
    hop = Bounce(sems, blocks, bounce)
    stores = [sems.copy(lambda j=j: gacc.at[j], lambda j=j: g_hbm.at[j]) for j in range(SLOTS)]
    actions = merge(steps(a, JOB_PLAN[0]), steps(b, JOB_PLAN[1]), [(5 + k, s) for k, s in enumerate(hop.steps)],
                    ticks('7,13', gather.forwards()))

    @pl.when(step == 0)
    def _():
        peers.barrier()
        for job in jobs:
            job.both('start')
        gather.start(range(2))
    at_ticks(actions, step)

    def emit(s):
        dx_ref[:, pl.ds(pl.multiple_of(s * seq, seq), seq)] = acc[...].astype(BF16)
    acc = body[1]
    attn_step(peers, x_ref, dy_ref, w_ref, *body, emit)

    @pl.when(step == SLOTS * SLOTS - 1)
    def _():
        with jax.named_scope('e00_a_out_'):
            a.out()
        with jax.named_scope('e01_for_c_in_stores__c_start_'):
            for c in stores:
                c().start()
        with jax.named_scope('e02_b_both_add2_'):
            b.both('add2')
        with jax.named_scope('e03_gather_finish_'):
            gather.finish()
        with jax.named_scope('e04_for_c_in_stores__c_wait_'):
            for c in stores:
                c().wait()
        with jax.named_scope('e05_b_out_'):
            b.out()
        with jax.named_scope('e06_jobs__job_finish_'):
            for job in jobs:
                job.finish()


def attn_last_kernel(x_ref, dy_ref, w_ref, partial, dxg, red, red_last, *rest):
    body, rest = rest[:ATTN_SCRATCH], rest[ATTN_SCRATCH:]
    acc, gacc, mine, dxb, free = body[1], body[2], rest[:2], rest[-5], rest[-4]
    step = pl.program_id(0) * SLOTS + pl.program_id(1)
    seqs = pl.num_programs(0)
    peers, sems = Peers(), Sems(*rest[-3:])
    nred = red.shape[1]
    a, b = jobs = [Scatter(sems, peers, lambda s, j=j: partial.at[s, j], lambda x, j=j: mine[j].at[x], rest[2 + 4 * j:6 + 4 * j], lambda j=j: red.at[j],
                           (0, nred)) for j in range(2)]
    h = nred // 2
    ends = [Scatter(sems, peers, lambda s: gacc.at[s], lambda x: gacc.at[2 * x], rest[2:6], lambda j=j: red_last.at[pl.ds(j * h, h)], (j * h, h), load=False)
            for j in range(2)]
    t = peers.t
    t2 = (t + 2) % SLOTS
    sib, xp, fwd, mine_dx = [], [], [], []
    for s in range(SLOTS):
        def src(s=s):
            return dxb.at[s]

        def dst(s=s):
            return dxg.at[t * SLOTS + s]

        def other(s=s):
            return dxg.at[t2 * SLOTS + s]
        mine_dx.append(sems.copy(src, dst))
        sib.append(sems.remote(src, dst, peers.sib))
        xp.append(sems.remote(src, dst, peers.xp))
        fwd.append(sems.remote(other, other, peers.sib))

    def freed(i):
        for peer in ([peers.sib], [peers.yp, peers.zp], [peers.yp, peers.zp], [peers.xp])[i]:
            pl.semaphore_signal(free.at[i], inc=1, device_id=peer, device_id_type=MESH)

    def forward(s):
        xp[s]().wait_recv()
        fwd[s]().start()

    def early():
        pl.semaphore_wait(free.at[0], 1)
        for job in ends:
            job.start(0)
    actions = merge(steps(a, JOB_PLAN[0]), steps(b, JOB_PLAN[1]), steps(a, '13send3'),
                    ticks('2,8,13,9,13,15', [functools.partial(freed, i) for i in range(3)] + [functools.partial(forward, i) for i in range(2)] + [early]))

    @pl.when(step == 0)
    def _():
        peers.barrier()
        for job in jobs:
            job.both('start')
    at_ticks(actions, step)

    def emit(s):
        dxb[s] = acc[...].T.astype(BF16)
        for k in range(SLOTS):
            @pl.when(s == k)
            def _(k=k):
                for c in (xp, sib, mine_dx):
                    c[k]().start()
    attn_step(peers, x_ref, dy_ref, w_ref, *body, emit)

    @pl.when(step == SLOTS * SLOTS - 1)
    def _():
        with jax.named_scope('e00_ends__job_start_1__job_add0_0_'):
            for job in ends:
                job.start(1)
                job.add0(0)
        with jax.named_scope('e01_pl_semaphore_wait_free_at_1_2_'):
            pl.semaphore_wait(free.at[1], 2)
        with jax.named_scope('e02_ends__job_send1_0_'):
            for job in ends:
                job.send1(0)
        with jax.named_scope('e03_forward_2_'):
            forward(2)
        with jax.named_scope('e04_b_both_add2_'):
            b.both('add2')
        with jax.named_scope('e05_ends__job_add0_1_'):
            for job in ends:
                job.add0(1)
        with jax.named_scope('e06_b_send3_'):
            b.send3()
        with jax.named_scope('e07_ends__job_send1_1_'):
            for job in ends:
                job.send1(1)
        with jax.named_scope('e08_pl_semaphore_wait_free_at_2_2_'):
            pl.semaphore_wait(free.at[2], 2)
        with jax.named_scope('e09_ends__job_add1_0__job_send2_0_'):
            for job in ends:
                job.add1(0)
                job.send2(0)
        with jax.named_scope('e10_a_add3_'):
            a.add3()
        with jax.named_scope('e11_freed_3_'):
            freed(3)
        with jax.named_scope('e12_ends__job_add1_1__job_send2_1_'):
            for job in ends:
                job.add1(1)
                job.send2(1)
        with jax.named_scope('e13_forward_3_'):
            forward(3)
        with jax.named_scope('e14_a_out_'):
            a.out()
        with jax.named_scope('e15_b_add3_'):
            b.add3()
        with jax.named_scope('e16_b_out_'):
            b.out()
        with jax.named_scope('e17_pl_semaphore_wait_free_at_3_1_'):
            pl.semaphore_wait(free.at[3], 1)
        with jax.named_scope('e18_ends__job_both_add2__job_send3_'):
            for job in ends:
                job.both('add2')
                job.send3()
        with jax.named_scope('e19_for_s_in_range_SLOTS__mine_dx_s_wa'):
            for s in range(SLOTS):
                mine_dx[s]().wait()
                sib[s]().wait()
                xp[s]().wait_send()
        with jax.named_scope('e20_ends__job_add3__job_out_'):
            for job in ends:
                job.add3()
                job.out()
        with jax.named_scope('e21_for_s_in_range_SLOTS__fwd_s_wait_'):
            for s in range(SLOTS):
                fwd[s]().wait()
        with jax.named_scope('e22_jobs_ends__job_finish_'):
            for job in jobs + ends:
                job.finish()


def attn_specs(layer, x, w):
    slots, nw, d = w.shape
    seq = x.shape[2]
    seqs = x.shape[1] // slots
    tok = seqs * seq
    nqkv = nw * 3 // 4
    in_specs = [pl.BlockSpec((1, 1, seq, d), lambda s, j: (layer, lax.axis_index('tp') * seqs + s, 0, 0)), whole(d, tok), whole(slots, nw, d), ANY]
    scratch = [pltpu.VMEM((2, d, seq), BF16), pltpu.VMEM((d, seq), F32), pltpu.VMEM((slots, 4, d // 4, nw), F32), pltpu.VMEM((nqkv, seq), BF16),
               pltpu.VMEM((nw - nqkv, seq), BF16), pltpu.VMEM((2, nw, seq), BF16), pltpu.VMEM((2, d // 3, seq), BF16)]
    scratch += [pltpu.VMEM((2, 4, d // 4, d), F32)] * 2 + scatter_bufs(d // 4, d) * 2
    red = jax.ShapeDtypeStruct((2, d // 4, d), F32)
    return (slots, seqs), in_specs, scratch, red, tok


def attn_first(layer, x, dy, w, partial, wup, wdn):
    grid, in_specs, scratch, red, tok = attn_specs(layer, x, w)
    slots, nw, d = w.shape
    gathered = [jax.ShapeDtypeStruct((slots, d, d), BF16)] * 2
    return pl.pallas_call(
        functools.partial(attn_first_kernel, layer),
        out_shape=[jax.ShapeDtypeStruct((d, tok), BF16), jax.ShapeDtypeStruct((slots, 4, d // 4, nw), F32)] + gathered + [jax.ShapeDtypeStruct((2,) + red.shape, F32)],
        grid=grid,
        in_specs=in_specs + [ANY, ANY],
        out_specs=[whole(d, tok)] + [ANY] * 4,
        scratch_shapes=scratch + [pltpu.VMEM((d, d), BF16)] + SEMS,
        compiler_params=params(2, 2),
        name='attn_first',
    )(x, dy, w, partial, wup, wdn)


def attn_last(layer, x, dy, w, partial):
    grid, in_specs, scratch, red, tok = attn_specs(layer, x, w)
    slots, nw, d = w.shape
    seq = x.shape[2]
    return pl.pallas_call(
        attn_last_kernel,
        out_shape=[jax.ShapeDtypeStruct((x.shape[1], seq, d), BF16), red, jax.ShapeDtypeStruct(red.shape[1:], F32)],
        grid=grid,
        in_specs=in_specs,
        out_specs=[ANY] * 3,
        scratch_shapes=scratch + [pltpu.VMEM((slots, seq, d), BF16), pltpu.SemaphoreType.REGULAR((4,))] + SEMS,
        compiler_params=params(3, 2),
        name='attn_last',
    )(x, dy, w, partial)


def solution(mesh):
    assert dict(mesh.shape) == {'dpy': 2, 'dpx': 2, 'tp': SLOTS}
    act_spec = P(None, DATA_AXES, None, None)

    def device_backward(x_saved, y_saved, dz_top, w_qkv, w_out, w_up, w_down):
        layers, d = w_up.shape[:2]
        assert layers == 2
        heads, hd = w_out.shape[1:3]
        n = 3 * heads * hd
        wq = w_qkv.transpose(0, 2, 3, 4, 1).reshape(layers, n, d)
        wo = w_out.reshape(layers, heads * hd, d)
        dy1, gm1, wa1 = mlp_first(1, y_saved, dz_top, w_up, w_down, wq, wo)
        dx1, ga1, w1_0, w2_0, half = attn_first(1, x_saved, dy1, wa1, gm1, w_up, w_down)
        dy0, gm0, wa0, ra1, rm1 = mlp_second(0, y_saved, dx1, w1_0, w2_0, ga1, half, wq, wo)
        d_input, rm0, ra0 = attn_last(0, x_saved, dy0, wa0, gm0)
        g_a = jnp.stack([ra0, ra1])
        g_qkv = g_a[:, :, :n].reshape(layers, d // 4, 3, heads, hd)
        g_out = g_a[:, :, n:].transpose(0, 2, 1).reshape(layers, heads, hd, d // 4)
        return d_input, g_qkv, g_out, jnp.stack([rm0[1], rm1[1]]), jnp.stack([rm0[0], rm1[0]])

    tp_last = P(None, None, None, 'tp', None), P(None, 'tp', None, None), P(None, None, 'tp'), P(None, 'tp', None)
    return jax.shard_map(device_backward, mesh=mesh,
                         in_specs=(act_spec, act_spec, P(DATA_AXES, None, None)) + tp_last,
                         out_specs=(P(DATA_AXES, None, None), P(None, DATA_AXES, None, 'tp', None), P(None, 'tp', None, DATA_AXES), P(None, DATA_AXES, 'tp'), P(None, ('tp', 'dpy', 'dpx'), None)),
                         check_vma=False)
```

```python
import functools
import math
import re

import jax
import jax.numpy as jnp
from jax import lax
from jax.experimental import pallas as pl
from jax.experimental.pallas import tpu as pltpu
from jax.sharding import PartitionSpec as P

DATA_AXES = ('dpy', 'dpx')
F32 = jnp.float32
BF16 = jnp.bfloat16
HEAD = 64
SLOTS = 4
LOOK_AHEAD = 3
NN = (((1,), (0,)), ((), ()))
NT = (((1,), (1,)), ((), ()))
VMEM_LIMIT = 63 * 1024 * 1024
MESH = pl.DeviceIdType.MESH
ANY = pl.BlockSpec(memory_space=pl.ANY)


def dot(a, b, dims):
    return lax.dot_general(a, b, dims, preferred_element_type=F32)


class Peers:
    def __init__(self):
        z, y, t = lax.axis_index('dpy'), lax.axis_index('dpx'), lax.axis_index('tp')
        self.z, self.y, self.t = z, y, t
        self.sib = (z, y, t + 1 - 2 * (t % 2))
        self.xp = (z, y, (t + 2) % 4)
        self.yp = (z, 1 - y, t)
        self.zp = (1 - z, y, t)

    def barrier(self):
        sem = pltpu.get_barrier_semaphore()
        with jax.named_scope('entry'):
            for peer in (self.sib, self.xp, self.yp, self.zp):
                pl.semaphore_signal(sem, inc=1, device_id=peer, device_id_type=MESH)
            pl.semaphore_wait(sem, 4)

    def rel(self, d):
        zr = self.z if d // 2 == 0 else 1 - self.z
        yr = self.y if d % 2 == 0 else 1 - self.y
        return zr * 2 + yr


class Sems:
    def __init__(self, send, recv, local):
        self.send, self.recv, self.local = send, recv, local
        self.n = self.m = 0

    def remote(self, src, dst, peer):
        i = self.n
        self.n += 1
        return lambda: pltpu.make_async_remote_copy(src_ref=src(), dst_ref=dst(), send_sem=self.send.at[i], recv_sem=self.recv.at[i],
                                                    device_id=peer, device_id_type=MESH)

    def copy(self, src, dst):
        i = self.m
        self.m += 1
        return lambda: pltpu.make_async_copy(src(), dst(), self.local.at[i])

    def copies(self, n, src, dst):
        first = self.m
        self.m += n
        return lambda i: pltpu.make_async_copy(src(i), dst(i), self.local.at[first + i])


def at_ticks(actions, tick, position=0, points=1):
    for k in sorted(actions):
        if k % points == position:
            @pl.when(tick == k)
            def _(k=k):
                with jax.named_scope('t%d' % k):
                    for action in actions[k]:
                        action()


class Scatter:
    def __init__(self, sems, peers, partial, mine, bufs, out, rows, load=True, half_out=None):
        r0, r1, r2, r3 = self.bufs = bufs
        first, count = rows
        h = count // 2
        self.mine, self.all, self.lo, self.hi = mine, pl.ds(first, count), pl.ds(first, h), pl.ds(first + h, h)
        self.half = half = pl.ds(first // 2, h)
        every, lo, hi = self.all, self.lo, self.hi
        self.load, self.c0, self.c1, self.c2 = [], [], [], []
        for x in range(2):
            def near(k, part, x=x):
                return lambda: mine(x).at[k, part]

            def place(buf, *index):
                return lambda: buf.at[index]
            if load:
                self.load.append(sems.copy(lambda x=x: partial(2 * x).at[:, every], near(slice(None), every)))
            self.c0.append(sems.remote(lambda x=x: partial(2 * x + 1).at[:, every], place(r0, x, slice(None), every), peers.sib))
            self.c1.append([sems.remote(near(2 * k + 1, lo), place(r1, 0, x, k, half), peers.yp) for k in range(2)]
                           + [sems.remote(near(2 + k, hi), place(r1, 1, x, k, half), peers.zp) for k in range(2)])
            self.c2.append([sems.remote(near(2, lo), place(r2, 0, x, half), peers.zp), sems.remote(near(1, hi), place(r2, 1, x, half), peers.yp)])
        if half_out is None:
            self.c3 = sems.remote(lambda: mine(1).at[0, every], place(r3, every), peers.xp)
            self.store = [sems.copy(lambda: mine(0).at[0, every], out)]
        else:
            self.c3 = None
            self.store = [sems.copy(lambda x=x: mine(x).at[0, every], lambda x=x: half_out(x)) for x in range(2)]

    def start(self, x):
        self.c0[x]().start()
        if self.load:
            self.load[x]().start()

    def add0(self, x):
        if self.load:
            self.load[x]().wait()
        self.c0[x]().wait_recv()
        mine, r0 = self.mine(x), self.bufs[0].at[x]

        def body(k, carry):
            mine[k, self.all] = mine[k, self.all] + r0[k, self.all]
            return carry
        lax.fori_loop(0, 4, body, 0)

    def send1(self, x):
        for c in self.c1[x]:
            c().start()

    def add1(self, x):
        for c in self.c1[x]:
            c().wait_recv()
        mine, r1 = self.mine(x), self.bufs[1]

        def body(k, carry):
            mine[2 * k, self.lo] = mine[2 * k, self.lo] + r1[0, x, k, self.half]
            mine[k, self.hi] = mine[k, self.hi] + r1[1, x, k, self.half]
            return carry
        lax.fori_loop(0, 2, body, 0)

    def send2(self, x):
        for c in self.c2[x]:
            c().start()

    def add2(self, x):
        for c in self.c2[x]:
            c().wait_recv()
        mine, r2 = self.mine(x), self.bufs[2]
        mine[0, self.lo] = mine[0, self.lo] + r2[0, x, self.half]
        mine[0, self.hi] = mine[0, self.hi] + r2[1, x, self.half]

    def send3(self):
        self.c3().start()

    def add3(self):
        self.c3().wait_recv()
        mine = self.mine(0)
        mine[0, self.all] = (mine[0, self.all] + self.bufs[3][self.all]) * (1 / SLOTS)

    def out(self):
        for c in self.store:
            c().start()

    def finish(self):
        for c in self.c0 + sum(self.c1, []) + sum(self.c2, []) + ([self.c3] if self.c3 else []):
            c().wait_send()
        for c in self.store:
            c().wait()

    def both(self, name):
        for x in range(2):
            getattr(self, name)(x)


def scatter_bufs(rows, d):
    return [pltpu.VMEM((2, 4, rows, d), F32), pltpu.VMEM((2, 2, 2, rows // 2, d), F32), pltpu.VMEM((2, 2, rows // 2, d), F32), pltpu.VMEM((rows, d), F32)]


def steps(job, plan):
    out = []
    for tick, name, half in re.findall('([0-9]+)([a-z]+[0-3]?)([xy]?)', plan):
        if half:
            action = functools.partial(getattr(job, name), int(half == 'y'))
        else:
            action = functools.partial(job.both, name) if name[-1] in '012' else getattr(job, name)
        out.append((int(tick), action))
    return out


def ticks(plan, actions):
    return list(zip(map(int, plan.split(',')), actions))


class Gather:
    def __init__(self, sems, peers, blocks):
        self.sib = [sems.remote(own, lambda dst=dst: dst(1), peers.sib) for own, dst in blocks]
        self.xp = [sems.remote(own, lambda dst=dst: dst(2), peers.xp) for own, dst in blocks]
        self.fwd = [sems.remote(lambda dst=dst: dst(2), lambda dst=dst: dst(3), peers.sib) for own, dst in blocks]

    def start(self, blocks):
        for i in blocks:
            self.sib[i]().start()
            self.xp[i]().start()

    def forward(self, i):
        self.xp[i]().wait_recv()
        self.fwd[i]().start()

    def forwards(self):
        return [functools.partial(self.forward, i) for i in range(len(self.fwd))]

    def finish(self):
        for i in range(len(self.sib)):
            self.sib[i]().wait_recv()
            self.fwd[i]().wait_recv()
            self.sib[i]().wait_send()
            self.xp[i]().wait_send()
            self.fwd[i]().wait_send()


class Bounce:
    def __init__(self, sems, items, buf):
        self.steps = []
        prev = None
        for own, dst, rows in items:
            ld = sems.copy(own, lambda rows=rows: buf.at[pl.ds(0, rows)])
            st = sems.copy(lambda rows=rows: buf.at[pl.ds(0, rows)], lambda dst=dst: dst(0))
            self.steps.append(functools.partial(self.load, prev, ld))
            self.steps.append(functools.partial(self.flip, ld, st))
            prev = st
        self.steps.append(lambda prev=prev: prev().wait())

    @staticmethod
    def load(prev, ld):
        if prev is not None:
            prev().wait()
        ld().start()

    @staticmethod
    def flip(ld, st):
        ld().wait()
        st().start()


def merge(*lists):
    actions = {}
    for pairs in lists:
        for k, action in pairs:
            actions.setdefault(k, []).append(action)
    return actions


SEMS = [pltpu.SemaphoreType.DMA((96,)), pltpu.SemaphoreType.DMA((96,)), pltpu.SemaphoreType.DMA((32,))]


def leading(*shape):
    return pl.BlockSpec((1,) + shape, lambda j, *_: (j,) + (0,) * len(shape))


def params(collective_id, axes):
    return pltpu.CompilerParams(vmem_limit_bytes=VMEM_LIMIT, dimension_semantics=('arbitrary',) * axes, collective_id=collective_id, has_side_effects=True)


def mlp_slot(slot, seqs, seq, w1, w2, w1t, yt, dz, acc, gt, dht, tick, arrive, emit):
    w1t[...] = w1[...].T

    def block(i, carry):
        tick(i)
        with jax.named_scope('arrive'):
            pl.when(slot == 0)(lambda: arrive(i))
        cols = pl.ds(pl.multiple_of(i * seq, seq), seq)
        h = dot(w1t[...], yt[:, cols], NN)
        dg = dot(w2[...], dz[:, cols], NN)
        c0 = math.sqrt(2 / math.pi)
        c1 = 0.044715 * c0
        h2 = h * h
        t = jnp.tanh(h * (c0 + c1 * h2))
        q = 0.5 * t + 0.5
        g = h * q
        dh = dg * (q + (g * (1.0 - t)) * (c0 + (3 * c1) * h2))
        gt[:, cols] = g.astype(BF16)
        dh = dh.astype(BF16)
        dht[:, cols] = dh
        acc[:, cols] += dot(w1[...], dh, NN)
        with jax.named_scope('memit'):
            pl.when(slot == SLOTS - 1)(lambda: emit(i))
        return carry
    lax.fori_loop(0, seqs, block, 0)


def tokens(i, seq):
    return pl.ds(pl.multiple_of(i * seq, seq), seq)


class MlpIo:
    def __init__(self, sems, peers, seqs, seq, loads, acc, dz, dyb, dy_hbm, gbuf, g_hbm):
        self.seqs, self.seq, self.peers = seqs, seq, peers
        self.loads, self.acc, self.dz, self.dyb, self.gbuf = loads, acc, dz, dyb, gbuf
        self.dy = sems.copies(seqs, lambda i: dyb.at[:, tokens(i, seq)], lambda i: dy_hbm.at[:, tokens(i, seq)])
        self.g = [sems.copy(lambda j=j: gbuf.at[j], lambda j=j: g_hbm.at[pl.program_id(0), j]) for j in range(2)]

    def start(self):
        for load, _ in self.loads:
            for i in range(self.seqs):
                load(i).start()

    def arrive(self, i):
        for load, use in self.loads:
            load(i).wait()
            use(i)
        cols = tokens(i, self.seq)
        self.acc[:, cols] = jnp.zeros((self.acc.shape[0], self.seq), F32)

    def emit(self, i):
        cols = tokens(i, self.seq)
        self.dyb[:, cols] = (self.dz[:, cols].astype(F32) + self.acc[:, cols]).astype(BF16)
        self.dy(i).start()

    def put(self, j, g):
        pl.when(pl.program_id(0) > 0)(lambda: self.g[j]().wait())
        rows = self.gbuf.shape[-2]
        for k in range(4):
            self.gbuf[j, self.peers.rel(k)] = g[k * rows:(k + 1) * rows]
        self.g[j]().start()

    def finish(self):
        for i in range(self.seqs):
            self.dy(i).wait()
        for c in self.g:
            c().wait()


def mlp_rest(slot, actions, io, w1, w2, w1t, yt, gt, dht):
    seqs, seq, dz, acc = io.seqs, io.seq, io.dz, io.acc
    points = seqs + 2
    first = slot * points

    def tick(i):
        at_ticks({k: v for k, v in actions.items() if k % points < seqs}, first + i)
    mlp_slot(slot, seqs, seq, w1, w2, w1t, yt, dz, acc, gt, dht, tick, io.arrive, io.emit)
    at_ticks(actions, first + seqs, seqs, points)
    with jax.named_scope('dw2'):
        io.put(0, dot(gt[...], dz[...], NT))
    at_ticks(actions, first + seqs + 1, seqs + 1, points)
    with jax.named_scope('dw1'):
        io.put(1, dot(yt[...], dht[...], NT))


def attn_weights(layer, wq, wo, wa_g):
    nq, d = wq.shape[1:]
    return [(lambda: wq.at[layer], lambda j: wa_g.at[j, pl.ds(0, nq)], nq), (lambda: wo.at[layer], lambda j: wa_g.at[j, pl.ds(nq, d - nq)], d - nq)]


class Spread:
    def __init__(self, sems, peers, wb, pieces):
        rows = wb.shape[2] // pieces
        y = peers.y

        def piece(slot, m, k):
            return lambda: wb.at[slot, m, pl.ds(k * rows, rows)]
        every = range(pieces)
        self.sib = sems.remote(lambda: wb.at[0], lambda: wb.at[1], peers.sib)
        self.xp = [sems.remote(piece(0, y, k), piece(2, y, k), peers.xp) for k in every]
        self.fy, self.wy = [], []
        for k in every:
            self.fy.append(sems.remote(piece(2, y, k), piece(2, y, k), peers.yp))
            sems.n -= 1
            self.wy.append(sems.remote(piece(2, 1 - y, k), piece(2, 1 - y, k), peers.yp))
        self.fs = [sems.remote(piece(2, y, k), piece(3, y, k), peers.sib) for k in every]
        self.fs2 = [sems.remote(piece(2, 1 - y, k), piece(3, 1 - y, k), peers.sib) for k in every]

    def start(self):
        for c in self.xp + [self.sib]:
            c().start()

    def forward(self, k):
        self.xp[k]().wait_recv()
        self.fy[k]().start()
        self.fs[k]().start()

    def forward2(self, k):
        self.wy[k]().wait_recv()
        self.fs2[k]().start()

    def arrived(self):
        for c in self.fs + self.fs2:
            c().wait_recv()

    def finish(self):
        for c in [self.sib] + self.xp + self.fy + self.fs + self.fs2:
            c().wait_send()


def turned(src, dst, seq):
    def use(i):
        dst[:, tokens(i, seq)] = src[i].T
    return use


def mlp_first_kernel(layer, y, dz_in, wup, wdn, wq, wo, dy_hbm, g_hbm, wa_g, yb, dzb, yt, dzt, acc, w1t, gt, dht, wb, bounce, dyb, gbuf, *rest):
    slot = pl.program_id(0)
    seqs, seq = yb.shape[:2]
    peers, sems = Peers(), Sems(*rest)
    mine = peers.t * seqs
    loads = [(sems.copies(seqs, lambda i: y.at[layer, mine + i], lambda i: yb.at[i]), turned(yb, yt, seq)),
             (sems.copies(seqs, lambda i: dz_in.at[mine + i], lambda i: dzb.at[i]), turned(dzb, dzt, seq))]
    io = MlpIo(sems, peers, seqs, seq, loads, acc, dzt, dyb, dy_hbm, gbuf, g_hbm)
    own = [sems.copy(lambda w=w: w.at[layer], lambda m=m: wb.at[0, m]) for m, w in enumerate((wup, wdn))]
    blocks = attn_weights(layer, wq, wo, wa_g)
    gather = Gather(sems, peers, [r[:2] for r in blocks])
    hop = Bounce(sems, blocks, bounce)
    spread = Spread(sems, peers, wb, SLOTS)

    @pl.when(slot == 0)
    def _():
        with jax.named_scope('e00_for_c_in_own__c_start_'):
            for c in own:
                c().start()
        with jax.named_scope('e01_io_start_'):
            io.start()
        with jax.named_scope('e02_peers_barrier_'):
            peers.barrier()
        with jax.named_scope('e03_for_c_in_own__c_wait_'):
            for c in own:
                c().wait()
        with jax.named_scope('e04_spread_start_'):
            spread.start()
        with jax.named_scope('e05_gather_start_range_2_'):
            gather.start(range(2))

    @pl.when(slot == 1)
    def _():
        with jax.named_scope('e00_spread_sib_wait_recv_'):
            spread.sib().wait_recv()

    @pl.when(slot == 2)
    def _():
        with jax.named_scope('e00_spread_forward2_2_'):
            spread.forward2(2)
        with jax.named_scope('e01_spread_forward2_3_'):
            spread.forward2(3)

    @pl.when(slot == 3)
    def _():
        with jax.named_scope('e00_spread_arrived_'):
            spread.arrived()
    every = range(SLOTS)
    actions = merge([(14 + k, s) for k, s in enumerate(hop.steps)], ticks('4,5,8,10', [functools.partial(spread.forward, k) for k in every]),
                    ticks('7,11', [functools.partial(spread.forward2, k) for k in every]), ticks('21', gather.forwards()))
    mlp_rest(slot, actions, io, wb.at[slot, 0], wb.at[slot, 1], w1t, yt, gt, dht)

    @pl.when(slot == SLOTS - 1)
    def _():
        with jax.named_scope('e00_gather_forward_1_'):
            gather.forward(1)
        with jax.named_scope('e01_io_finish_'):
            io.finish()
        with jax.named_scope('e02_spread_finish_'):
            spread.finish()
        with jax.named_scope('e03_gather_finish_'):
            gather.finish()


def mlp_first(layer, y, dz, wup, wdn, wq, wo):
    d, f = wup.shape[1:]
    seq = y.shape[2]
    seqs = y.shape[1] // SLOTS
    tok = seqs * seq
    return pl.pallas_call(
        functools.partial(mlp_first_kernel, layer),
        out_shape=(jax.ShapeDtypeStruct((d, tok), BF16), jax.ShapeDtypeStruct((SLOTS, 2, 4, d // 4, f), F32), jax.ShapeDtypeStruct((SLOTS, d, d), BF16)),
        grid=(SLOTS,),
        in_specs=[ANY] * 6,
        out_specs=[ANY] * 3,
        scratch_shapes=[pltpu.VMEM((seqs, seq, d), BF16)] * 2 + [pltpu.VMEM((d, tok), BF16)] * 2
        + [pltpu.VMEM((d, tok), F32), pltpu.VMEM((f, d), BF16), pltpu.VMEM((f, tok), BF16), pltpu.VMEM((f, tok), BF16), pltpu.VMEM((SLOTS, 2, d, f), BF16),
           pltpu.VMEM((d, d), BF16), pltpu.VMEM((d, tok), BF16), pltpu.VMEM((2, 4, d // 4, f), F32)] + SEMS,
        compiler_params=params(0, 1),
        name='mlp_first',
    )(y, dz, wup, wdn, wq, wo)


def mlp_second_kernel(layer, w1_ref, w2_ref, y, dz_in, partial, half, wq, wo, dy_hbm, g_hbm, wa_g, red, red_half, yb, yt, dzt, acc, w1t, gt, dht, bounce, dyb, gbuf, mine,
                      *rest):
    slot = pl.program_id(0)
    seqs, seq = yb.shape[:2]
    bufs, rest = rest[:4], rest[4:]
    peers, sems = Peers(), Sems(*rest[2:])
    place = peers.t * seqs
    loads = [(sems.copies(seqs, lambda i: y.at[layer, place + i], lambda i: yb.at[i]), turned(yb, yt, seq)),
             (sems.copies(seqs, lambda i: dz_in.at[:, tokens(i, seq)], lambda i: dzt.at[:, tokens(i, seq)]), lambda i: None)]
    io = MlpIo(sems, peers, seqs, seq, loads, acc, dzt, dyb, dy_hbm, gbuf, g_hbm)
    blocks = attn_weights(layer, wq, wo, wa_g)
    gather = Gather(sems, peers, [r[:2] for r in blocks])
    hop = Bounce(sems, blocks, bounce)
    rows = mine.shape[2] // 2
    a, b = jobs = [Scatter(sems, peers, lambda s: partial.at[s], lambda x: mine.at[x], bufs, lambda j=j: red.at[pl.ds(j * rows, rows)], (j * rows, rows)) for j in range(2)]

    h0, h1 = rest[:2]
    mine_half = sems.copy(lambda: half.at[0], lambda: h0)
    x_half = sems.remote(lambda: half.at[1], lambda: h1, peers.xp)
    store_half = sems.copy(lambda: h0, lambda: red_half)

    def add_half():
        mine_half().wait()
        x_half().wait_recv()
        h0[...] = (h0[...] + h1[...]) * (1 / SLOTS)

    @pl.when(slot == 0)
    def _():
        with jax.named_scope('e00_io_start_'):
            io.start()
        with jax.named_scope('e01_peers_barrier_'):
            peers.barrier()
        with jax.named_scope('e02_jobs__job_both_start_'):
            for job in jobs:
                job.both('start')
        with jax.named_scope('e03_x_half_start_'):
            x_half().start()
        with jax.named_scope('e04_mine_half_start_'):
            mine_half().start()
        with jax.named_scope('e05_gather_start_range_2_'):
            gather.start(range(2))
    actions = merge([(4 + k, s) for k, s in enumerate(hop.steps)], ticks('17,22,12,13', gather.forwards() + [add_half, lambda: store_half().start()]),
                    steps(a, '3add0,4send1,10add1,11send2,17add2,18send3,22add3,23out'),
                    steps(b, '4add0,5send1,15add1,16send2,20add2,21send3'))
    mlp_rest(slot, actions, io, w1_ref.at[0], w2_ref.at[0], w1t, yt, gt, dht)

    @pl.when(slot == SLOTS - 1)
    def _():
        with jax.named_scope('e00_b_add3_'):
            b.add3()
        with jax.named_scope('e01_io_finish_'):
            io.finish()
        with jax.named_scope('e02_gather_finish_'):
            gather.finish()
        with jax.named_scope('e03_x_half_wait_send_'):
            x_half().wait_send()
        with jax.named_scope('e04_store_half_wait_'):
            store_half().wait()
        with jax.named_scope('e05_b_out_'):
            b.out()
        with jax.named_scope('e06_a_finish_'):
            a.finish()
        with jax.named_scope('e07_b_finish_'):
            b.finish()


def mlp_second(layer, y, dz, w1, w2, partial, half, wq, wo):
    d, f = w1.shape[1:]
    seq = y.shape[2]
    seqs = y.shape[1] // SLOTS
    tok = seqs * seq
    return pl.pallas_call(
        functools.partial(mlp_second_kernel, layer),
        out_shape=(jax.ShapeDtypeStruct((d, tok), BF16), jax.ShapeDtypeStruct((SLOTS, 2, 4, d // 4, f), F32), jax.ShapeDtypeStruct((SLOTS, d, d), BF16),
                   jax.ShapeDtypeStruct((d // 4, d), F32), jax.ShapeDtypeStruct(half.shape[1:], F32)),
        grid=(SLOTS,),
        in_specs=[leading(d, f), leading(f, d)] + [ANY] * 6,
        out_specs=[ANY] * 5,
        scratch_shapes=[pltpu.VMEM((seqs, seq, d), BF16), pltpu.VMEM((d, tok), BF16), pltpu.VMEM((d, tok), BF16), pltpu.VMEM((d, tok), F32), pltpu.VMEM((f, d), BF16),
                        pltpu.VMEM((f, tok), BF16), pltpu.VMEM((f, tok), BF16), pltpu.VMEM((d, d), BF16), pltpu.VMEM((d, tok), BF16),
                        pltpu.VMEM((2, 4, d // 4, f), F32), pltpu.VMEM((2, 4, d // 4, d), F32)]
        + scatter_bufs(d // 4, d) + [pltpu.VMEM(half.shape[1:], F32)] * 2 + SEMS,
        compiler_params=params(1, 1),
        name='mlp_second',
    )(w1, w2, y, dz, partial, half, wq, wo)


def attn_step(sems, peers, x_ref, dy_hbm, w_hbm, dy_ref, w_ref, xt, acc, gacc, qkv, do, b1, b2, begin, act, emit):
    s, slot = pl.program_id(0), pl.program_id(1)
    step = s * SLOTS + slot
    last = SLOTS * SLOTS - 1
    before = jnp.maximum(step - 1, 0)
    seq, d = x_ref.shape[-2:]
    nqkv = qkv.shape[0]
    third = nqkv // 3
    split = d - b2.shape[1]
    rows = d // 4

    load_w = sems.copies(SLOTS, lambda i: w_hbm.at[i], lambda i: w_ref.at[i])
    load_dy = sems.copies(SLOTS, lambda i: dy_hbm.at[:, tokens(i, seq)], lambda i: dy_ref.at[:, tokens(i, seq)])

    @pl.when(step == 0)
    def _():
        for i in range(SLOTS):
            load_w(i).start()
            load_dy(i).start()
        begin()
        def clear(j, carry):
            gacc[j // 4, j % 4] = jnp.zeros(gacc.shape[2:], F32)
            b1[j % 2] = jnp.zeros(b1.shape[1:], BF16)
            b2[j % 2] = jnp.zeros(b2.shape[1:], BF16)
            return carry
        lax.fori_loop(0, SLOTS * 4, clear, 0)
    act()
    with jax.named_scope('loadw'):
        pl.when(s == 0)(lambda: load_w(slot).wait())

    @pl.when(slot == 0)
    def _():
        with jax.named_scope('e00_load_dy_s_wait_'):
            load_dy(s).wait()
        with jax.named_scope('e01_xt_s_2_x_ref_0_0_T'):
            xt[s % 2] = x_ref[0, 0].T

    def grads(n, par):
        ps, pj = n // SLOTS, n % SLOTS
        third_d = d // 3

        def weights(c):
            cols = slice(c * third_d, (c + 1) * third_d)
            g = dot(xt[ps % 2], b1[par, cols], NT)
            if c == 2:
                g = g + dot(dy_ref[:, tokens(ps, seq)], b2[par], NT)
            for k in range(4):
                r = peers.rel(k)
                gacc[pj, r, :, cols] = gacc[pj, r, :, cols] + g[k * rows:(k + 1) * rows]

        def inputs(c):
            part = slice(c * third_d, (c + 1) * third_d)
            acc[part] += dot(w_ref[pj, :, part].T, b1[par], NN)
        return [functools.partial(f, c) for c in range(3) for f in (weights, inputs)]
    with jax.named_scope("main"):
        x_t = xt[s % 2]
        dy_t = dy_ref[:, tokens(s, seq)]
        now = step % 2
        qkv[...] = dot(w_ref[slot, pl.ds(0, nqkv), :], x_t, NN).astype(BF16)
        do[...] = dot(w_ref[slot, pl.ds(nqkv, d - nqkv), :], dy_t, NN).astype(BF16)
        scale = HEAD ** -0.5
        exp_scale = scale * math.log2(math.e)
        qb = seq // 2
        units = [(h, slice(c * qb, (c + 1) * qb)) for h in range(third // HEAD) for c in range(2)]

        def scores(h, qc):
            q_rows, k_rows, v_rows = head_rows(h)
            return dot(qkv[k_rows, :].T, qkv[q_rows, qc], NN), dot(qkv[v_rows, :].T, do[q_rows, qc] * scale, NN)

        def head_rows(h):
            return [slice(i * third + h * HEAD, i * third + (h + 1) * HEAD) for i in range(3)]
        for piece in grads(before, 1 - step % 2):
            piece()
        ahead = [scores(*unit) for unit in units[:LOOK_AHEAD]]
        for n, (h, qc) in enumerate(units):
            sc, dp_t = ahead.pop(0)
            if n + LOOK_AHEAD < len(units):
                ahead.append(scores(*units[n + LOOK_AHEAD]))
            q_rows, k_rows, v_rows = head_rows(h)
            m = jnp.max(sc, axis=0, keepdims=True)
            e = jnp.exp2((sc - m) * exp_scale)
            inv = 1.0 / jnp.sum(e, axis=0, keepdims=True)
            rd = jnp.sum(e * dp_t, axis=0, keepdims=True) * inv
            p = e * inv
            p_bf = p.astype(BF16)
            ds = (p * (dp_t - rd)).astype(BF16)
            b2[now, pl.ds(b2.shape[1] - third + h * HEAD, HEAD), qc] = dot(qkv[v_rows, :], p_bf, NN).astype(BF16)
            b1[now, q_rows, qc] = dot(qkv[k_rows, :], ds, NN).astype(BF16)
            dv_c = dot(do[q_rows, qc], p_bf, NT)
            dk_c = dot(qkv[q_rows, qc], ds, NT)
            if n % 2 == 0:
                dv, dk = dv_c, dk_c
            else:
                b1[now, k_rows] = (dk + dk_c).astype(BF16)
                b1[now, v_rows] = (dv + dv_c).astype(BF16)

    @pl.when(slot == 0)
    def _():
        @pl.when(s > 0)
        def _():
            emit(s - 1)
        acc[...] = dy_ref[:, tokens(s, seq)].astype(F32)

    @pl.when(step == last)
    def _():
        with jax.named_scope('e00_for_piece_in_grads_last_last_2__pi'):
            for piece in grads(last, last % 2):
                piece()
        with jax.named_scope('e01_emit_s_'):
            emit(s)


ATTN_IN = 3
ATTN_SCRATCH = 9
JOB_PLAN = '1add0,2send1,7add1,8send2,12add2', '2add0,3send1x,8send1y,10add1x,11send2x,14add1y,15send2y'


def attn_first_kernel(layer, x_ref, dy_hbm, w_hbm, partial, wup, wdn, dx_hbm, g_hbm, w1_g, w2_g, half, *rest):
    body, rest = rest[:ATTN_SCRATCH], rest[ATTN_SCRATCH:]
    acc, gacc, mine, bounce = body[3], body[4], rest[:2], rest[-4]
    seq = x_ref.shape[-2]
    step = pl.program_id(0) * SLOTS + pl.program_id(1)
    peers, sems = Peers(), Sems(*rest[-3:])
    a, b = jobs = [Scatter(sems, peers, lambda s, j=j: partial.at[s, j], lambda x, j=j: mine[j].at[x], rest[2 + 4 * j:6 + 4 * j], None,
                           (0, half.shape[2]), half_out=lambda x, j=j: half.at[x, j]) for j in range(2)]
    blocks = [(lambda w=w: w.at[layer - 1], lambda j, g=g: g.at[j], wup.shape[1]) for w, g in ((wup, w1_g), (wdn, w2_g))]
    gather = Gather(sems, peers, [r[:2] for r in blocks])
    hop = Bounce(sems, blocks, bounce)
    stores = [sems.copy(lambda j=j: gacc.at[j], lambda j=j: g_hbm.at[j]) for j in range(SLOTS)]
    actions = merge(steps(a, JOB_PLAN[0]), steps(b, JOB_PLAN[1]), [(5 + k, s) for k, s in enumerate(hop.steps)],
                    ticks('7,13', gather.forwards()))

    dxb = rest[-5]
    store_dx = sems.copies(SLOTS, lambda i: dxb.at[i], lambda i: dx_hbm.at[:, tokens(i, seq)])

    def begin():
        peers.barrier()
        for job in jobs:
            job.both('start')
        gather.start(range(2))

    def emit(s):
        dxb[s] = acc[...].astype(BF16)
        store_dx(s).start()
    attn_step(sems, peers, x_ref, dy_hbm, w_hbm, *body, begin, lambda: at_ticks(actions, step), emit)

    @pl.when(step == SLOTS * SLOTS - 1)
    def _():
        with jax.named_scope('e00_for_c_in_stores__c_start_'):
            for c in stores:
                c().start()
        with jax.named_scope('e01_a_out_'):
            a.out()
        with jax.named_scope('e02_b_both_add2_'):
            b.both('add2')
        with jax.named_scope('e03_gather_finish_'):
            gather.finish()
        with jax.named_scope('e04_for_c_in_stores__c_wait_'):
            for c in stores:
                c().wait()
        with jax.named_scope('e05_b_out_'):
            b.out()
        with jax.named_scope('e06_for_i_in_range_SLOTS__store_dx_i_w'):
            for i in range(SLOTS):
                store_dx(i).wait()
        with jax.named_scope('e07_jobs__job_finish_'):
            for job in jobs:
                job.finish()


def attn_last_kernel(x_ref, dy_hbm, w_hbm, partial, dxg, red, red_last, *rest):
    body, rest = rest[:ATTN_SCRATCH], rest[ATTN_SCRATCH:]
    acc, gacc, mine, dxb, free = body[3], body[4], rest[:2], rest[-5], rest[-4]
    step = pl.program_id(0) * SLOTS + pl.program_id(1)
    seqs = pl.num_programs(0)
    peers, sems = Peers(), Sems(*rest[-3:])
    nred = red.shape[1]
    a, b = jobs = [Scatter(sems, peers, lambda s, j=j: partial.at[s, j], lambda x, j=j: mine[j].at[x], rest[2 + 4 * j:6 + 4 * j], lambda j=j: red.at[j],
                           (0, nred)) for j in range(2)]
    h = nred // 2
    ends = [Scatter(sems, peers, lambda s: gacc.at[s], lambda x: gacc.at[2 * x], rest[2:6], lambda j=j: red_last.at[pl.ds(j * h, h)], (j * h, h), load=False)
            for j in range(2)]
    t = peers.t
    t2 = (t + 2) % SLOTS
    sib, xp, fwd, mine_dx = [], [], [], []
    for s in range(SLOTS):
        def src(s=s):
            return dxb.at[s]

        def dst(s=s):
            return dxg.at[t * SLOTS + s]

        def other(s=s):
            return dxg.at[t2 * SLOTS + s]
        mine_dx.append(sems.copy(src, dst))
        sib.append(sems.remote(src, dst, peers.sib))
        xp.append(sems.remote(src, dst, peers.xp))
        fwd.append(sems.remote(other, other, peers.sib))

    def freed(i):
        for peer in ([peers.sib], [peers.yp, peers.zp], [peers.yp, peers.zp], [peers.xp])[i]:
            pl.semaphore_signal(free.at[i], inc=1, device_id=peer, device_id_type=MESH)

    def forward(s):
        xp[s]().wait_recv()
        fwd[s]().start()

    def early():
        pl.semaphore_wait(free.at[0], 1)
        for job in ends:
            job.start(0)
    actions = merge(steps(a, '1add0y,2send1y,5add1y,6send2y,9add2y,10send3,12add1x,13send2x'), steps(b, '1add0y,2send1y,7add1y,8send2y,10add2y,11send3,15add1x'),
                    *[steps(job, '2add0x,8send1x') for job in jobs],
                    ticks('3,13,9,14,15', [functools.partial(freed, i) for i in range(2)] + [functools.partial(forward, i) for i in range(2)] + [early]))

    def begin():
        peers.barrier()
        for x in (1, 0):
            for job in jobs:
                job.start(x)

    def emit(s):
        dxb[s] = acc[...].T.astype(BF16)
        for k in range(SLOTS):
            @pl.when(s == k)
            def _(k=k):
                for c in (xp, sib, mine_dx):
                    c[k]().start()
    attn_step(sems, peers, x_ref, dy_hbm, w_hbm, *body, begin, lambda: at_ticks(actions, step), emit)

    @pl.when(step == SLOTS * SLOTS - 1)
    def _():
        with jax.named_scope('e00_b_send2_0_'):
            b.send2(0)
        with jax.named_scope('e01_ends__job_start_1__job_add0_0_'):
            for job in ends:
                job.start(1)
                job.add0(0)
        with jax.named_scope('e02_pl_semaphore_wait_free_at_1_2_'):
            pl.semaphore_wait(free.at[1], 2)
        with jax.named_scope('e03_a_add2_0_'):
            a.add2(0)
        with jax.named_scope('e04_freed_2_'):
            freed(2)
        with jax.named_scope('e05_ends__job_send1_0_'):
            for job in ends:
                job.send1(0)
        with jax.named_scope('e06_a_add3_'):
            a.add3()
        with jax.named_scope('e07_freed_3_'):
            freed(3)
        with jax.named_scope('e08_ends__job_add0_1_'):
            for job in ends:
                job.add0(1)
        with jax.named_scope('e09_a_out_'):
            a.out()
        with jax.named_scope('e10_b_add2_0_'):
            b.add2(0)
        with jax.named_scope('e11_ends__job_send1_1_'):
            for job in ends:
                job.send1(1)
        with jax.named_scope('e12_b_add3_'):
            b.add3()
        with jax.named_scope('e13_forward_2_'):
            forward(2)
        with jax.named_scope('e14_b_out_'):
            b.out()
        with jax.named_scope('e15_pl_semaphore_wait_free_at_2_2_'):
            pl.semaphore_wait(free.at[2], 2)
        with jax.named_scope('e16_ends__job_add1_0__job_send2_0_'):
            for job in ends:
                job.add1(0)
                job.send2(0)
        with jax.named_scope('e17_ends__job_add1_1__job_send2_1_'):
            for job in ends:
                job.add1(1)
                job.send2(1)
        with jax.named_scope('e18_pl_semaphore_wait_free_at_3_1_'):
            pl.semaphore_wait(free.at[3], 1)
        with jax.named_scope('e19_forward_3_'):
            forward(3)
        with jax.named_scope('e20_ends__job_both_add2__job_send3_'):
            for job in ends:
                job.both('add2')
                job.send3()
        with jax.named_scope('e21_for_s_in_range_SLOTS__mine_dx_s_wa'):
            for s in range(SLOTS):
                mine_dx[s]().wait()
                sib[s]().wait()
                xp[s]().wait_send()
        with jax.named_scope('e22_ends__job_add3__job_out_'):
            for job in ends:
                job.add3()
                job.out()
        with jax.named_scope('e23_for_s_in_range_SLOTS__fwd_s_wait_'):
            for s in range(SLOTS):
                fwd[s]().wait()
        with jax.named_scope('e24_jobs_ends__job_finish_'):
            for job in jobs + ends:
                job.finish()


def attn_specs(layer, x, w):
    slots, nw, d = w.shape
    seq = x.shape[2]
    seqs = x.shape[1] // slots
    tok = seqs * seq
    nqkv = nw * 3 // 4
    in_specs = [pl.BlockSpec((1, 1, seq, d), lambda s, j: (layer, lax.axis_index('tp') * seqs + s, 0, 0))] + [ANY] * 3
    scratch = [pltpu.VMEM((d, tok), BF16), pltpu.VMEM((slots, nw, d), BF16), pltpu.VMEM((2, d, seq), BF16), pltpu.VMEM((d, seq), F32), pltpu.VMEM((slots, 4, d // 4, nw), F32), pltpu.VMEM((nqkv, seq), BF16),
               pltpu.VMEM((nw - nqkv, seq), BF16), pltpu.VMEM((2, nw, seq), BF16), pltpu.VMEM((2, d // 3, seq), BF16)]
    scratch += [pltpu.VMEM((2, 4, d // 4, d), F32)] * 2 + scatter_bufs(d // 4, d) * 2
    red = jax.ShapeDtypeStruct((2, d // 4, d), F32)
    return (slots, seqs), in_specs, scratch, red, tok


def attn_first(layer, x, dy, w, partial, wup, wdn):
    grid, in_specs, scratch, red, tok = attn_specs(layer, x, w)
    slots, nw, d = w.shape
    gathered = [jax.ShapeDtypeStruct((slots, d, d), BF16)] * 2
    return pl.pallas_call(
        functools.partial(attn_first_kernel, layer),
        out_shape=[jax.ShapeDtypeStruct((d, tok), BF16), jax.ShapeDtypeStruct((slots, 4, d // 4, nw), F32)] + gathered + [jax.ShapeDtypeStruct((2,) + red.shape, F32)],
        grid=grid,
        in_specs=in_specs + [ANY, ANY],
        out_specs=[ANY] * 5,
        scratch_shapes=scratch + [pltpu.VMEM((slots, d, tok // slots), BF16), pltpu.VMEM((d, d), BF16)] + SEMS,
        compiler_params=params(2, 2),
        name='attn_first',
    )(x, dy, w, partial, wup, wdn)


def attn_last(layer, x, dy, w, partial):
    grid, in_specs, scratch, red, tok = attn_specs(layer, x, w)
    slots, nw, d = w.shape
    seq = x.shape[2]
    return pl.pallas_call(
        attn_last_kernel,
        out_shape=[jax.ShapeDtypeStruct((x.shape[1], seq, d), BF16), red, jax.ShapeDtypeStruct(red.shape[1:], F32)],
        grid=grid,
        in_specs=in_specs,
        out_specs=[ANY] * 3,
        scratch_shapes=scratch + [pltpu.VMEM((slots, seq, d), BF16), pltpu.SemaphoreType.REGULAR((4,))] + SEMS,
        compiler_params=params(3, 2),
        name='attn_last',
    )(x, dy, w, partial)


def solution(mesh):
    assert dict(mesh.shape) == {'dpy': 2, 'dpx': 2, 'tp': SLOTS}
    act_spec = P(None, DATA_AXES, None, None)

    def device_backward(x_saved, y_saved, dz_top, w_qkv, w_out, w_up, w_down):
        layers, d = w_up.shape[:2]
        assert layers == 2
        heads, hd = w_out.shape[1:3]
        n = 3 * heads * hd
        wq = w_qkv.transpose(0, 2, 3, 4, 1).reshape(layers, n, d)
        wo = w_out.reshape(layers, heads * hd, d)
        dy1, gm1, wa1 = mlp_first(1, y_saved, dz_top, w_up, w_down, wq, wo)
        dx1, ga1, w1_0, w2_0, half = attn_first(1, x_saved, dy1, wa1, gm1, w_up, w_down)
        dy0, gm0, wa0, ra1, rm1 = mlp_second(0, y_saved, dx1, w1_0, w2_0, ga1, half, wq, wo)
        d_input, rm0, ra0 = attn_last(0, x_saved, dy0, wa0, gm0)
        g_a = jnp.stack([ra0, ra1])
        g_qkv = g_a[:, :, :n].reshape(layers, d // 4, 3, heads, hd)
        g_out = g_a[:, :, n:].transpose(0, 2, 1).reshape(layers, heads, hd, d // 4)
        return d_input, g_qkv, g_out, jnp.stack([rm0[1], rm1[1]]), jnp.stack([rm0[0], rm1[0]])

    tp_last = P(None, None, None, 'tp', None), P(None, 'tp', None, None), P(None, None, 'tp'), P(None, 'tp', None)
    return jax.shard_map(device_backward, mesh=mesh,
                         in_specs=(act_spec, act_spec, P(DATA_AXES, None, None)) + tp_last,
                         out_specs=(P(DATA_AXES, None, None), P(None, DATA_AXES, None, 'tp', None), P(None, 'tp', None, DATA_AXES), P(None, DATA_AXES, 'tp'), P(None, ('tp', 'dpy', 'dpx'), None)),
                         check_vma=False)
```

```python
import functools
import math
import re

import jax
import jax.numpy as jnp
from jax import lax
from jax.experimental import pallas as pl
from jax.experimental.pallas import tpu as pltpu
from jax.sharding import PartitionSpec as P

DATA_AXES = ('dpy', 'dpx')
F32 = jnp.float32
BF16 = jnp.bfloat16
HEAD = 64
SLOTS = 4
LOOK_AHEAD = 3
PIECES = 8
NN = (((1,), (0,)), ((), ()))
NT = (((1,), (1,)), ((), ()))
VMEM_LIMIT = 63 * 1024 * 1024
MESH = pl.DeviceIdType.MESH
ANY = pl.BlockSpec(memory_space=pl.ANY)


def dot(a, b, dims):
    return lax.dot_general(a, b, dims, preferred_element_type=F32)


class Peers:
    def __init__(self):
        z, y, t = lax.axis_index('dpy'), lax.axis_index('dpx'), lax.axis_index('tp')
        self.z, self.y, self.t = z, y, t
        self.sib = (z, y, t + 1 - 2 * (t % 2))
        self.xp = (z, y, (t + 2) % 4)
        self.yp = (z, 1 - y, t)
        self.zp = (1 - z, y, t)

    def barrier(self):
        sem = pltpu.get_barrier_semaphore()
        with jax.named_scope('entry'):
            for peer in (self.sib, self.xp, self.yp, self.zp):
                pl.semaphore_signal(sem, inc=1, device_id=peer, device_id_type=MESH)
            pl.semaphore_wait(sem, 4)

    def rel(self, d):
        zr = self.z if d // 2 == 0 else 1 - self.z
        yr = self.y if d % 2 == 0 else 1 - self.y
        return zr * 2 + yr


class Sems:
    def __init__(self, send, recv, local):
        self.send, self.recv, self.local = send, recv, local
        self.n = self.m = 0

    def remote(self, src, dst, peer):
        i = self.n
        self.n += 1
        return lambda: pltpu.make_async_remote_copy(src_ref=src(), dst_ref=dst(), send_sem=self.send.at[i], recv_sem=self.recv.at[i],
                                                    device_id=peer, device_id_type=MESH)

    def copy(self, src, dst):
        i = self.m
        self.m += 1
        return lambda: pltpu.make_async_copy(src(), dst(), self.local.at[i])

    def copies(self, n, src, dst):
        first = self.m
        self.m += n
        return lambda i: pltpu.make_async_copy(src(i), dst(i), self.local.at[first + i])


def at_ticks(actions, tick, position=0, points=1):
    for k in sorted(actions):
        if k % points == position:
            @pl.when(tick == k)
            def _(k=k):
                with jax.named_scope('t%d' % k):
                    for action in actions[k]:
                        action()


class Scatter:
    def __init__(self, sems, peers, partial, mine, bufs, out, rows, load=True, half_out=None):
        r0, r1, r2, r3 = self.bufs = bufs
        first, count = rows
        h = count // 2
        self.mine, self.all, self.lo, self.hi = mine, pl.ds(first, count), pl.ds(first, h), pl.ds(first + h, h)
        self.half = half = pl.ds(first // 2, h)
        every, lo, hi = self.all, self.lo, self.hi
        self.load, self.c0, self.c1, self.c2 = [], [], [], []
        for x in range(2):
            def near(k, part, x=x):
                return lambda: mine(x).at[k, part]

            def place(buf, *index):
                return lambda: buf.at[index]
            if load:
                self.load.append(sems.copy(lambda x=x: partial(2 * x).at[:, every], near(slice(None), every)))
            self.c0.append(sems.remote(lambda x=x: partial(2 * x + 1).at[:, every], place(r0, x, slice(None), every), peers.sib))
            self.c1.append([sems.remote(near(2 * k + 1, lo), place(r1, 0, x, k, half), peers.yp) for k in range(2)]
                           + [sems.remote(near(2 + k, hi), place(r1, 1, x, k, half), peers.zp) for k in range(2)])
            self.c2.append([sems.remote(near(2, lo), place(r2, 0, x, half), peers.zp), sems.remote(near(1, hi), place(r2, 1, x, half), peers.yp)])
        if half_out is None:
            self.c3 = sems.remote(lambda: mine(1).at[0, every], place(r3, every), peers.xp)
            self.store = [sems.copy(lambda: mine(0).at[0, every], out)]
        else:
            self.c3 = None
            self.store = [sems.copy(lambda x=x: mine(x).at[0, every], lambda x=x: half_out(x)) for x in range(2)]

    def start(self, x):
        self.c0[x]().start()
        if self.load:
            self.load[x]().start()

    def add0(self, x):
        if self.load:
            self.load[x]().wait()
        self.c0[x]().wait_recv()
        mine, r0 = self.mine(x), self.bufs[0].at[x]

        def body(k, carry):
            mine[k, self.all] = mine[k, self.all] + r0[k, self.all]
            return carry
        lax.fori_loop(0, 4, body, 0)

    def send1(self, x):
        for c in self.c1[x]:
            c().start()

    def add1(self, x):
        for c in self.c1[x]:
            c().wait_recv()
        mine, r1 = self.mine(x), self.bufs[1]

        def body(k, carry):
            mine[2 * k, self.lo] = mine[2 * k, self.lo] + r1[0, x, k, self.half]
            mine[k, self.hi] = mine[k, self.hi] + r1[1, x, k, self.half]
            return carry
        lax.fori_loop(0, 2, body, 0)

    def send2(self, x):
        for c in self.c2[x]:
            c().start()

    def add2(self, x):
        for c in self.c2[x]:
            c().wait_recv()
        mine, r2 = self.mine(x), self.bufs[2]
        mine[0, self.lo] = mine[0, self.lo] + r2[0, x, self.half]
        mine[0, self.hi] = mine[0, self.hi] + r2[1, x, self.half]

    def send3(self):
        self.c3().start()

    def add3(self):
        self.c3().wait_recv()
        mine = self.mine(0)
        mine[0, self.all] = (mine[0, self.all] + self.bufs[3][self.all]) * (1 / SLOTS)

    def out(self):
        for c in self.store:
            c().start()

    def finish(self):
        for c in self.c0 + sum(self.c1, []) + sum(self.c2, []) + ([self.c3] if self.c3 else []):
            c().wait_send()
        for c in self.store:
            c().wait()

    def both(self, name):
        for x in range(2):
            getattr(self, name)(x)


def scatter_bufs(rows, d):
    return [pltpu.VMEM((2, 4, rows, d), F32), pltpu.VMEM((2, 2, 2, rows // 2, d), F32), pltpu.VMEM((2, 2, rows // 2, d), F32), pltpu.VMEM((rows, d), F32)]


def steps(job, plan):
    out = []
    for tick, name, half in re.findall('([0-9]+)([a-z]+[0-3]?)([xy]?)', plan):
        if half:
            action = functools.partial(getattr(job, name), int(half == 'y'))
        else:
            action = functools.partial(job.both, name) if name[-1] in '012' else getattr(job, name)
        out.append((int(tick), action))
    return out


def ticks(plan, actions):
    return list(zip(map(int, plan.split(',')), actions))


class Gather:
    def __init__(self, sems, peers, blocks):
        self.sib = [sems.remote(own, lambda dst=dst: dst(1), peers.sib) for own, dst in blocks]
        self.xp = [sems.remote(own, lambda dst=dst: dst(2), peers.xp) for own, dst in blocks]
        self.fwd = [sems.remote(lambda dst=dst: dst(2), lambda dst=dst: dst(3), peers.sib) for own, dst in blocks]

    def start(self, blocks):
        for i in blocks:
            self.sib[i]().start()
            self.xp[i]().start()

    def forward(self, i):
        self.xp[i]().wait_recv()
        self.fwd[i]().start()

    def forwards(self):
        return [functools.partial(self.forward, i) for i in range(len(self.fwd))]

    def finish(self):
        for i in range(len(self.sib)):
            self.sib[i]().wait_recv()
            self.fwd[i]().wait_recv()
            self.sib[i]().wait_send()
            self.xp[i]().wait_send()
            self.fwd[i]().wait_send()


class Bounce:
    def __init__(self, sems, items, buf):
        self.steps = []
        prev = None
        for own, dst, rows in items:
            ld = sems.copy(own, lambda rows=rows: buf.at[pl.ds(0, rows)])
            st = sems.copy(lambda rows=rows: buf.at[pl.ds(0, rows)], lambda dst=dst: dst(0))
            self.steps.append(functools.partial(self.load, prev, ld))
            self.steps.append(functools.partial(self.flip, ld, st))
            prev = st
        self.steps.append(lambda prev=prev: prev().wait())

    @staticmethod
    def load(prev, ld):
        if prev is not None:
            prev().wait()
        ld().start()

    @staticmethod
    def flip(ld, st):
        ld().wait()
        st().start()


def merge(*lists):
    actions = {}
    for pairs in lists:
        for k, action in pairs:
            actions.setdefault(k, []).append(action)
    return actions


SEMS = [pltpu.SemaphoreType.DMA((96,)), pltpu.SemaphoreType.DMA((96,)), pltpu.SemaphoreType.DMA((32,))]


def leading(*shape):
    return pl.BlockSpec((1,) + shape, lambda j, *_: (j,) + (0,) * len(shape))


def params(collective_id, axes):
    return pltpu.CompilerParams(vmem_limit_bytes=VMEM_LIMIT, dimension_semantics=('arbitrary',) * axes, collective_id=collective_id, has_side_effects=True)


def mlp_slot(slot, seqs, seq, w1, w2, w1t, yt, dz, acc, gt, dht, tick, arrive, emit):
    w1t[...] = w1[...].T

    def block(i, carry):
        tick(i)
        with jax.named_scope('arrive'):
            pl.when(slot == 0)(lambda: arrive(i))
        cols = pl.ds(pl.multiple_of(i * seq, seq), seq)
        h = dot(w1t[...], yt[:, cols], NN)
        dg = dot(w2[...], dz[:, cols], NN)
        c0 = math.sqrt(2 / math.pi)
        c1 = 0.044715 * c0
        h2 = h * h
        t = jnp.tanh(h * (c0 + c1 * h2))
        q = 0.5 * t + 0.5
        g = h * q
        dh = dg * (q + (g * (1.0 - t)) * (c0 + (3 * c1) * h2))
        gt[:, cols] = g.astype(BF16)
        dh = dh.astype(BF16)
        dht[:, cols] = dh
        acc[:, cols] += dot(w1[...], dh, NN)
        with jax.named_scope('memit'):
            pl.when(slot == SLOTS - 1)(lambda: emit(i))
        return carry
    lax.fori_loop(0, seqs, block, 0)


def tokens(i, seq):
    return pl.ds(pl.multiple_of(i * seq, seq), seq)


class MlpIo:
    def __init__(self, sems, peers, seqs, seq, loads, acc, dz, dyb, dy_hbm, gbuf, g_hbm):
        self.seqs, self.seq, self.peers = seqs, seq, peers
        self.loads, self.acc, self.dz, self.dyb, self.gbuf = loads, acc, dz, dyb, gbuf
        self.dy = sems.copies(seqs, lambda i: dyb.at[:, tokens(i, seq)], lambda i: dy_hbm.at[:, tokens(i, seq)])
        self.g = [sems.copy(lambda j=j: gbuf.at[j], lambda j=j: g_hbm.at[pl.program_id(0), j]) for j in range(2)]

    def start(self):
        for load, _ in self.loads:
            for i in range(self.seqs):
                load(i).start()

    def arrive(self, i):
        for load, use in self.loads:
            load(i).wait()
            use(i)
        cols = tokens(i, self.seq)
        self.acc[:, cols] = jnp.zeros((self.acc.shape[0], self.seq), F32)

    def emit(self, i):
        cols = tokens(i, self.seq)
        self.dyb[:, cols] = (self.dz[:, cols].astype(F32) + self.acc[:, cols]).astype(BF16)
        self.dy(i).start()

    def grads(self, j, a, b):
        pl.when(pl.program_id(0) > 0)(lambda: self.g[j]().wait())
        rows, width = self.gbuf.shape[-2:]
        split, half = width * 2 // 3, width // 2
        for lo, hi, c0, c1 in ((0, width, 0, split), (0, half, split, width), (half, width, split, width)):
            g = dot(a[lo:hi], b[c0:c1], NT)
            for k in range(g.shape[0] // rows):
                self.gbuf[j, self.peers.rel(lo // rows + k), :, c0:c1] = g[k * rows:(k + 1) * rows]
        self.g[j]().start()

    def finish(self):
        for i in range(self.seqs):
            self.dy(i).wait()
        for c in self.g:
            c().wait()


def mlp_rest(slot, actions, io, w1, w2, w1t, yt, gt, dht):
    seqs, seq, dz, acc = io.seqs, io.seq, io.dz, io.acc
    points = seqs + 2
    first = slot * points

    def tick(i):
        at_ticks({k: v for k, v in actions.items() if k % points < seqs}, first + i)
    mlp_slot(slot, seqs, seq, w1, w2, w1t, yt, dz, acc, gt, dht, tick, io.arrive, io.emit)
    at_ticks(actions, first + seqs, seqs, points)
    with jax.named_scope('dw2'):
        io.grads(0, gt, dz)
    at_ticks(actions, first + seqs + 1, seqs + 1, points)
    with jax.named_scope('dw1'):
        io.grads(1, yt, dht)


def attn_weights(layer, wq, wo, wa_g):
    nq, d = wq.shape[1:]
    return [(lambda: wq.at[layer], lambda j: wa_g.at[j, pl.ds(0, nq)], nq), (lambda: wo.at[layer], lambda j: wa_g.at[j, pl.ds(nq, d - nq)], d - nq)]


class Spread:
    def __init__(self, sems, peers, wb, pieces):
        rows = wb.shape[2] // pieces
        y = peers.y

        def piece(slot, m, k):
            return lambda: wb.at[slot, m, pl.ds(k * rows, rows)]
        every = range(pieces)
        self.sib = sems.remote(lambda: wb.at[0], lambda: wb.at[1], peers.sib)
        self.xp = [sems.remote(piece(0, y, k), piece(2, y, k), peers.xp) for k in every]
        self.fy, self.wy = [], []
        for k in every:
            self.fy.append(sems.remote(piece(2, y, k), piece(2, y, k), peers.yp))
            sems.n -= 1
            self.wy.append(sems.remote(piece(2, 1 - y, k), piece(2, 1 - y, k), peers.yp))
        self.fs = [sems.remote(piece(2, y, k), piece(3, y, k), peers.sib) for k in every]
        self.fs2 = [sems.remote(piece(2, 1 - y, k), piece(3, 1 - y, k), peers.sib) for k in every]

    def start(self):
        for c in self.xp + [self.sib]:
            c().start()

    def forward(self, k):
        self.xp[k]().wait_recv()
        self.fy[k]().start()
        self.fs[k]().start()

    def forward2(self, k):
        self.wy[k]().wait_recv()
        self.fs2[k]().start()

    def arrived(self):
        for c in self.fs + self.fs2:
            c().wait_recv()

    def finish(self):
        for c in [self.sib] + self.xp + self.fy + self.fs + self.fs2:
            c().wait_send()


def turned(src, dst, seq):
    def use(i):
        dst[:, tokens(i, seq)] = src[i].T
    return use


def mlp_first_kernel(layer, y, dz_in, wup, wdn, wq, wo, dy_hbm, g_hbm, wa_g, yb, dzb, yt, dzt, acc, w1t, gt, dht, wb, bounce, dyb, gbuf, *rest):
    slot = pl.program_id(0)
    seqs, seq = yb.shape[:2]
    peers, sems = Peers(), Sems(*rest)
    mine = peers.t * seqs
    loads = [(sems.copies(seqs, lambda i: y.at[layer, mine + i], lambda i: yb.at[i]), turned(yb, yt, seq)),
             (sems.copies(seqs, lambda i: dz_in.at[mine + i], lambda i: dzb.at[i]), turned(dzb, dzt, seq))]
    io = MlpIo(sems, peers, seqs, seq, loads, acc, dzt, dyb, dy_hbm, gbuf, g_hbm)
    own = [sems.copy(lambda w=w: w.at[layer], lambda m=m: wb.at[0, m]) for m, w in enumerate((wup, wdn))]
    blocks = attn_weights(layer, wq, wo, wa_g)
    gather = Gather(sems, peers, [r[:2] for r in blocks])
    hop = Bounce(sems, blocks, bounce)
    spread = Spread(sems, peers, wb, PIECES)

    @pl.when(slot == 0)
    def _():
        with jax.named_scope('e57'):
            for c in own:
                c().start()
        with jax.named_scope('e58'):
            io.start()
        with jax.named_scope('e59'):
            peers.barrier()
        with jax.named_scope('e60'):
            for c in own:
                c().wait()
        with jax.named_scope('e61'):
            spread.start()
        with jax.named_scope('e62'):
            gather.start(range(2))

    @pl.when(slot == 1)
    def _():
        with jax.named_scope('e56'):
            spread.sib().wait_recv()

    @pl.when(slot == 2)
    def _():
        with jax.named_scope('e55'):
            for k in range(5, PIECES):
                spread.forward2(k)

    @pl.when(slot == 3)
    def _():
        with jax.named_scope('e54'):
            spread.arrived()
    every = range(PIECES)
    actions = merge([(14 + k, s) for k, s in enumerate(hop.steps)], ticks('2,3,4,5,7,8,10,11', [functools.partial(spread.forward, k) for k in every]),
                    ticks('7,8,9,10,11', [functools.partial(spread.forward2, k) for k in every]), ticks('21', gather.forwards()))
    mlp_rest(slot, actions, io, wb.at[slot, 0], wb.at[slot, 1], w1t, yt, gt, dht)

    @pl.when(slot == SLOTS - 1)
    def _():
        with jax.named_scope('e50'):
            gather.forward(1)
        with jax.named_scope('e51'):
            io.finish()
        with jax.named_scope('e52'):
            spread.finish()
        with jax.named_scope('e53'):
            gather.finish()


def mlp_first(layer, y, dz, wup, wdn, wq, wo):
    d, f = wup.shape[1:]
    seq = y.shape[2]
    seqs = y.shape[1] // SLOTS
    tok = seqs * seq
    return pl.pallas_call(
        functools.partial(mlp_first_kernel, layer),
        out_shape=(jax.ShapeDtypeStruct((d, tok), BF16), jax.ShapeDtypeStruct((SLOTS, 2, 4, d // 4, f), F32), jax.ShapeDtypeStruct((SLOTS, d, d), BF16)),
        grid=(SLOTS,),
        in_specs=[ANY] * 6,
        out_specs=[ANY] * 3,
        scratch_shapes=[pltpu.VMEM((seqs, seq, d), BF16)] * 2 + [pltpu.VMEM((d, tok), BF16)] * 2
        + [pltpu.VMEM((d, tok), F32), pltpu.VMEM((f, d), BF16), pltpu.VMEM((f, tok), BF16), pltpu.VMEM((f, tok), BF16), pltpu.VMEM((SLOTS, 2, d, f), BF16),
           pltpu.VMEM((d, d), BF16), pltpu.VMEM((d, tok), BF16), pltpu.VMEM((2, 4, d // 4, f), F32)] + SEMS,
        compiler_params=params(0, 1),
        name='mlp_first',
    )(y, dz, wup, wdn, wq, wo)


def mlp_second_kernel(layer, w1_ref, w2_ref, y, dz_in, partial, half, dy_hbm, g_hbm, red, red_half, yb, yt, dzt, acc, w1t, gt, dht, dyb, gbuf, mine, *rest):
    slot = pl.program_id(0)
    seqs, seq = yb.shape[:2]
    bufs, rest = rest[:4], rest[4:]
    peers, sems = Peers(), Sems(*rest[2:])
    place = peers.t * seqs
    loads = [(sems.copies(seqs, lambda i: y.at[layer, place + i], lambda i: yb.at[i]), turned(yb, yt, seq)),
             (sems.copies(seqs, lambda i: dz_in.at[:, tokens(i, seq)], lambda i: dzt.at[:, tokens(i, seq)]), lambda i: None)]
    io = MlpIo(sems, peers, seqs, seq, loads, acc, dzt, dyb, dy_hbm, gbuf, g_hbm)
    rows = mine.shape[2] // 2
    a, b = jobs = [Scatter(sems, peers, lambda s: partial.at[s], lambda x: mine.at[x], bufs, lambda j=j: red.at[pl.ds(j * rows, rows)], (j * rows, rows)) for j in range(2)]

    h0, h1 = rest[:2]
    mine_half = sems.copy(lambda: half.at[0], lambda: h0)
    x_half = sems.remote(lambda: half.at[1], lambda: h1, peers.xp)
    store_half = sems.copy(lambda: h0, lambda: red_half)

    def add_half():
        mine_half().wait()
        x_half().wait_recv()
        h0[...] = (h0[...] + h1[...]) * (1 / SLOTS)

    @pl.when(slot == 0)
    def _():
        with jax.named_scope('e45'):
            io.start()
        with jax.named_scope('e46'):
            peers.barrier()
        with jax.named_scope('e47'):
            for job in jobs:
                job.both('start')
        with jax.named_scope('e48'):
            x_half().start()
        with jax.named_scope('e49'):
            mine_half().start()
    actions = merge(ticks('17,18', [add_half, lambda: store_half().start()]),
                    steps(a, '3add0,4send1,10add1,11send2,18add2,19send3,22add3,23out'),
                    steps(b, '4add0,5send1,16add1,17send2,21add2,22send3'))
    mlp_rest(slot, actions, io, w1_ref.at[0], w2_ref.at[0], w1t, yt, gt, dht)

    @pl.when(slot == SLOTS - 1)
    def _():
        with jax.named_scope('e38'):
            b.add3()
        with jax.named_scope('e39'):
            io.finish()
        with jax.named_scope('e40'):
            x_half().wait_send()
        with jax.named_scope('e41'):
            store_half().wait()
        with jax.named_scope('e42'):
            b.out()
        with jax.named_scope('e43'):
            a.finish()
        with jax.named_scope('e44'):
            b.finish()


def mlp_second(layer, y, dz, w1, w2, partial, half):
    d, f = w1.shape[1:]
    seq = y.shape[2]
    seqs = y.shape[1] // SLOTS
    tok = seqs * seq
    return pl.pallas_call(
        functools.partial(mlp_second_kernel, layer),
        out_shape=(jax.ShapeDtypeStruct((d, tok), BF16), jax.ShapeDtypeStruct((SLOTS, 2, 4, d // 4, f), F32),
                   jax.ShapeDtypeStruct((d // 4, d), F32), jax.ShapeDtypeStruct(half.shape[1:], F32)),
        grid=(SLOTS,),
        in_specs=[leading(d, f), leading(f, d)] + [ANY] * 4,
        out_specs=[ANY] * 4,
        scratch_shapes=[pltpu.VMEM((seqs, seq, d), BF16), pltpu.VMEM((d, tok), BF16), pltpu.VMEM((d, tok), BF16), pltpu.VMEM((d, tok), F32), pltpu.VMEM((f, d), BF16),
                        pltpu.VMEM((f, tok), BF16), pltpu.VMEM((f, tok), BF16), pltpu.VMEM((d, tok), BF16),
                        pltpu.VMEM((2, 4, d // 4, f), F32), pltpu.VMEM((2, 4, d // 4, d), F32)]
        + scatter_bufs(d // 4, d) + [pltpu.VMEM(half.shape[1:], F32)] * 2 + SEMS,
        compiler_params=params(1, 1),
        name='mlp_second',
    )(w1, w2, y, dz, partial, half)


def attn_step(sems, peers, x_ref, dy_hbm, w_hbm, dy_ref, w_ref, xt, acc, gacc, qkv, do, b1, b2, begin, act, emit):
    s, slot = pl.program_id(0), pl.program_id(1)
    step = s * SLOTS + slot
    last = SLOTS * SLOTS - 1
    before = jnp.maximum(step - 1, 0)
    seq, d = x_ref.shape[-2:]
    nqkv = qkv.shape[0]
    third = nqkv // 3
    split = d - b2.shape[1]
    rows = d // 4

    load_w = sems.copies(SLOTS, lambda i: w_hbm.at[i], lambda i: w_ref.at[i])
    load_dy = sems.copies(SLOTS, lambda i: dy_hbm.at[:, tokens(i, seq)], lambda i: dy_ref.at[:, tokens(i, seq)])

    @pl.when(step == 0)
    def _():
        for i in range(SLOTS):
            load_w(i).start()
            load_dy(i).start()
        begin()
        def clear(j, carry):
            gacc[j // 4, j % 4] = jnp.zeros(gacc.shape[2:], F32)
            b1[j % 2] = jnp.zeros(b1.shape[1:], BF16)
            b2[j % 2] = jnp.zeros(b2.shape[1:], BF16)
            return carry
        lax.fori_loop(0, SLOTS * 4, clear, 0)
    act()
    with jax.named_scope('loadw'):
        pl.when(s == 0)(lambda: load_w(slot).wait())

    @pl.when(slot == 0)
    def _():
        with jax.named_scope('e36'):
            load_dy(s).wait()
        with jax.named_scope('e37'):
            xt[s % 2] = x_ref[0, 0].T

    def grads(n, par):
        ps, pj = n // SLOTS, n % SLOTS
        third_d = d // 3

        def weights(c):
            cols = slice(c * third_d, (c + 1) * third_d)
            g = dot(xt[ps % 2], b1[par, cols], NT)
            if c == 2:
                g = g + dot(dy_ref[:, tokens(ps, seq)], b2[par], NT)
            for k in range(4):
                r = peers.rel(k)
                gacc[pj, r, :, cols] = gacc[pj, r, :, cols] + g[k * rows:(k + 1) * rows]

        def inputs(c):
            part = slice(c * third_d, (c + 1) * third_d)
            acc[part] += dot(w_ref[pj, :, part].T, b1[par], NN)
        return [functools.partial(f, c) for c in range(3) for f in (weights, inputs)]
    with jax.named_scope("main"):
        x_t = xt[s % 2]
        dy_t = dy_ref[:, tokens(s, seq)]
        now = step % 2
        qkv[...] = dot(w_ref[slot, pl.ds(0, nqkv), :], x_t, NN).astype(BF16)
        do[...] = dot(w_ref[slot, pl.ds(nqkv, d - nqkv), :], dy_t, NN).astype(BF16)
        scale = HEAD ** -0.5
        exp_scale = scale * math.log2(math.e)
        qb = seq // 2
        units = [(h, slice(c * qb, (c + 1) * qb)) for h in range(third // HEAD) for c in range(2)]

        def scores(h, qc):
            q_rows, k_rows, v_rows = head_rows(h)
            return dot(qkv[k_rows, :].T, qkv[q_rows, qc], NN), dot(qkv[v_rows, :].T, do[q_rows, qc] * scale, NN)

        def head_rows(h):
            return [slice(i * third + h * HEAD, i * third + (h + 1) * HEAD) for i in range(3)]
        for piece in grads(before, 1 - step % 2):
            piece()
        ahead = [scores(*unit) for unit in units[:LOOK_AHEAD]]
        for n, (h, qc) in enumerate(units):
            sc, dp_t = ahead.pop(0)
            if n + LOOK_AHEAD < len(units):
                ahead.append(scores(*units[n + LOOK_AHEAD]))
            q_rows, k_rows, v_rows = head_rows(h)
            m = jnp.max(sc, axis=0, keepdims=True)
            e = jnp.exp2((sc - m) * exp_scale)
            inv = 1.0 / jnp.sum(e, axis=0, keepdims=True)
            rd = jnp.sum(e * dp_t, axis=0, keepdims=True) * inv
            p = e * inv
            p_bf = p.astype(BF16)
            ds = (p * (dp_t - rd)).astype(BF16)
            b2[now, pl.ds(b2.shape[1] - third + h * HEAD, HEAD), qc] = dot(qkv[v_rows, :], p_bf, NN).astype(BF16)
            b1[now, q_rows, qc] = dot(qkv[k_rows, :], ds, NN).astype(BF16)
            dv_c = dot(do[q_rows, qc], p_bf, NT)
            dk_c = dot(qkv[q_rows, qc], ds, NT)
            if n % 2 == 0:
                dv, dk = dv_c, dk_c
            else:
                b1[now, k_rows] = (dk + dk_c).astype(BF16)
                b1[now, v_rows] = (dv + dv_c).astype(BF16)

    @pl.when(slot == 0)
    def _():
        @pl.when(s > 0)
        def _():
            emit(s - 1)
        acc[...] = dy_ref[:, tokens(s, seq)].astype(F32)

    @pl.when(step == last)
    def _():
        with jax.named_scope('e34'):
            for piece in grads(last, last % 2):
                piece()
        with jax.named_scope('e35'):
            emit(s)


ATTN_IN = 3
ATTN_SCRATCH = 9
JOB_PLAN = '1add0,2send1,7add1,8send2,12add2', '2add0,3send1x,8send1y,10add1x,11send2x,14add1y,15send2y'


def attn_first_kernel(layer, x_ref, dy_hbm, w_hbm, partial, wup, wdn, wq, wo, dx_hbm, g_hbm, w1_g, w2_g, wa_g, half, *rest):
    body, rest = rest[:ATTN_SCRATCH], rest[ATTN_SCRATCH:]
    acc, gacc, mine, bounce = body[3], body[4], rest[:2], rest[-4]
    seq = x_ref.shape[-2]
    step = pl.program_id(0) * SLOTS + pl.program_id(1)
    peers, sems = Peers(), Sems(*rest[-3:])
    a, b = jobs = [Scatter(sems, peers, lambda s, j=j: partial.at[s, j], lambda x, j=j: mine[j].at[x], rest[2 + 4 * j:6 + 4 * j], None,
                           (0, half.shape[2]), half_out=lambda x, j=j: half.at[x, j]) for j in range(2)]
    blocks = [(lambda w=w: w.at[layer - 1], lambda j, g=g: g.at[j], wup.shape[1]) for w, g in ((wup, w1_g), (wdn, w2_g))] + attn_weights(layer - 1, wq, wo, wa_g)
    gather = Gather(sems, peers, [r[:2] for r in blocks])
    hop = Bounce(sems, blocks, bounce)
    stores = [sems.copy(lambda j=j: gacc.at[j], lambda j=j: g_hbm.at[j]) for j in range(SLOTS)]
    actions = merge(steps(a, JOB_PLAN[0]), steps(b, JOB_PLAN[1]), [(5 + k, s) for k, s in enumerate(hop.steps)],
                    ticks('6,11,15', gather.forwards()), ticks('14,15', [lambda c=c: c().start() for c in stores]))

    dxb = rest[-5]
    store_dx = sems.copies(SLOTS, lambda i: dxb.at[i], lambda i: dx_hbm.at[:, tokens(i, seq)])

    def begin():
        peers.barrier()
        for job in jobs:
            job.both('start')
        gather.start(range(len(blocks)))

    def emit(s):
        dxb[s] = acc[...].astype(BF16)
        store_dx(s).start()
    attn_step(sems, peers, x_ref, dy_hbm, w_hbm, *body, begin, lambda: at_ticks(actions, step), emit)

    @pl.when(step == SLOTS * SLOTS - 1)
    def _():
        with jax.named_scope('e25'):
            for c in stores[2:]:
                c().start()
        with jax.named_scope('e26'):
            gather.forward(3)
        with jax.named_scope('e27'):
            a.out()
        with jax.named_scope('e28'):
            b.both('add2')
        with jax.named_scope('e29'):
            gather.finish()
        with jax.named_scope('e30'):
            for c in stores:
                c().wait()
        with jax.named_scope('e31'):
            b.out()
        with jax.named_scope('e32'):
            for i in range(SLOTS):
                store_dx(i).wait()
        with jax.named_scope('e33'):
            for job in jobs:
                job.finish()


def attn_last_kernel(x_ref, dy_hbm, w_hbm, partial, dxg, red, red_last, *rest):
    body, rest = rest[:ATTN_SCRATCH], rest[ATTN_SCRATCH:]
    acc, gacc, mine, dxb, free = body[3], body[4], rest[:2], rest[-5], rest[-4]
    step = pl.program_id(0) * SLOTS + pl.program_id(1)
    seqs = pl.num_programs(0)
    peers, sems = Peers(), Sems(*rest[-3:])
    nred = red.shape[1]
    a, b = jobs = [Scatter(sems, peers, lambda s, j=j: partial.at[s, j], lambda x, j=j: mine[j].at[x], rest[2 + 4 * j:6 + 4 * j], lambda j=j: red.at[j],
                           (0, nred)) for j in range(2)]
    h = nred // 2
    ends = [Scatter(sems, peers, lambda s: gacc.at[s], lambda x: gacc.at[2 * x], rest[2:6], lambda j=j: red_last.at[pl.ds(j * h, h)], (j * h, h), load=False)
            for j in range(2)]
    t = peers.t
    t2 = (t + 2) % SLOTS
    sib, xp, fwd, mine_dx = [], [], [], []
    for s in range(SLOTS):
        def src(s=s):
            return dxb.at[s]

        def dst(s=s):
            return dxg.at[t * SLOTS + s]

        def other(s=s):
            return dxg.at[t2 * SLOTS + s]
        mine_dx.append(sems.copy(src, dst))
        sib.append(sems.remote(src, dst, peers.sib))
        xp.append(sems.remote(src, dst, peers.xp))
        fwd.append(sems.remote(other, other, peers.sib))

    def freed(i):
        for peer in ([peers.sib], [peers.yp, peers.zp], [peers.yp, peers.zp], [peers.xp])[i]:
            pl.semaphore_signal(free.at[i], inc=1, device_id=peer, device_id_type=MESH)

    def forward(s):
        xp[s]().wait_recv()
        fwd[s]().start()

    def early():
        pl.semaphore_wait(free.at[0], 1)
        for job in ends:
            job.start(0)
    actions = merge(steps(a, '1add0y,2send1y,5add1y,6send2y,9add2y,10send3,12add1x,13send2x'), steps(b, '1add0y,2send1y,7add1y,8send2y,10add2y,11send3,14add1x,15send2x'),
                    *[steps(job, '2add0x,8send1x') for job in jobs],
                    ticks('3,13,9,14,15', [functools.partial(freed, i) for i in range(2)] + [functools.partial(forward, i) for i in range(2)] + [early]))

    def begin():
        peers.barrier()
        for x in (1, 0):
            for job in jobs:
                job.start(x)

    def emit(s):
        dxb[s] = acc[...].T.astype(BF16)
        for k in range(SLOTS):
            @pl.when(s == k)
            def _(k=k):
                for c in (xp, sib, mine_dx):
                    c[k]().start()
    attn_step(sems, peers, x_ref, dy_hbm, w_hbm, *body, begin, lambda: at_ticks(actions, step), emit)

    @pl.when(step == SLOTS * SLOTS - 1)
    def _():
        with jax.named_scope('e1'):
            for job in ends:
                job.start(1)
                job.add0(0)
        with jax.named_scope('e2'):
            pl.semaphore_wait(free.at[1], 2)
        with jax.named_scope('e3'):
            a.add2(0)
        with jax.named_scope('e4'):
            freed(2)
        with jax.named_scope('e5'):
            for job in ends:
                job.send1(0)
        with jax.named_scope('e6'):
            a.add3()
        with jax.named_scope('e7'):
            freed(3)
        with jax.named_scope('e8'):
            for job in ends:
                job.add0(1)
        with jax.named_scope('e9'):
            a.out()
        with jax.named_scope('e10'):
            b.add2(0)
        with jax.named_scope('e11'):
            for job in ends:
                job.send1(1)
        with jax.named_scope('e12'):
            b.add3()
        with jax.named_scope('e13'):
            b.out()
        with jax.named_scope('e14'):
            pl.semaphore_wait(free.at[2], 2)
        with jax.named_scope('e15'):
            pl.semaphore_wait(free.at[3], 1)
        with jax.named_scope('e16'):
            for job in ends:
                job.add1(0)
                job.send2(0)
        with jax.named_scope('e17'):
            forward(2)
        with jax.named_scope('e18'):
            for job in ends:
                job.add1(1)
                job.send2(1)
        with jax.named_scope('e19'):
            for job in ends:
                job.both('add2')
                job.send3()
        with jax.named_scope('e20'):
            forward(3)
        with jax.named_scope('e21'):
            for s in range(SLOTS):
                mine_dx[s]().wait()
                sib[s]().wait()
                xp[s]().wait_send()
        with jax.named_scope('e22'):
            for job in ends:
                job.add3()
                job.out()
        with jax.named_scope('e23'):
            for s in range(SLOTS):
                fwd[s]().wait()
        with jax.named_scope('e24'):
            for job in jobs + ends:
                job.finish()


def attn_specs(layer, x, w):
    slots, nw, d = w.shape
    seq = x.shape[2]
    seqs = x.shape[1] // slots
    tok = seqs * seq
    nqkv = nw * 3 // 4
    in_specs = [pl.BlockSpec((1, 1, seq, d), lambda s, j: (layer, lax.axis_index('tp') * seqs + s, 0, 0))] + [ANY] * 3
    scratch = [pltpu.VMEM((d, tok), BF16), pltpu.VMEM((slots, nw, d), BF16), pltpu.VMEM((2, d, seq), BF16), pltpu.VMEM((d, seq), F32), pltpu.VMEM((slots, 4, d // 4, nw), F32), pltpu.VMEM((nqkv, seq), BF16),
               pltpu.VMEM((nw - nqkv, seq), BF16), pltpu.VMEM((2, nw, seq), BF16), pltpu.VMEM((2, d // 3, seq), BF16)]
    scratch += [pltpu.VMEM((2, 4, d // 4, d), F32)] * 2 + scatter_bufs(d // 4, d) * 2
    red = jax.ShapeDtypeStruct((2, d // 4, d), F32)
    return (slots, seqs), in_specs, scratch, red, tok


def attn_first(layer, x, dy, w, partial, *weights):
    grid, in_specs, scratch, red, tok = attn_specs(layer, x, w)
    slots, nw, d = w.shape
    gathered = [jax.ShapeDtypeStruct((slots, d, d), BF16)] * 3
    return pl.pallas_call(
        functools.partial(attn_first_kernel, layer),
        out_shape=[jax.ShapeDtypeStruct((d, tok), BF16), jax.ShapeDtypeStruct((slots, 4, d // 4, nw), F32)] + gathered + [jax.ShapeDtypeStruct((2,) + red.shape, F32)],
        grid=grid,
        in_specs=in_specs + [ANY] * len(weights),
        out_specs=[ANY] * 6,
        scratch_shapes=scratch + [pltpu.VMEM((slots, d, tok // slots), BF16), pltpu.VMEM((d, d), BF16)] + SEMS,
        compiler_params=params(2, 2),
        name='attn_first',
    )(x, dy, w, partial, *weights)


def attn_last(layer, x, dy, w, partial):
    grid, in_specs, scratch, red, tok = attn_specs(layer, x, w)
    slots, nw, d = w.shape
    seq = x.shape[2]
    return pl.pallas_call(
        attn_last_kernel,
        out_shape=[jax.ShapeDtypeStruct((x.shape[1], seq, d), BF16), red, jax.ShapeDtypeStruct(red.shape[1:], F32)],
        grid=grid,
        in_specs=in_specs,
        out_specs=[ANY] * 3,
        scratch_shapes=scratch + [pltpu.VMEM((slots, seq, d), BF16), pltpu.SemaphoreType.REGULAR((4,))] + SEMS,
        compiler_params=params(3, 2),
        name='attn_last',
    )(x, dy, w, partial)


def solution(mesh):
    assert dict(mesh.shape) == {'dpy': 2, 'dpx': 2, 'tp': SLOTS}
    act_spec = P(None, DATA_AXES, None, None)

    def device_backward(x_saved, y_saved, dz_top, w_qkv, w_out, w_up, w_down):
        layers, d = w_up.shape[:2]
        assert layers == 2
        heads, hd = w_out.shape[1:3]
        n = 3 * heads * hd
        wq = w_qkv.transpose(0, 2, 3, 4, 1).reshape(layers, n, d)
        wo = w_out.reshape(layers, heads * hd, d)
        dy1, gm1, wa1 = mlp_first(1, y_saved, dz_top, w_up, w_down, wq, wo)
        dx1, ga1, w1_0, w2_0, wa0, half = attn_first(1, x_saved, dy1, wa1, gm1, w_up, w_down, wq, wo)
        dy0, gm0, ra1, rm1 = mlp_second(0, y_saved, dx1, w1_0, w2_0, ga1, half)
        d_input, rm0, ra0 = attn_last(0, x_saved, dy0, wa0, gm0)
        g_a = jnp.stack([ra0, ra1])
        g_qkv = g_a[:, :, :n].reshape(layers, d // 4, 3, heads, hd)
        g_out = g_a[:, :, n:].transpose(0, 2, 1).reshape(layers, heads, hd, d // 4)
        return d_input, g_qkv, g_out, jnp.stack([rm0[1], rm1[1]]), jnp.stack([rm0[0], rm1[0]])

    tp_last = P(None, None, None, 'tp', None), P(None, 'tp', None, None), P(None, None, 'tp'), P(None, 'tp', None)
    return jax.shard_map(device_backward, mesh=mesh,
                         in_specs=(act_spec, act_spec, P(DATA_AXES, None, None)) + tp_last,
                         out_specs=(P(DATA_AXES, None, None), P(None, DATA_AXES, None, 'tp', None), P(None, 'tp', None, DATA_AXES), P(None, DATA_AXES, 'tp'), P(None, ('tp', 'dpy', 'dpx'), None)),
                         check_vma=False)
```

```python
import functools
import math
import re

import jax
import jax.numpy as jnp
from jax import lax
from jax.experimental import pallas as pl
from jax.experimental.pallas import tpu as pltpu
from jax.sharding import PartitionSpec as P

DATA_AXES = ('dpy', 'dpx')
F32 = jnp.float32
BF16 = jnp.bfloat16
HEAD = 64
SLOTS = 4
LOOK_AHEAD = 3
PIECES = 8
NN = (((1,), (0,)), ((), ()))
NT = (((1,), (1,)), ((), ()))
VMEM_LIMIT = 63 * 1024 * 1024
MESH = pl.DeviceIdType.MESH
ANY = pl.BlockSpec(memory_space=pl.ANY)


def dot(a, b, dims):
    return lax.dot_general(a, b, dims, preferred_element_type=F32)


class Peers:
    def __init__(self):
        z, y, t = lax.axis_index('dpy'), lax.axis_index('dpx'), lax.axis_index('tp')
        self.z, self.y, self.t = z, y, t
        self.sib = (z, y, t + 1 - 2 * (t % 2))
        self.xp = (z, y, (t + 2) % 4)
        self.yp = (z, 1 - y, t)
        self.zp = (1 - z, y, t)

    def barrier(self):
        sem = pltpu.get_barrier_semaphore()
        with jax.named_scope('entry'):
            for peer in (self.sib, self.xp, self.yp, self.zp):
                pl.semaphore_signal(sem, inc=1, device_id=peer, device_id_type=MESH)
            pl.semaphore_wait(sem, 4)

    def rel(self, d):
        zr = self.z if d // 2 == 0 else 1 - self.z
        yr = self.y if d % 2 == 0 else 1 - self.y
        return zr * 2 + yr


class Sems:
    def __init__(self, send, recv, local):
        self.send, self.recv, self.local = send, recv, local
        self.n = self.m = 0

    def remote(self, src, dst, peer):
        i = self.n
        self.n += 1
        return lambda: pltpu.make_async_remote_copy(src_ref=src(), dst_ref=dst(), send_sem=self.send.at[i], recv_sem=self.recv.at[i],
                                                    device_id=peer, device_id_type=MESH)

    def copy(self, src, dst):
        i = self.m
        self.m += 1
        return lambda: pltpu.make_async_copy(src(), dst(), self.local.at[i])

    def copies(self, n, src, dst):
        first = self.m
        self.m += n
        return lambda i: pltpu.make_async_copy(src(i), dst(i), self.local.at[first + i])


def at_ticks(actions, tick, position=0, points=1):
    for k in sorted(actions):
        if k % points == position:
            @pl.when(tick == k)
            def _(k=k):
                with jax.named_scope('t%d' % k):
                    for action in actions[k]:
                        action()


class Scatter:
    def __init__(self, sems, peers, partial, mine, bufs, out, rows, load=True, half_out=None):
        r0, r1, r2, r3 = self.bufs = bufs
        first, count = rows
        h = count // 2
        self.mine, self.all, self.lo, self.hi = mine, pl.ds(first, count), pl.ds(first, h), pl.ds(first + h, h)
        self.half = half = pl.ds(first // 2, h)
        every, lo, hi = self.all, self.lo, self.hi
        self.load, self.c0, self.c1, self.c2 = [], [], [], []
        for x in range(2):
            def near(k, part, x=x):
                return lambda: mine(x).at[k, part]

            def place(buf, *index):
                return lambda: buf.at[index]
            if load:
                self.load.append(sems.copy(lambda x=x: partial(2 * x).at[:, every], near(slice(None), every)))
            self.c0.append(sems.remote(lambda x=x: partial(2 * x + 1).at[:, every], place(r0, x, slice(None), every), peers.sib))
            self.c1.append([sems.remote(near(2 * k + 1, lo), place(r1, 0, x, k, half), peers.yp) for k in range(2)]
                           + [sems.remote(near(2 + k, hi), place(r1, 1, x, k, half), peers.zp) for k in range(2)])
            self.c2.append([sems.remote(near(2, lo), place(r2, 0, x, half), peers.zp), sems.remote(near(1, hi), place(r2, 1, x, half), peers.yp)])
        if half_out is None:
            self.c3 = sems.remote(lambda: mine(1).at[0, every], place(r3, every), peers.xp)
            self.store = [sems.copy(lambda: mine(0).at[0, every], out)]
        else:
            self.c3 = None
            self.store = [sems.copy(lambda x=x: mine(x).at[0, every], lambda x=x: half_out(x)) for x in range(2)]

    def start(self, x):
        self.c0[x]().start()
        if self.load:
            self.load[x]().start()

    def add0(self, x):
        if self.load:
            self.load[x]().wait()
        self.c0[x]().wait_recv()
        mine, r0 = self.mine(x), self.bufs[0].at[x]

        def body(k, carry):
            mine[k, self.all] = mine[k, self.all] + r0[k, self.all]
            return carry
        lax.fori_loop(0, 4, body, 0)

    def send1(self, x):
        for c in self.c1[x]:
            c().start()

    def add1(self, x):
        for c in self.c1[x]:
            c().wait_recv()
        mine, r1 = self.mine(x), self.bufs[1]

        def body(k, carry):
            mine[2 * k, self.lo] = mine[2 * k, self.lo] + r1[0, x, k, self.half]
            mine[k, self.hi] = mine[k, self.hi] + r1[1, x, k, self.half]
            return carry
        lax.fori_loop(0, 2, body, 0)

    def send2(self, x):
        for c in self.c2[x]:
            c().start()

    def add2(self, x):
        for c in self.c2[x]:
            c().wait_recv()
        mine, r2 = self.mine(x), self.bufs[2]
        mine[0, self.lo] = mine[0, self.lo] + r2[0, x, self.half]
        mine[0, self.hi] = mine[0, self.hi] + r2[1, x, self.half]

    def send3(self):
        self.c3().start()

    def add3(self):
        self.c3().wait_recv()
        mine = self.mine(0)
        mine[0, self.all] = (mine[0, self.all] + self.bufs[3][self.all]) * (1 / SLOTS)

    def out(self):
        for c in self.store:
            c().start()

    def finish(self):
        for c in self.c0 + sum(self.c1, []) + sum(self.c2, []) + ([self.c3] if self.c3 else []):
            c().wait_send()
        for c in self.store:
            c().wait()

    def both(self, name):
        for x in range(2):
            getattr(self, name)(x)


def scatter_bufs(rows, d):
    return [pltpu.VMEM((2, 4, rows, d), F32), pltpu.VMEM((2, 2, 2, rows // 2, d), F32), pltpu.VMEM((2, 2, rows // 2, d), F32), pltpu.VMEM((rows, d), F32)]


def steps(job, plan):
    out = []
    for tick, name, half in re.findall('([0-9]+)([a-z]+[0-3]?)([xy]?)', plan):
        if half:
            action = functools.partial(getattr(job, name), int(half == 'y'))
        else:
            action = functools.partial(job.both, name) if name[-1] in '012' else getattr(job, name)
        out.append((int(tick), action))
    return out


def ticks(plan, actions):
    return list(zip(map(int, plan.split(',')), actions))


class Gather:
    def __init__(self, sems, peers, blocks):
        self.sib = [sems.remote(own, lambda dst=dst: dst(1), peers.sib) for own, dst in blocks]
        self.xp = [sems.remote(own, lambda dst=dst: dst(2), peers.xp) for own, dst in blocks]
        self.fwd = [sems.remote(lambda dst=dst: dst(2), lambda dst=dst: dst(3), peers.sib) for own, dst in blocks]

    def start(self, blocks):
        for i in blocks:
            self.sib[i]().start()
            self.xp[i]().start()

    def forward(self, i):
        self.xp[i]().wait_recv()
        self.fwd[i]().start()

    def forwards(self):
        return [functools.partial(self.forward, i) for i in range(len(self.fwd))]

    def finish(self):
        for i in range(len(self.sib)):
            self.sib[i]().wait_recv()
            self.fwd[i]().wait_recv()
            self.sib[i]().wait_send()
            self.xp[i]().wait_send()
            self.fwd[i]().wait_send()


class Bounce:
    def __init__(self, sems, items, buf):
        self.steps = []
        prev = None
        for own, dst, rows in items:
            ld = sems.copy(own, lambda rows=rows: buf.at[pl.ds(0, rows)])
            st = sems.copy(lambda rows=rows: buf.at[pl.ds(0, rows)], lambda dst=dst: dst(0))
            self.steps.append(functools.partial(self.load, prev, ld))
            self.steps.append(functools.partial(self.flip, ld, st))
            prev = st
        self.steps.append(lambda prev=prev: prev().wait())

    @staticmethod
    def load(prev, ld):
        if prev is not None:
            prev().wait()
        ld().start()

    @staticmethod
    def flip(ld, st):
        ld().wait()
        st().start()


def merge(*lists):
    actions = {}
    for pairs in lists:
        for k, action in pairs:
            actions.setdefault(k, []).append(action)
    return actions


SEMS = [pltpu.SemaphoreType.DMA((96,)), pltpu.SemaphoreType.DMA((96,)), pltpu.SemaphoreType.DMA((32,))]


def leading(*shape):
    return pl.BlockSpec((1,) + shape, lambda j, *_: (j,) + (0,) * len(shape))


def params(collective_id, axes):
    return pltpu.CompilerParams(vmem_limit_bytes=VMEM_LIMIT, dimension_semantics=('arbitrary',) * axes, collective_id=collective_id, has_side_effects=True)


def mlp_slot(slot, seqs, seq, w1, w2, w1t, yt, dz, acc, gt, dht, tick, arrive, emit):
    w1t[...] = w1[...].T

    def block(i, carry):
        tick(i)
        with jax.named_scope('arrive'):
            pl.when(slot == 0)(lambda: arrive(i))
        cols = pl.ds(pl.multiple_of(i * seq, seq), seq)
        h = dot(w1t[...], yt[:, cols], NN)
        dg = dot(w2[...], dz[:, cols], NN)
        c0 = math.sqrt(2 / math.pi)
        c1 = 0.044715 * c0
        h2 = h * h
        t = jnp.tanh(h * (c0 + c1 * h2))
        q = 0.5 * t + 0.5
        g = h * q
        dh = dg * (q + (g * (1.0 - t)) * (c0 + (3 * c1) * h2))
        gt[:, cols] = g.astype(BF16)
        dh = dh.astype(BF16)
        dht[:, cols] = dh
        acc[:, cols] += dot(w1[...], dh, NN)
        with jax.named_scope('memit'):
            pl.when(slot == SLOTS - 1)(lambda: emit(i))
        return carry
    lax.fori_loop(0, seqs, block, 0)


def tokens(i, seq):
    return pl.ds(pl.multiple_of(i * seq, seq), seq)


class MlpIo:
    def __init__(self, sems, peers, seqs, seq, loads, acc, dz, dyb, dy_hbm, gbuf, g_hbm):
        self.seqs, self.seq, self.peers = seqs, seq, peers
        self.loads, self.acc, self.dz, self.dyb, self.gbuf = loads, acc, dz, dyb, gbuf
        self.dy = sems.copies(seqs, lambda i: dyb.at[:, tokens(i, seq)], lambda i: dy_hbm.at[:, tokens(i, seq)])
        self.g = [sems.copy(lambda j=j: gbuf.at[j], lambda j=j: g_hbm.at[pl.program_id(0), j]) for j in range(2)]

    def start(self):
        for load, _ in self.loads:
            for i in range(self.seqs):
                load(i).start()

    def arrive(self, i):
        for load, use in self.loads:
            load(i).wait()
            use(i)
        cols = tokens(i, self.seq)
        self.acc[:, cols] = jnp.zeros((self.acc.shape[0], self.seq), F32)

    def emit(self, i):
        cols = tokens(i, self.seq)
        self.dyb[:, cols] = (self.dz[:, cols].astype(F32) + self.acc[:, cols]).astype(BF16)
        self.dy(i).start()

    def grads(self, j, a, b):
        pl.when(pl.program_id(0) > 0)(lambda: self.g[j]().wait())
        rows, width = self.gbuf.shape[-2:]
        split, half = width * 2 // 3, width // 2
        for lo, hi, c0, c1 in ((0, width, 0, split), (0, half, split, width), (half, width, split, width)):
            g = dot(a[lo:hi], b[c0:c1], NT)
            for k in range(g.shape[0] // rows):
                self.gbuf[j, self.peers.rel(lo // rows + k), :, c0:c1] = g[k * rows:(k + 1) * rows]
        self.g[j]().start()

    def finish(self):
        for i in range(self.seqs):
            self.dy(i).wait()
        for c in self.g:
            c().wait()


def mlp_rest(slot, actions, io, w1, w2, w1t, yt, gt, dht):
    seqs, seq, dz, acc = io.seqs, io.seq, io.dz, io.acc
    points = seqs + 2
    first = slot * points

    def tick(i):
        at_ticks({k: v for k, v in actions.items() if k % points < seqs}, first + i)
    mlp_slot(slot, seqs, seq, w1, w2, w1t, yt, dz, acc, gt, dht, tick, io.arrive, io.emit)
    at_ticks(actions, first + seqs, seqs, points)
    with jax.named_scope('dw2'):
        io.grads(0, gt, dz)
    at_ticks(actions, first + seqs + 1, seqs + 1, points)
    with jax.named_scope('dw1'):
        io.grads(1, yt, dht)


def attn_weights(layer, wq, wo, wa_g):
    nq, d = wq.shape[1:]
    return [(lambda: wq.at[layer], lambda j: wa_g.at[j, pl.ds(0, nq)], nq), (lambda: wo.at[layer], lambda j: wa_g.at[j, pl.ds(nq, d - nq)], d - nq)]


class Spread:
    def __init__(self, sems, peers, wb, pieces):
        rows = wb.shape[2] // pieces
        y = peers.y

        def piece(slot, m, k):
            return lambda: wb.at[slot, m, pl.ds(k * rows, rows)]
        every = range(pieces)
        self.sib = sems.remote(lambda: wb.at[0], lambda: wb.at[1], peers.sib)
        self.xp = [sems.remote(piece(0, y, k), piece(2, y, k), peers.xp) for k in every]
        self.fy, self.wy = [], []
        for k in every:
            self.fy.append(sems.remote(piece(2, y, k), piece(2, y, k), peers.yp))
            sems.n -= 1
            self.wy.append(sems.remote(piece(2, 1 - y, k), piece(2, 1 - y, k), peers.yp))
        self.fs = [sems.remote(piece(2, y, k), piece(3, y, k), peers.sib) for k in every]
        self.fs2 = [sems.remote(piece(2, 1 - y, k), piece(3, 1 - y, k), peers.sib) for k in every]

    def start(self):
        for c in self.xp + [self.sib]:
            c().start()

    def forward(self, k):
        self.xp[k]().wait_recv()
        self.fy[k]().start()
        self.fs[k]().start()

    def forward2(self, k):
        self.wy[k]().wait_recv()
        self.fs2[k]().start()

    def arrived(self):
        for c in self.fs + self.fs2:
            c().wait_recv()

    def finish(self):
        for c in [self.sib] + self.xp + self.fy + self.fs + self.fs2:
            c().wait_send()


def turned(src, dst, seq):
    def use(i):
        dst[:, tokens(i, seq)] = src[i].T
    return use


def mlp_first_kernel(layer, y, dz_in, wup, wdn, wq, wo, dy_hbm, g_hbm, wa_g, yb, dzb, yt, dzt, acc, w1t, gt, dht, wb, bounce, dyb, gbuf, *rest):
    slot = pl.program_id(0)
    seqs, seq = yb.shape[:2]
    peers, sems = Peers(), Sems(*rest)
    mine = peers.t * seqs
    loads = [(sems.copies(seqs, lambda i: y.at[layer, mine + i], lambda i: yb.at[i]), turned(yb, yt, seq)),
             (sems.copies(seqs, lambda i: dz_in.at[mine + i], lambda i: dzb.at[i]), turned(dzb, dzt, seq))]
    io = MlpIo(sems, peers, seqs, seq, loads, acc, dzt, dyb, dy_hbm, gbuf, g_hbm)
    own = [sems.copy(lambda w=w: w.at[layer], lambda m=m: wb.at[0, m]) for m, w in enumerate((wup, wdn))]
    blocks = attn_weights(layer, wq, wo, wa_g)
    gather = Gather(sems, peers, [r[:2] for r in blocks])
    hop = Bounce(sems, blocks, bounce)
    spread = Spread(sems, peers, wb, PIECES)

    @pl.when(slot == 0)
    def _():
        with jax.named_scope('e56'):
            for c in own:
                c().start()
        with jax.named_scope('e57'):
            io.start()
        with jax.named_scope('e58'):
            peers.barrier()
        with jax.named_scope('e59'):
            for c in own:
                c().wait()
        with jax.named_scope('e60'):
            spread.start()
        with jax.named_scope('e61'):
            gather.start(range(2))

    @pl.when(slot == 1)
    def _():
        with jax.named_scope('e55'):
            spread.sib().wait_recv()

    @pl.when(slot == 2)
    def _():
        with jax.named_scope('e54'):
            for k in range(5, PIECES):
                spread.forward2(k)

    @pl.when(slot == 3)
    def _():
        with jax.named_scope('e53'):
            spread.arrived()
    every = range(PIECES)
    actions = merge([(14 + k, s) for k, s in enumerate(hop.steps)], ticks('2,3,4,5,7,8,10,11', [functools.partial(spread.forward, k) for k in every]),
                    ticks('7,8,9,10,11', [functools.partial(spread.forward2, k) for k in every]), ticks('21', gather.forwards()))
    mlp_rest(slot, actions, io, wb.at[slot, 0], wb.at[slot, 1], w1t, yt, gt, dht)

    @pl.when(slot == SLOTS - 1)
    def _():
        with jax.named_scope('e49'):
            gather.forward(1)
        with jax.named_scope('e50'):
            io.finish()
        with jax.named_scope('e51'):
            spread.finish()
        with jax.named_scope('e52'):
            gather.finish()


def mlp_first(layer, y, dz, wup, wdn, wq, wo):
    d, f = wup.shape[1:]
    seq = y.shape[2]
    seqs = y.shape[1] // SLOTS
    tok = seqs * seq
    return pl.pallas_call(
        functools.partial(mlp_first_kernel, layer),
        out_shape=(jax.ShapeDtypeStruct((d, tok), BF16), jax.ShapeDtypeStruct((SLOTS, 2, 4, d // 4, f), F32), jax.ShapeDtypeStruct((SLOTS, d, d), BF16)),
        grid=(SLOTS,),
        in_specs=[ANY] * 6,
        out_specs=[ANY] * 3,
        scratch_shapes=[pltpu.VMEM((seqs, seq, d), BF16)] * 2 + [pltpu.VMEM((d, tok), BF16)] * 2
        + [pltpu.VMEM((d, tok), F32), pltpu.VMEM((f, d), BF16), pltpu.VMEM((f, tok), BF16), pltpu.VMEM((f, tok), BF16), pltpu.VMEM((SLOTS, 2, d, f), BF16),
           pltpu.VMEM((d, d), BF16), pltpu.VMEM((d, tok), BF16), pltpu.VMEM((2, 4, d // 4, f), F32)] + SEMS,
        compiler_params=params(0, 1),
        name='mlp_first',
    )(y, dz, wup, wdn, wq, wo)


def mlp_second_kernel(layer, w1_ref, w2_ref, y, dz_in, partial, half, dy_hbm, g_hbm, red, red_half, yb, yt, dzt, acc, w1t, gt, dht, dyb, gbuf, mine, *rest):
    slot = pl.program_id(0)
    seqs, seq = yb.shape[:2]
    bufs, rest = rest[:4], rest[4:]
    peers, sems = Peers(), Sems(*rest[2:])
    place = peers.t * seqs
    loads = [(sems.copies(seqs, lambda i: y.at[layer, place + i], lambda i: yb.at[i]), turned(yb, yt, seq)),
             (sems.copies(seqs, lambda i: dz_in.at[:, tokens(i, seq)], lambda i: dzt.at[:, tokens(i, seq)]), lambda i: None)]
    io = MlpIo(sems, peers, seqs, seq, loads, acc, dzt, dyb, dy_hbm, gbuf, g_hbm)
    rows = mine.shape[2] // 2
    a, b = jobs = [Scatter(sems, peers, lambda s: partial.at[s], lambda x: mine.at[x], bufs, lambda j=j: red.at[pl.ds(j * rows, rows)], (j * rows, rows)) for j in range(2)]

    h0, h1 = rest[:2]
    mine_half = sems.copy(lambda: half.at[0], lambda: h0)
    x_half = sems.remote(lambda: half.at[1], lambda: h1, peers.xp)
    store_half = sems.copy(lambda: h0, lambda: red_half)

    def add_half():
        mine_half().wait()
        x_half().wait_recv()
        h0[...] = (h0[...] + h1[...]) * (1 / SLOTS)

    @pl.when(slot == 0)
    def _():
        with jax.named_scope('e44'):
            io.start()
        with jax.named_scope('e45'):
            peers.barrier()
        with jax.named_scope('e46'):
            for job in jobs:
                job.both('start')
        with jax.named_scope('e47'):
            x_half().start()
        with jax.named_scope('e48'):
            mine_half().start()
    actions = merge(ticks('17,18', [add_half, lambda: store_half().start()]),
                    steps(a, '3add0,4send1,10add1,11send2,18add2,19send3,22add3,23out'),
                    steps(b, '4add0,5send1,16add1,17send2,21add2,22send3'))
    mlp_rest(slot, actions, io, w1_ref.at[0], w2_ref.at[0], w1t, yt, gt, dht)

    @pl.when(slot == SLOTS - 1)
    def _():
        with jax.named_scope('e37'):
            b.add3()
        with jax.named_scope('e38'):
            io.finish()
        with jax.named_scope('e39'):
            x_half().wait_send()
        with jax.named_scope('e40'):
            store_half().wait()
        with jax.named_scope('e41'):
            b.out()
        with jax.named_scope('e42'):
            a.finish()
        with jax.named_scope('e43'):
            b.finish()


def mlp_second(layer, y, dz, w1, w2, partial, half):
    d, f = w1.shape[1:]
    seq = y.shape[2]
    seqs = y.shape[1] // SLOTS
    tok = seqs * seq
    return pl.pallas_call(
        functools.partial(mlp_second_kernel, layer),
        out_shape=(jax.ShapeDtypeStruct((d, tok), BF16), jax.ShapeDtypeStruct((SLOTS, 2, 4, d // 4, f), F32),
                   jax.ShapeDtypeStruct((d // 4, d), F32), jax.ShapeDtypeStruct(half.shape[1:], F32)),
        grid=(SLOTS,),
        in_specs=[leading(d, f), leading(f, d)] + [ANY] * 4,
        out_specs=[ANY] * 4,
        scratch_shapes=[pltpu.VMEM((seqs, seq, d), BF16), pltpu.VMEM((d, tok), BF16), pltpu.VMEM((d, tok), BF16), pltpu.VMEM((d, tok), F32), pltpu.VMEM((f, d), BF16),
                        pltpu.VMEM((f, tok), BF16), pltpu.VMEM((f, tok), BF16), pltpu.VMEM((d, tok), BF16),
                        pltpu.VMEM((2, 4, d // 4, f), F32), pltpu.VMEM((2, 4, d // 4, d), F32)]
        + scatter_bufs(d // 4, d) + [pltpu.VMEM(half.shape[1:], F32)] * 2 + SEMS,
        compiler_params=params(1, 1),
        name='mlp_second',
    )(w1, w2, y, dz, partial, half)


def attn_step(sems, peers, x_ref, dy_hbm, w_hbm, dy_ref, w_ref, xt, acc, gacc, qkv, do, b1, b2, begin, act, emit, ending=lambda: None):
    s, slot = pl.program_id(0), pl.program_id(1)
    step = s * SLOTS + slot
    last = SLOTS * SLOTS - 1
    before = jnp.maximum(step - 1, 0)
    seq, d = x_ref.shape[-2:]
    nqkv = qkv.shape[0]
    third = nqkv // 3
    split = d - b2.shape[1]
    rows = d // 4

    load_w = sems.copies(SLOTS, lambda i: w_hbm.at[i], lambda i: w_ref.at[i])
    load_dy = sems.copies(SLOTS, lambda i: dy_hbm.at[:, tokens(i, seq)], lambda i: dy_ref.at[:, tokens(i, seq)])

    @pl.when(step == 0)
    def _():
        for i in range(SLOTS):
            load_w(i).start()
            load_dy(i).start()
        begin()
        def clear(j, carry):
            gacc[j // 4, j % 4] = jnp.zeros(gacc.shape[2:], F32)
            b1[j % 2] = jnp.zeros(b1.shape[1:], BF16)
            b2[j % 2] = jnp.zeros(b2.shape[1:], BF16)
            return carry
        lax.fori_loop(0, SLOTS * 4, clear, 0)
    act()
    with jax.named_scope('loadw'):
        pl.when(s == 0)(lambda: load_w(slot).wait())

    @pl.when(slot == 0)
    def _():
        with jax.named_scope('e35'):
            load_dy(s).wait()
        with jax.named_scope('e36'):
            xt[s % 2] = x_ref[0, 0].T

    def grads(n, par):
        ps, pj = n // SLOTS, n % SLOTS
        third_d = d // 3

        def weights(c):
            cols = slice(c * third_d, (c + 1) * third_d)
            g = dot(xt[ps % 2], b1[par, cols], NT)
            if c == 2:
                g = g + dot(dy_ref[:, tokens(ps, seq)], b2[par], NT)
            for k in range(4):
                r = peers.rel(k)
                gacc[pj, r, :, cols] = gacc[pj, r, :, cols] + g[k * rows:(k + 1) * rows]

        def inputs(c):
            part = slice(c * third_d, (c + 1) * third_d)
            acc[part] += dot(w_ref[pj, :, part].T, b1[par], NN)
        return [functools.partial(f, c) for c in range(3) for f in (weights, inputs)]
    with jax.named_scope("main"):
        x_t = xt[s % 2]
        dy_t = dy_ref[:, tokens(s, seq)]
        now = step % 2
        qkv[...] = dot(w_ref[slot, pl.ds(0, nqkv), :], x_t, NN).astype(BF16)
        do[...] = dot(w_ref[slot, pl.ds(nqkv, d - nqkv), :], dy_t, NN).astype(BF16)
        scale = HEAD ** -0.5
        exp_scale = scale * math.log2(math.e)
        qb = seq // 2
        units = [(h, slice(c * qb, (c + 1) * qb)) for h in range(third // HEAD) for c in range(2)]

        def scores(h, qc):
            q_rows, k_rows, v_rows = head_rows(h)
            return dot(qkv[k_rows, :].T, qkv[q_rows, qc], NN), dot(qkv[v_rows, :].T, do[q_rows, qc] * scale, NN)

        def head_rows(h):
            return [slice(i * third + h * HEAD, i * third + (h + 1) * HEAD) for i in range(3)]
        for piece in grads(before, 1 - step % 2):
            piece()
        ahead = [scores(*unit) for unit in units[:LOOK_AHEAD]]
        for n, (h, qc) in enumerate(units):
            sc, dp_t = ahead.pop(0)
            if n + LOOK_AHEAD < len(units):
                ahead.append(scores(*units[n + LOOK_AHEAD]))
            q_rows, k_rows, v_rows = head_rows(h)
            m = jnp.max(sc, axis=0, keepdims=True)
            e = jnp.exp2((sc - m) * exp_scale)
            inv = 1.0 / jnp.sum(e, axis=0, keepdims=True)
            rd = jnp.sum(e * dp_t, axis=0, keepdims=True) * inv
            p = e * inv
            p_bf = p.astype(BF16)
            ds = (p * (dp_t - rd)).astype(BF16)
            b2[now, pl.ds(b2.shape[1] - third + h * HEAD, HEAD), qc] = dot(qkv[v_rows, :], p_bf, NN).astype(BF16)
            b1[now, q_rows, qc] = dot(qkv[k_rows, :], ds, NN).astype(BF16)
            dv_c = dot(do[q_rows, qc], p_bf, NT)
            dk_c = dot(qkv[q_rows, qc], ds, NT)
            if n % 2 == 0:
                dv, dk = dv_c, dk_c
            else:
                b1[now, k_rows] = (dk + dk_c).astype(BF16)
                b1[now, v_rows] = (dv + dv_c).astype(BF16)

    @pl.when(slot == 0)
    def _():
        @pl.when(s > 0)
        def _():
            emit(s - 1)
        acc[...] = dy_ref[:, tokens(s, seq)].astype(F32)

    @pl.when(step == last)
    def _():
        with jax.named_scope('e32'):
            ending()
        with jax.named_scope('e33'):
            for piece in grads(last, last % 2):
                piece()
        with jax.named_scope('e34'):
            emit(s)


ATTN_IN = 3
ATTN_SCRATCH = 9
JOB_PLAN = '1add0,1send1,6add1,6send2,11add2', '2add0,2send1x,6send1y,9add1x,9send2x,13add1y,13send2y'


def attn_first_kernel(layer, x_ref, dy_hbm, w_hbm, partial, wup, wdn, wq, wo, dx_hbm, g_hbm, w1_g, w2_g, wa_g, half, *rest):
    body, rest = rest[:ATTN_SCRATCH], rest[ATTN_SCRATCH:]
    acc, gacc, mine, bounce = body[3], body[4], rest[:2], rest[-4]
    seq = x_ref.shape[-2]
    step = pl.program_id(0) * SLOTS + pl.program_id(1)
    peers, sems = Peers(), Sems(*rest[-3:])
    a, b = jobs = [Scatter(sems, peers, lambda s, j=j: partial.at[s, j], lambda x, j=j: mine[j].at[x], rest[2 + 4 * j:6 + 4 * j], None,
                           (0, half.shape[2]), half_out=lambda x, j=j: half.at[x, j]) for j in range(2)]
    blocks = [(lambda w=w: w.at[layer - 1], lambda j, g=g: g.at[j], wup.shape[1]) for w, g in ((wup, w1_g), (wdn, w2_g))] + attn_weights(layer - 1, wq, wo, wa_g)
    gather = Gather(sems, peers, [r[:2] for r in blocks])
    hop = Bounce(sems, blocks, bounce)
    stores = [sems.copy(lambda j=j: gacc.at[j], lambda j=j: g_hbm.at[j]) for j in range(SLOTS)]
    actions = merge(steps(a, JOB_PLAN[0]), steps(b, JOB_PLAN[1]), [(5 + k, s) for k, s in enumerate(hop.steps)],
                    ticks('6,11,15', gather.forwards()), ticks('14,15', [lambda c=c: c().start() for c in stores]))

    dxb = rest[-5]
    store_dx = sems.copies(SLOTS, lambda i: dxb.at[i], lambda i: dx_hbm.at[:, tokens(i, seq)])

    def begin():
        peers.barrier()
        for job in jobs:
            job.both('start')
        gather.start(range(len(blocks)))

    def emit(s):
        dxb[s] = acc[...].astype(BF16)
        store_dx(s).start()
    attn_step(sems, peers, x_ref, dy_hbm, w_hbm, *body, begin, lambda: at_ticks(actions, step), emit)

    @pl.when(step == SLOTS * SLOTS - 1)
    def _():
        with jax.named_scope('e23'):
            for c in stores[2:]:
                c().start()
        with jax.named_scope('e24'):
            gather.forward(3)
        with jax.named_scope('e25'):
            a.out()
        with jax.named_scope('e26'):
            b.both('add2')
        with jax.named_scope('e27'):
            gather.finish()
        with jax.named_scope('e28'):
            for c in stores:
                c().wait()
        with jax.named_scope('e29'):
            b.out()
        with jax.named_scope('e30'):
            for i in range(SLOTS):
                store_dx(i).wait()
        with jax.named_scope('e31'):
            for job in jobs:
                job.finish()


def attn_last_kernel(x_ref, dy_hbm, w_hbm, partial, dxg, red, red_last, *rest):
    body, rest = rest[:ATTN_SCRATCH], rest[ATTN_SCRATCH:]
    acc, gacc, mine, dxb, free = body[3], body[4], rest[:2], rest[-5], rest[-4]
    step = pl.program_id(0) * SLOTS + pl.program_id(1)
    seqs = pl.num_programs(0)
    peers, sems = Peers(), Sems(*rest[-3:])
    nred = red.shape[1]
    a, b = jobs = [Scatter(sems, peers, lambda s, j=j: partial.at[s, j], lambda x, j=j: mine[j].at[x], rest[2 + 4 * j:6 + 4 * j], lambda j=j: red.at[j],
                           (0, nred)) for j in range(2)]
    h = nred // 2
    ends = [Scatter(sems, peers, lambda s: gacc.at[s], lambda x: gacc.at[2 * x], rest[2:6], lambda j=j: red_last.at[pl.ds(j * h, h)], (j * h, h), load=False)
            for j in range(2)]
    t = peers.t
    t2 = (t + 2) % SLOTS
    sib, xp, fwd, mine_dx = [], [], [], []
    for s in range(SLOTS):
        def src(s=s):
            return dxb.at[s]

        def dst(s=s):
            return dxg.at[t * SLOTS + s]

        def other(s=s):
            return dxg.at[t2 * SLOTS + s]
        mine_dx.append(sems.copy(src, dst))
        sib.append(sems.remote(src, dst, peers.sib))
        xp.append(sems.remote(src, dst, peers.xp))
        fwd.append(sems.remote(other, other, peers.sib))

    def freed(i):
        for peer in ([peers.sib], [peers.yp, peers.zp], [peers.yp, peers.zp], [peers.xp])[i]:
            pl.semaphore_signal(free.at[i], inc=1, device_id=peer, device_id_type=MESH)

    def forward(s):
        xp[s]().wait_recv()
        fwd[s]().start()

    def early():
        pl.semaphore_wait(free.at[0], 1)
        for job in ends:
            job.start(0)

    def early_add():
        pl.semaphore_wait(free.at[1], 2)
        for job in ends:
            job.add0(0)
        for job in ends:
            job.send1(0)
    actions = merge(steps(a, '1add0y,1send1y,4add1y,4send2y,8add2y,8send3,10add1x,10send2x'), steps(b, '1add0y,1send1y,7add1y,7send2y,12add2y,12send3,14add1x,14send2x'),
                    steps(a, '2add0x,6send1x'), steps(b, '2add0x,7send1x'),
                    ticks('3,11,9,13,15', [functools.partial(freed, i) for i in range(2)] + [functools.partial(forward, i) for i in range(2)] + [early]))

    def begin():
        peers.barrier()
        for x in (1, 0):
            for job in jobs:
                job.start(x)

    def emit(s):
        dxb[s] = acc[...].T.astype(BF16)
        for k in range(SLOTS):
            @pl.when(s == k)
            def _(k=k):
                for c in (xp, sib, mine_dx):
                    c[k]().start()
    attn_step(sems, peers, x_ref, dy_hbm, w_hbm, *body, begin, lambda: at_ticks(actions, step), emit, early_add)

    @pl.when(step == SLOTS * SLOTS - 1)
    def _():
        with jax.named_scope('e1'):
            for job in ends:
                job.start(1)
        with jax.named_scope('e2'):
            a.add2(0)
        with jax.named_scope('e3'):
            freed(2)
        with jax.named_scope('e4'):
            a.add3()
        with jax.named_scope('e5'):
            freed(3)
        with jax.named_scope('e6'):
            for job in ends:
                job.add0(1)
        with jax.named_scope('e7'):
            a.out()
        with jax.named_scope('e8'):
            b.add2(0)
        with jax.named_scope('e9'):
            for job in ends:
                job.send1(1)
        with jax.named_scope('e10'):
            b.add3()
        with jax.named_scope('e11'):
            b.out()
        with jax.named_scope('e12'):
            pl.semaphore_wait(free.at[2], 2)
        with jax.named_scope('e13'):
            pl.semaphore_wait(free.at[3], 1)
        with jax.named_scope('e14'):
            for job in ends:
                job.add1(0)
                job.send2(0)
        with jax.named_scope('e15'):
            forward(2)
        with jax.named_scope('e16'):
            for job in ends:
                job.add1(1)
                job.send2(1)
        with jax.named_scope('e17'):
            for job in ends:
                job.both('add2')
                job.send3()
        with jax.named_scope('e18'):
            forward(3)
        with jax.named_scope('e19'):
            for s in range(SLOTS):
                mine_dx[s]().wait()
                sib[s]().wait()
                xp[s]().wait_send()
        with jax.named_scope('e20'):
            for job in ends:
                job.add3()
                job.out()
        with jax.named_scope('e21'):
            for s in range(SLOTS):
                fwd[s]().wait()
        with jax.named_scope('e22'):
            for job in jobs + ends:
                job.finish()


def attn_specs(layer, x, w):
    slots, nw, d = w.shape
    seq = x.shape[2]
    seqs = x.shape[1] // slots
    tok = seqs * seq
    nqkv = nw * 3 // 4
    in_specs = [pl.BlockSpec((1, 1, seq, d), lambda s, j: (layer, lax.axis_index('tp') * seqs + s, 0, 0))] + [ANY] * 3
    scratch = [pltpu.VMEM((d, tok), BF16), pltpu.VMEM((slots, nw, d), BF16), pltpu.VMEM((2, d, seq), BF16), pltpu.VMEM((d, seq), F32), pltpu.VMEM((slots, 4, d // 4, nw), F32), pltpu.VMEM((nqkv, seq), BF16),
               pltpu.VMEM((nw - nqkv, seq), BF16), pltpu.VMEM((2, nw, seq), BF16), pltpu.VMEM((2, d // 3, seq), BF16)]
    scratch += [pltpu.VMEM((2, 4, d // 4, d), F32)] * 2 + scatter_bufs(d // 4, d) * 2
    red = jax.ShapeDtypeStruct((2, d // 4, d), F32)
    return (slots, seqs), in_specs, scratch, red, tok


def attn_first(layer, x, dy, w, partial, *weights):
    grid, in_specs, scratch, red, tok = attn_specs(layer, x, w)
    slots, nw, d = w.shape
    gathered = [jax.ShapeDtypeStruct((slots, d, d), BF16)] * 3
    return pl.pallas_call(
        functools.partial(attn_first_kernel, layer),
        out_shape=[jax.ShapeDtypeStruct((d, tok), BF16), jax.ShapeDtypeStruct((slots, 4, d // 4, nw), F32)] + gathered + [jax.ShapeDtypeStruct((2,) + red.shape, F32)],
        grid=grid,
        in_specs=in_specs + [ANY] * len(weights),
        out_specs=[ANY] * 6,
        scratch_shapes=scratch + [pltpu.VMEM((slots, d, tok // slots), BF16), pltpu.VMEM((d, d), BF16)] + SEMS,
        compiler_params=params(2, 2),
        name='attn_first',
    )(x, dy, w, partial, *weights)


def attn_last(layer, x, dy, w, partial):
    grid, in_specs, scratch, red, tok = attn_specs(layer, x, w)
    slots, nw, d = w.shape
    seq = x.shape[2]
    return pl.pallas_call(
        attn_last_kernel,
        out_shape=[jax.ShapeDtypeStruct((x.shape[1], seq, d), BF16), red, jax.ShapeDtypeStruct(red.shape[1:], F32)],
        grid=grid,
        in_specs=in_specs,
        out_specs=[ANY] * 3,
        scratch_shapes=scratch + [pltpu.VMEM((slots, seq, d), BF16), pltpu.SemaphoreType.REGULAR((4,))] + SEMS,
        compiler_params=params(3, 2),
        name='attn_last',
    )(x, dy, w, partial)


def finish_kernel(dxg, ra0, ra1, rm0, rm1, dx, g_qkv, g_out, g_down, g_up, buf, wide, mlp, tq, to, sems):
    n = dxg.shape[0]
    nq = tq.shape[1]
    count = [n]

    def copy(src, dst, i=None):
        if i is None:
            i = count[0]
            count[0] += 1
        return pltpu.make_async_copy(src, dst, sems.at[i])
    small = [copy(ra0, wide.at[0]), copy(ra1, wide.at[1]), copy(rm0, mlp.at[0]), copy(rm1, mlp.at[1])]
    first = count[0]
    for c in small:
        c.start()

    def load(i, carry):
        copy(dxg.at[i], buf.at[i], i).start()
        return carry
    lax.fori_loop(0, n, load, 0)
    for c in small:
        c.wait()
    out = [copy(mlp.at[k, j], g.at[k]) for j, g in enumerate((g_down, g_up)) for k in range(2)]
    for c in out:
        c.start()
    for k in range(2):
        tq[k] = wide[k, :, :nq].T
        to[k] = wide[k, :, nq:].T
    last = [copy(tq, g_qkv), copy(to, g_out)]
    for c in last:
        c.start()

    def move(i, carry):
        copy(dxg.at[i], buf.at[i], i).wait()
        copy(buf.at[i], dx.at[i], i).start()
        return carry
    lax.fori_loop(0, n, move, 0)

    def done(i, carry):
        copy(buf.at[i], dx.at[i], i).wait()
        return carry
    lax.fori_loop(0, n, done, 0)
    for c in out + last:
        c.wait()


def finish(nq, dxg, ra0, ra1, rm0, rm1):
    rows, d = ra0.shape
    shapes = [dxg.shape, (2, nq, rows), (2, d - nq, rows), (2, rows, d), (2, rows, d)]
    return pl.pallas_call(
        finish_kernel,
        out_shape=[jax.ShapeDtypeStruct(shapes[0], BF16)] + [jax.ShapeDtypeStruct(shape, F32) for shape in shapes[1:]],
        in_specs=[ANY] * 5,
        out_specs=[ANY] * 5,
        scratch_shapes=[pltpu.VMEM(dxg.shape, BF16), pltpu.VMEM((2, rows, d), F32), pltpu.VMEM((2,) + rm0.shape, F32), pltpu.VMEM(shapes[1], F32),
                        pltpu.VMEM(shapes[2], F32), pltpu.SemaphoreType.DMA((32,))],
        compiler_params=pltpu.CompilerParams(vmem_limit_bytes=VMEM_LIMIT),
        name='finish',
    )(dxg, ra0, ra1, rm0, rm1)


def solution(mesh):
    assert dict(mesh.shape) == {'dpy': 2, 'dpx': 2, 'tp': SLOTS}
    act_spec = P(None, DATA_AXES, None, None)

    def device_backward(x_saved, y_saved, dz_top, w_qkv, w_out, w_up, w_down):
        layers, d = w_up.shape[:2]
        assert layers == 2
        heads, hd = w_out.shape[1:3]
        n = 3 * heads * hd
        wq = w_qkv.transpose(0, 2, 3, 4, 1).reshape(layers, n, d)
        wo = w_out.reshape(layers, heads * hd, d)
        dy1, gm1, wa1 = mlp_first(1, y_saved, dz_top, w_up, w_down, wq, wo)
        dx1, ga1, w1_0, w2_0, wa0, half = attn_first(1, x_saved, dy1, wa1, gm1, w_up, w_down, wq, wo)
        dy0, gm0, ra1, rm1 = mlp_second(0, y_saved, dx1, w1_0, w2_0, ga1, half)
        d_input, rm0, ra0 = attn_last(0, x_saved, dy0, wa0, gm0)
        d_input, g_qkv, g_out, g_down, g_up = finish(n, d_input, ra0, ra1, rm0, rm1)
        g_qkv = g_qkv.reshape(layers, 3, heads, hd, d // 4).transpose(0, 4, 1, 2, 3)
        return d_input, g_qkv, g_out.reshape(layers, heads, hd, d // 4), g_up, g_down

    tp_last = P(None, None, None, 'tp', None), P(None, 'tp', None, None), P(None, None, 'tp'), P(None, 'tp', None)
    return jax.shard_map(device_backward, mesh=mesh,
                         in_specs=(act_spec, act_spec, P(DATA_AXES, None, None)) + tp_last,
                         out_specs=(P(DATA_AXES, None, None), P(None, DATA_AXES, None, 'tp', None), P(None, 'tp', None, DATA_AXES), P(None, DATA_AXES, 'tp'), P(None, ('tp', 'dpy', 'dpx'), None)),
                         check_vma=False)
```

```python
import functools
import math
import re

import jax
import jax.numpy as jnp
from jax import lax
from jax.experimental import pallas as pl
from jax.experimental.pallas import tpu as pltpu
from jax.sharding import PartitionSpec as P

DATA_AXES = ('dpy', 'dpx')
F32 = jnp.float32
BF16 = jnp.bfloat16
HEAD = 64
SLOTS = 4
LOOK_AHEAD = 3
PIECES = 8
NN = (((1,), (0,)), ((), ()))
NT = (((1,), (1,)), ((), ()))
VMEM_LIMIT = 63 * 1024 * 1024
MESH = pl.DeviceIdType.MESH
ANY = pl.BlockSpec(memory_space=pl.ANY)


def dot(a, b, dims):
    return lax.dot_general(a, b, dims, preferred_element_type=F32)


class Peers:
    def __init__(self):
        z, y, t = lax.axis_index('dpy'), lax.axis_index('dpx'), lax.axis_index('tp')
        self.z, self.y, self.t = z, y, t
        self.sib = (z, y, t + 1 - 2 * (t % 2))
        self.xp = (z, y, (t + 2) % 4)
        self.yp = (z, 1 - y, t)
        self.zp = (1 - z, y, t)

    def barrier(self):
        sem = pltpu.get_barrier_semaphore()
        with jax.named_scope('entry'):
            for peer in (self.sib, self.xp, self.yp, self.zp):
                pl.semaphore_signal(sem, inc=1, device_id=peer, device_id_type=MESH)
            pl.semaphore_wait(sem, 4)

    def rel(self, d):
        zr = self.z if d // 2 == 0 else 1 - self.z
        yr = self.y if d % 2 == 0 else 1 - self.y
        return zr * 2 + yr


class Sems:
    def __init__(self, send, recv, local):
        self.send, self.recv, self.local = send, recv, local
        self.n = self.m = 0

    def remote(self, src, dst, peer):
        i = self.n
        self.n += 1
        return lambda: pltpu.make_async_remote_copy(src_ref=src(), dst_ref=dst(), send_sem=self.send.at[i], recv_sem=self.recv.at[i],
                                                    device_id=peer, device_id_type=MESH)

    def copy(self, src, dst):
        i = self.m
        self.m += 1
        return lambda: pltpu.make_async_copy(src(), dst(), self.local.at[i])

    def copies(self, n, src, dst):
        first = self.m
        self.m += n
        return lambda i: pltpu.make_async_copy(src(i), dst(i), self.local.at[first + i])


def at_ticks(actions, tick, position=0, points=1):
    for k in sorted(actions):
        if k % points == position:
            @pl.when(tick == k)
            def _(k=k):
                with jax.named_scope('t%d' % k):
                    for action in actions[k]:
                        action()


class Scatter:
    def __init__(self, sems, peers, partial, mine, bufs, out, rows, load=True, half_out=None):
        r0, r1, r2, r3 = self.bufs = bufs
        first, count = rows
        h = count // 2
        self.mine, self.all, self.lo, self.hi = mine, pl.ds(first, count), pl.ds(first, h), pl.ds(first + h, h)
        self.half = half = pl.ds(first // 2, h)
        every, lo, hi = self.all, self.lo, self.hi
        self.load, self.c0, self.c1, self.c2 = [], [], [], []
        for x in range(2):
            def near(k, part, x=x):
                return lambda: mine(x).at[k, part]

            def place(buf, *index):
                return lambda: buf.at[index]
            if load:
                self.load.append(sems.copy(lambda x=x: partial(2 * x).at[:, every], near(slice(None), every)))
            self.c0.append(sems.remote(lambda x=x: partial(2 * x + 1).at[:, every], place(r0, x, slice(None), every), peers.sib))
            self.c1.append([sems.remote(near(2 * k + 1, lo), place(r1, 0, x, k, half), peers.yp) for k in range(2)]
                           + [sems.remote(near(2 + k, hi), place(r1, 1, x, k, half), peers.zp) for k in range(2)])
            self.c2.append([sems.remote(near(2, lo), place(r2, 0, x, half), peers.zp), sems.remote(near(1, hi), place(r2, 1, x, half), peers.yp)])
        if half_out is None:
            self.c3 = sems.remote(lambda: mine(1).at[0, every], place(r3, every), peers.xp)
            self.store = [sems.copy(lambda: mine(0).at[0, every], out)]
        else:
            self.c3 = None
            self.store = [sems.copy(lambda x=x: mine(x).at[0, every], lambda x=x: half_out(x)) for x in range(2)]

    def start(self, x):
        self.c0[x]().start()
        if self.load:
            self.load[x]().start()

    def add0(self, x):
        if self.load:
            self.load[x]().wait()
        self.c0[x]().wait_recv()
        mine, r0 = self.mine(x), self.bufs[0].at[x]

        def body(k, carry):
            mine[k, self.all] = mine[k, self.all] + r0[k, self.all]
            return carry
        lax.fori_loop(0, 4, body, 0)

    def send1(self, x):
        for c in self.c1[x]:
            c().start()

    def add1(self, x):
        for c in self.c1[x]:
            c().wait_recv()
        mine, r1 = self.mine(x), self.bufs[1]

        def body(k, carry):
            mine[2 * k, self.lo] = mine[2 * k, self.lo] + r1[0, x, k, self.half]
            mine[k, self.hi] = mine[k, self.hi] + r1[1, x, k, self.half]
            return carry
        lax.fori_loop(0, 2, body, 0)

    def send2(self, x):
        for c in self.c2[x]:
            c().start()

    def add2(self, x):
        for c in self.c2[x]:
            c().wait_recv()
        mine, r2 = self.mine(x), self.bufs[2]
        mine[0, self.lo] = mine[0, self.lo] + r2[0, x, self.half]
        mine[0, self.hi] = mine[0, self.hi] + r2[1, x, self.half]

    def send3(self):
        self.c3().start()

    def add3(self):
        self.c3().wait_recv()
        mine = self.mine(0)
        mine[0, self.all] = (mine[0, self.all] + self.bufs[3][self.all]) * (1 / SLOTS)

    def out(self):
        for c in self.store:
            c().start()

    def finish(self):
        for c in self.c0 + sum(self.c1, []) + sum(self.c2, []) + ([self.c3] if self.c3 else []):
            c().wait_send()
        for c in self.store:
            c().wait()

    def both(self, name):
        for x in range(2):
            getattr(self, name)(x)


def scatter_bufs(rows, d):
    return [pltpu.VMEM((2, 4, rows, d), F32), pltpu.VMEM((2, 2, 2, rows // 2, d), F32), pltpu.VMEM((2, 2, rows // 2, d), F32), pltpu.VMEM((rows, d), F32)]


def steps(job, plan):
    out = []
    for tick, name, half in re.findall('([0-9]+)([a-z]+[0-3]?)([xy]?)', plan):
        if half:
            action = functools.partial(getattr(job, name), int(half == 'y'))
        else:
            action = functools.partial(job.both, name) if name[-1] in '012' else getattr(job, name)
        out.append((int(tick), action))
    return out


def ticks(plan, actions):
    return list(zip(map(int, plan.split(',')), actions))


class Gather:
    def __init__(self, sems, peers, blocks):
        self.sib = [sems.remote(own, lambda dst=dst: dst(1), peers.sib) for own, dst in blocks]
        self.xp = [sems.remote(own, lambda dst=dst: dst(2), peers.xp) for own, dst in blocks]
        self.fwd = [sems.remote(lambda dst=dst: dst(2), lambda dst=dst: dst(3), peers.sib) for own, dst in blocks]

    def start(self, blocks):
        for i in blocks:
            self.sib[i]().start()
            self.xp[i]().start()

    def forward(self, i):
        self.xp[i]().wait_recv()
        self.fwd[i]().start()

    def forwards(self):
        return [functools.partial(self.forward, i) for i in range(len(self.fwd))]

    def finish(self):
        for i in range(len(self.sib)):
            self.sib[i]().wait_recv()
            self.fwd[i]().wait_recv()
            self.sib[i]().wait_send()
            self.xp[i]().wait_send()
            self.fwd[i]().wait_send()


class Bounce:
    def __init__(self, sems, items, buf):
        self.steps = []
        prev = None
        for own, dst, rows in items:
            ld = sems.copy(own, lambda rows=rows: buf.at[pl.ds(0, rows)])
            st = sems.copy(lambda rows=rows: buf.at[pl.ds(0, rows)], lambda dst=dst: dst(0))
            self.steps.append(functools.partial(self.load, prev, ld))
            self.steps.append(functools.partial(self.flip, ld, st))
            prev = st
        self.steps.append(lambda prev=prev: prev().wait())

    @staticmethod
    def load(prev, ld):
        if prev is not None:
            prev().wait()
        ld().start()

    @staticmethod
    def flip(ld, st):
        ld().wait()
        st().start()


def merge(*lists):
    actions = {}
    for pairs in lists:
        for k, action in pairs:
            actions.setdefault(k, []).append(action)
    return actions


SEMS = [pltpu.SemaphoreType.DMA((96,)), pltpu.SemaphoreType.DMA((96,)), pltpu.SemaphoreType.DMA((32,))]


def leading(*shape):
    return pl.BlockSpec((1,) + shape, lambda j, *_: (j,) + (0,) * len(shape))


def params(collective_id, axes):
    return pltpu.CompilerParams(vmem_limit_bytes=VMEM_LIMIT, dimension_semantics=('arbitrary',) * axes, collective_id=collective_id, has_side_effects=True)


def mlp_slot(slot, seqs, seq, w1, w2, w1t, yt, dz, acc, gt, dht, tick, arrive, emit):
    w1t[...] = w1[...].T

    def block(i, carry):
        tick(i)
        with jax.named_scope('arrive'):
            pl.when(slot == 0)(lambda: arrive(i))
        cols = pl.ds(pl.multiple_of(i * seq, seq), seq)
        h = dot(w1t[...], yt[:, cols], NN)
        dg = dot(w2[...], dz[:, cols], NN)
        c0 = math.sqrt(2 / math.pi)
        c1 = 0.044715 * c0
        h2 = h * h
        t = jnp.tanh(h * (c0 + c1 * h2))
        q = 0.5 * t + 0.5
        g = h * q
        dh = dg * (q + (g * (1.0 - t)) * (c0 + (3 * c1) * h2))
        gt[:, cols] = g.astype(BF16)
        dh = dh.astype(BF16)
        dht[:, cols] = dh
        acc[:, cols] += dot(w1[...], dh, NN)
        with jax.named_scope('memit'):
            pl.when(slot == SLOTS - 1)(lambda: emit(i))
        return carry
    lax.fori_loop(0, seqs, block, 0)


def tokens(i, seq):
    return pl.ds(pl.multiple_of(i * seq, seq), seq)


class MlpIo:
    def __init__(self, sems, peers, seqs, seq, loads, acc, dz, dyb, dy_hbm, gbuf, g_hbm):
        self.seqs, self.seq, self.peers = seqs, seq, peers
        self.loads, self.acc, self.dz, self.dyb, self.gbuf = loads, acc, dz, dyb, gbuf
        self.dy = sems.copies(seqs, lambda i: dyb.at[:, tokens(i, seq)], lambda i: dy_hbm.at[:, tokens(i, seq)])
        self.g = [sems.copy(lambda j=j: gbuf.at[j], lambda j=j: g_hbm.at[pl.program_id(0), j]) for j in range(2)]

    def start(self):
        for load, _ in self.loads:
            for i in range(self.seqs):
                load(i).start()

    def arrive(self, i):
        for load, use in self.loads:
            load(i).wait()
            use(i)
        cols = tokens(i, self.seq)
        self.acc[:, cols] = jnp.zeros((self.acc.shape[0], self.seq), F32)

    def emit(self, i):
        cols = tokens(i, self.seq)
        self.dyb[:, cols] = (self.dz[:, cols].astype(F32) + self.acc[:, cols]).astype(BF16)
        self.dy(i).start()

    def grads(self, j, a, b):
        pl.when(pl.program_id(0) > 0)(lambda: self.g[j]().wait())
        rows, width = self.gbuf.shape[-2:]
        split, half = width * 2 // 3, width // 2
        for lo, hi, c0, c1 in ((0, width, 0, split), (0, half, split, width), (half, width, split, width)):
            g = dot(a[lo:hi], b[c0:c1], NT)
            for k in range(g.shape[0] // rows):
                self.gbuf[j, self.peers.rel(lo // rows + k), :, c0:c1] = g[k * rows:(k + 1) * rows]
        self.g[j]().start()

    def finish(self):
        for i in range(self.seqs):
            self.dy(i).wait()
        for c in self.g:
            c().wait()


def mlp_rest(slot, actions, io, w1, w2, w1t, yt, gt, dht):
    seqs, seq, dz, acc = io.seqs, io.seq, io.dz, io.acc
    points = seqs + 2
    first = slot * points

    def tick(i):
        at_ticks({k: v for k, v in actions.items() if k % points < seqs}, first + i)
    mlp_slot(slot, seqs, seq, w1, w2, w1t, yt, dz, acc, gt, dht, tick, io.arrive, io.emit)
    at_ticks(actions, first + seqs, seqs, points)
    with jax.named_scope('dw2'):
        io.grads(0, gt, dz)
    at_ticks(actions, first + seqs + 1, seqs + 1, points)
    with jax.named_scope('dw1'):
        io.grads(1, yt, dht)


def attn_weights(layer, wq, wo, wa_g):
    nq, d = wq.shape[1:]
    return [(lambda: wq.at[layer], lambda j: wa_g.at[j, pl.ds(0, nq)], nq), (lambda: wo.at[layer], lambda j: wa_g.at[j, pl.ds(nq, d - nq)], d - nq)]


class Spread:
    def __init__(self, sems, peers, wb, pieces):
        rows = wb.shape[2] // pieces
        y = peers.y

        def piece(slot, m, k):
            return lambda: wb.at[slot, m, pl.ds(k * rows, rows)]
        every = range(pieces)
        self.sib = sems.remote(lambda: wb.at[0], lambda: wb.at[1], peers.sib)
        self.xp = [sems.remote(piece(0, y, k), piece(2, y, k), peers.xp) for k in every]
        self.fy, self.wy = [], []
        for k in every:
            self.fy.append(sems.remote(piece(2, y, k), piece(2, y, k), peers.yp))
            sems.n -= 1
            self.wy.append(sems.remote(piece(2, 1 - y, k), piece(2, 1 - y, k), peers.yp))
        self.fs = [sems.remote(piece(2, y, k), piece(3, y, k), peers.sib) for k in every]
        self.fs2 = [sems.remote(piece(2, 1 - y, k), piece(3, 1 - y, k), peers.sib) for k in every]

    def start(self):
        for c in self.xp + [self.sib]:
            c().start()

    def forward(self, k):
        self.xp[k]().wait_recv()
        self.fy[k]().start()
        self.fs[k]().start()

    def forward2(self, k):
        self.wy[k]().wait_recv()
        self.fs2[k]().start()

    def arrived(self):
        for c in self.fs + self.fs2:
            c().wait_recv()

    def finish(self):
        for c in [self.sib] + self.xp + self.fy + self.fs + self.fs2:
            c().wait_send()


def turned(src, dst, seq):
    def use(i):
        dst[:, tokens(i, seq)] = src[i].T
    return use


def mlp_first_kernel(layer, y, dz_in, wup, wdn, wq, wo, dy_hbm, g_hbm, wa_g, yb, dzb, yt, dzt, acc, w1t, gt, dht, wb, bounce, dyb, gbuf, *rest):
    slot = pl.program_id(0)
    seqs, seq = yb.shape[:2]
    peers, sems = Peers(), Sems(*rest)
    mine = peers.t * seqs
    loads = [(sems.copies(seqs, lambda i: y.at[layer, mine + i], lambda i: yb.at[i]), turned(yb, yt, seq)),
             (sems.copies(seqs, lambda i: dz_in.at[mine + i], lambda i: dzb.at[i]), turned(dzb, dzt, seq))]
    io = MlpIo(sems, peers, seqs, seq, loads, acc, dzt, dyb, dy_hbm, gbuf, g_hbm)
    own = [sems.copy(lambda w=w: w.at[layer], lambda m=m: wb.at[0, m]) for m, w in enumerate((wup, wdn))]
    blocks = attn_weights(layer, wq, wo, wa_g)
    gather = Gather(sems, peers, [r[:2] for r in blocks])
    hop = Bounce(sems, blocks, bounce)
    spread = Spread(sems, peers, wb, PIECES)

    @pl.when(slot == 0)
    def _():
        with jax.named_scope('e54'):
            for c in own:
                c().start()
        with jax.named_scope('e55'):
            io.start()
        with jax.named_scope('e56'):
            peers.barrier()
        with jax.named_scope('e57'):
            for c in own:
                c().wait()
        with jax.named_scope('e58'):
            spread.start()
        with jax.named_scope('e59'):
            gather.start(range(2))

    @pl.when(slot == 1)
    def _():
        with jax.named_scope('e53'):
            spread.sib().wait_recv()

    @pl.when(slot == 2)
    def _():
        with jax.named_scope('e52'):
            for k in range(5, PIECES):
                spread.forward2(k)

    @pl.when(slot == 3)
    def _():
        with jax.named_scope('e51'):
            spread.arrived()
    every = range(PIECES)
    actions = merge([(14 + k, s) for k, s in enumerate(hop.steps)], ticks('2,3,4,5,7,8,10,11', [functools.partial(spread.forward, k) for k in every]),
                    ticks('7,8,9,10,11', [functools.partial(spread.forward2, k) for k in every]), ticks('21', gather.forwards()))
    mlp_rest(slot, actions, io, wb.at[slot, 0], wb.at[slot, 1], w1t, yt, gt, dht)

    @pl.when(slot == SLOTS - 1)
    def _():
        with jax.named_scope('e47'):
            gather.forward(1)
        with jax.named_scope('e48'):
            io.finish()
        with jax.named_scope('e49'):
            spread.finish()
        with jax.named_scope('e50'):
            gather.finish()


def mlp_first(layer, y, dz, wup, wdn, wq, wo):
    d, f = wup.shape[1:]
    seq = y.shape[2]
    seqs = y.shape[1] // SLOTS
    tok = seqs * seq
    return pl.pallas_call(
        functools.partial(mlp_first_kernel, layer),
        out_shape=(jax.ShapeDtypeStruct((d, tok), BF16), jax.ShapeDtypeStruct((SLOTS, 2, 4, d // 4, f), F32), jax.ShapeDtypeStruct((SLOTS, d, d), BF16)),
        grid=(SLOTS,),
        in_specs=[ANY] * 6,
        out_specs=[ANY] * 3,
        scratch_shapes=[pltpu.VMEM((seqs, seq, d), BF16)] * 2 + [pltpu.VMEM((d, tok), BF16)] * 2
        + [pltpu.VMEM((d, tok), F32), pltpu.VMEM((f, d), BF16), pltpu.VMEM((f, tok), BF16), pltpu.VMEM((f, tok), BF16), pltpu.VMEM((SLOTS, 2, d, f), BF16),
           pltpu.VMEM((d, d), BF16), pltpu.VMEM((d, tok), BF16), pltpu.VMEM((2, 4, d // 4, f), F32)] + SEMS,
        compiler_params=params(0, 1),
        name='mlp_first',
    )(y, dz, wup, wdn, wq, wo)


def mlp_second_kernel(layer, w1_ref, w2_ref, y, dz_in, partial, half, dy_hbm, g_hbm, red, red_half, yb, yt, dzt, acc, w1t, gt, dht, dyb, gbuf, mine, *rest):
    slot = pl.program_id(0)
    seqs, seq = yb.shape[:2]
    bufs, rest = rest[:4], rest[4:]
    peers, sems = Peers(), Sems(*rest[2:])
    place = peers.t * seqs
    loads = [(sems.copies(seqs, lambda i: y.at[layer, place + i], lambda i: yb.at[i]), turned(yb, yt, seq)),
             (sems.copies(seqs, lambda i: dz_in.at[:, tokens(i, seq)], lambda i: dzt.at[:, tokens(i, seq)]), lambda i: None)]
    io = MlpIo(sems, peers, seqs, seq, loads, acc, dzt, dyb, dy_hbm, gbuf, g_hbm)
    rows = mine.shape[2] // 2
    a, b = jobs = [Scatter(sems, peers, lambda s: partial.at[s], lambda x: mine.at[x], bufs, lambda j=j: red.at[pl.ds(j * rows, rows)], (j * rows, rows)) for j in range(2)]

    h0, h1 = rest[:2]
    mine_half = sems.copy(lambda: half.at[0], lambda: h0)
    x_half = sems.remote(lambda: half.at[1], lambda: h1, peers.xp)
    store_half = sems.copy(lambda: h0, lambda: red_half)

    def add_half():
        mine_half().wait()
        x_half().wait_recv()
        h0[...] = (h0[...] + h1[...]) * (1 / SLOTS)

    @pl.when(slot == 0)
    def _():
        with jax.named_scope('e42'):
            io.start()
        with jax.named_scope('e43'):
            peers.barrier()
        with jax.named_scope('e44'):
            for job in jobs:
                job.both('start')
        with jax.named_scope('e45'):
            x_half().start()
        with jax.named_scope('e46'):
            mine_half().start()
    actions = merge(ticks('17,18', [add_half, lambda: store_half().start()]),
                    steps(a, '3add0,3send1,9add1,9send2,17add2,17send3,21add3,22out'),
                    steps(b, '4add0,4send1,14add1,14send2,19add2,19send3,23add3'))
    mlp_rest(slot, actions, io, w1_ref.at[0], w2_ref.at[0], w1t, yt, gt, dht)

    @pl.when(slot == SLOTS - 1)
    def _():
        with jax.named_scope('e36'):
            b.out()
        with jax.named_scope('e37'):
            io.finish()
        with jax.named_scope('e38'):
            x_half().wait_send()
        with jax.named_scope('e39'):
            store_half().wait()
        with jax.named_scope('e40'):
            a.finish()
        with jax.named_scope('e41'):
            b.finish()


def mlp_second(layer, y, dz, w1, w2, partial, half):
    d, f = w1.shape[1:]
    seq = y.shape[2]
    seqs = y.shape[1] // SLOTS
    tok = seqs * seq
    return pl.pallas_call(
        functools.partial(mlp_second_kernel, layer),
        out_shape=(jax.ShapeDtypeStruct((d, tok), BF16), jax.ShapeDtypeStruct((SLOTS, 2, 4, d // 4, f), F32),
                   jax.ShapeDtypeStruct((d // 4, d), F32), jax.ShapeDtypeStruct(half.shape[1:], F32)),
        grid=(SLOTS,),
        in_specs=[leading(d, f), leading(f, d)] + [ANY] * 4,
        out_specs=[ANY] * 4,
        scratch_shapes=[pltpu.VMEM((seqs, seq, d), BF16), pltpu.VMEM((d, tok), BF16), pltpu.VMEM((d, tok), BF16), pltpu.VMEM((d, tok), F32), pltpu.VMEM((f, d), BF16),
                        pltpu.VMEM((f, tok), BF16), pltpu.VMEM((f, tok), BF16), pltpu.VMEM((d, tok), BF16),
                        pltpu.VMEM((2, 4, d // 4, f), F32), pltpu.VMEM((2, 4, d // 4, d), F32)]
        + scatter_bufs(d // 4, d) + [pltpu.VMEM(half.shape[1:], F32)] * 2 + SEMS,
        compiler_params=params(1, 1),
        name='mlp_second',
    )(w1, w2, y, dz, partial, half)


def attn_step(sems, peers, x_ref, dy_hbm, w_hbm, dy_ref, w_ref, xt, acc, gacc, qkv, do, b1, b2, begin, act, emit, ending=lambda: None):
    s, slot = pl.program_id(0), pl.program_id(1)
    step = s * SLOTS + slot
    last = SLOTS * SLOTS - 1
    before = jnp.maximum(step - 1, 0)
    seq, d = x_ref.shape[-2:]
    nqkv = qkv.shape[0]
    third = nqkv // 3
    split = d - b2.shape[1]
    rows = d // 4

    load_w = sems.copies(SLOTS, lambda i: w_hbm.at[i], lambda i: w_ref.at[i])
    load_dy = sems.copies(SLOTS, lambda i: dy_hbm.at[:, tokens(i, seq)], lambda i: dy_ref.at[:, tokens(i, seq)])

    @pl.when(step == 0)
    def _():
        for i in range(SLOTS):
            load_w(i).start()
            load_dy(i).start()
        begin()
        def clear(j, carry):
            gacc[j // 4, j % 4] = jnp.zeros(gacc.shape[2:], F32)
            b1[j % 2] = jnp.zeros(b1.shape[1:], BF16)
            b2[j % 2] = jnp.zeros(b2.shape[1:], BF16)
            return carry
        lax.fori_loop(0, SLOTS * 4, clear, 0)
    act()
    with jax.named_scope('loadw'):
        pl.when(s == 0)(lambda: load_w(slot).wait())

    @pl.when(slot == 0)
    def _():
        with jax.named_scope('e34'):
            load_dy(s).wait()
        with jax.named_scope('e35'):
            xt[s % 2] = x_ref[0, 0].T

    def grads(n, par):
        ps, pj = n // SLOTS, n % SLOTS
        third_d = d // 3

        def weights(c):
            cols = slice(c * third_d, (c + 1) * third_d)
            g = dot(xt[ps % 2], b1[par, cols], NT)
            if c == 2:
                g = g + dot(dy_ref[:, tokens(ps, seq)], b2[par], NT)
            for k in range(4):
                r = peers.rel(k)
                gacc[pj, r, :, cols] = gacc[pj, r, :, cols] + g[k * rows:(k + 1) * rows]

        def inputs(c):
            part = slice(c * third_d, (c + 1) * third_d)
            acc[part] += dot(w_ref[pj, :, part].T, b1[par], NN)
        return [functools.partial(f, c) for c in range(3) for f in (weights, inputs)]
    with jax.named_scope("main"):
        x_t = xt[s % 2]
        dy_t = dy_ref[:, tokens(s, seq)]
        now = step % 2
        qkv[...] = dot(w_ref[slot, pl.ds(0, nqkv), :], x_t, NN).astype(BF16)
        do[...] = dot(w_ref[slot, pl.ds(nqkv, d - nqkv), :], dy_t, NN).astype(BF16)
        scale = HEAD ** -0.5
        exp_scale = scale * math.log2(math.e)
        qb = seq // 2
        units = [(h, slice(c * qb, (c + 1) * qb)) for h in range(third // HEAD) for c in range(2)]

        def scores(h, qc):
            q_rows, k_rows, v_rows = head_rows(h)
            return dot(qkv[k_rows, :].T, qkv[q_rows, qc], NN), dot(qkv[v_rows, :].T, do[q_rows, qc] * scale, NN)

        def head_rows(h):
            return [slice(i * third + h * HEAD, i * third + (h + 1) * HEAD) for i in range(3)]
        for piece in grads(before, 1 - step % 2):
            piece()
        ahead = [scores(*unit) for unit in units[:LOOK_AHEAD]]
        for n, (h, qc) in enumerate(units):
            sc, dp_t = ahead.pop(0)
            if n + LOOK_AHEAD < len(units):
                ahead.append(scores(*units[n + LOOK_AHEAD]))
            q_rows, k_rows, v_rows = head_rows(h)
            m = jnp.max(sc, axis=0, keepdims=True)
            e = jnp.exp2((sc - m) * exp_scale)
            inv = 1.0 / jnp.sum(e, axis=0, keepdims=True)
            rd = jnp.sum(e * dp_t, axis=0, keepdims=True) * inv
            p = e * inv
            p_bf = p.astype(BF16)
            ds = (p * (dp_t - rd)).astype(BF16)
            b2[now, pl.ds(b2.shape[1] - third + h * HEAD, HEAD), qc] = dot(qkv[v_rows, :], p_bf, NN).astype(BF16)
            b1[now, q_rows, qc] = dot(qkv[k_rows, :], ds, NN).astype(BF16)
            dv_c = dot(do[q_rows, qc], p_bf, NT)
            dk_c = dot(qkv[q_rows, qc], ds, NT)
            if n % 2 == 0:
                dv, dk = dv_c, dk_c
            else:
                b1[now, k_rows] = (dk + dk_c).astype(BF16)
                b1[now, v_rows] = (dv + dv_c).astype(BF16)

    @pl.when(slot == 0)
    def _():
        @pl.when(s > 0)
        def _():
            emit(s - 1)
        acc[...] = dy_ref[:, tokens(s, seq)].astype(F32)

    @pl.when(step == last)
    def _():
        with jax.named_scope('e31'):
            ending()
        with jax.named_scope('e32'):
            for piece in grads(last, last % 2):
                piece()
        with jax.named_scope('e33'):
            emit(s)


ATTN_IN = 3
ATTN_SCRATCH = 9
JOB_PLAN = '1add0,1send1,6add1,6send2,11add2', '2add0,2send1x,6send1y,9add1x,9send2x,13add1y,13send2y,15add2'


def attn_first_kernel(layer, x_ref, dy_hbm, w_hbm, partial, wup, wdn, wq, wo, dx_hbm, g_hbm, w1_g, w2_g, wa_g, half, *rest):
    body, rest = rest[:ATTN_SCRATCH], rest[ATTN_SCRATCH:]
    acc, gacc, mine, bounce = body[3], body[4], rest[:2], rest[-4]
    seq = x_ref.shape[-2]
    step = pl.program_id(0) * SLOTS + pl.program_id(1)
    peers, sems = Peers(), Sems(*rest[-3:])
    a, b = jobs = [Scatter(sems, peers, lambda s, j=j: partial.at[s, j], lambda x, j=j: mine[j].at[x], rest[2 + 4 * j:6 + 4 * j], None,
                           (0, half.shape[2]), half_out=lambda x, j=j: half.at[x, j]) for j in range(2)]
    blocks = [(lambda w=w: w.at[layer - 1], lambda j, g=g: g.at[j], wup.shape[1]) for w, g in ((wup, w1_g), (wdn, w2_g))] + attn_weights(layer - 1, wq, wo, wa_g)
    gather = Gather(sems, peers, [r[:2] for r in blocks])
    hop = Bounce(sems, blocks, bounce)
    stores = [sems.copy(lambda j=j: gacc.at[j], lambda j=j: g_hbm.at[j]) for j in range(SLOTS)]
    actions = merge(steps(a, JOB_PLAN[0]), steps(b, JOB_PLAN[1]), [(5 + k, s) for k, s in enumerate(hop.steps)],
                    ticks('6,11,15,15', gather.forwards()), ticks('14,15,12', [lambda c=c: c().start() for c in stores[:2]] + [a.out]))

    dxb = rest[-5]
    store_dx = sems.copies(SLOTS, lambda i: dxb.at[i], lambda i: dx_hbm.at[:, tokens(i, seq)])

    def begin():
        peers.barrier()
        for job in jobs:
            job.both('start')
        gather.start(range(len(blocks)))

    def emit(s):
        dxb[s] = acc[...].astype(BF16)
        store_dx(s).start()
    attn_step(sems, peers, x_ref, dy_hbm, w_hbm, *body, begin, lambda: at_ticks(actions, step), emit)

    @pl.when(step == SLOTS * SLOTS - 1)
    def _():
        with jax.named_scope('e25'):
            for c in stores[2:]:
                c().start()
        with jax.named_scope('e26'):
            b.out()
        with jax.named_scope('e27'):
            gather.finish()
        with jax.named_scope('e28'):
            for c in stores:
                c().wait()
        with jax.named_scope('e29'):
            for i in range(SLOTS):
                store_dx(i).wait()
        with jax.named_scope('e30'):
            for job in jobs:
                job.finish()


def attn_last_kernel(x_ref, dy_hbm, w_hbm, partial, dxg, red, red_last, *rest):
    body, rest = rest[:ATTN_SCRATCH], rest[ATTN_SCRATCH:]
    acc, gacc, mine, dxb, free = body[3], body[4], rest[:2], rest[-5], rest[-4]
    step = pl.program_id(0) * SLOTS + pl.program_id(1)
    seqs = pl.num_programs(0)
    peers, sems = Peers(), Sems(*rest[-3:])
    nred = red.shape[1]
    a, b = jobs = [Scatter(sems, peers, lambda s, j=j: partial.at[s, j], lambda x, j=j: mine[j].at[x], rest[2 + 4 * j:6 + 4 * j], lambda j=j: red.at[j],
                           (0, nred)) for j in range(2)]
    h = nred // 2
    ends = [Scatter(sems, peers, lambda s: gacc.at[s], lambda x: gacc.at[2 * x], rest[2:6], lambda j=j: red_last.at[pl.ds(j * h, h)], (j * h, h), load=False)
            for j in range(2)]
    t = peers.t
    t2 = (t + 2) % SLOTS
    sib, xp, fwd, mine_dx = [], [], [], []
    for s in range(SLOTS):
        def src(s=s):
            return dxb.at[s]

        def dst(s=s):
            return dxg.at[t * SLOTS + s]

        def other(s=s):
            return dxg.at[t2 * SLOTS + s]
        mine_dx.append(sems.copy(src, dst))
        sib.append(sems.remote(src, dst, peers.sib))
        xp.append(sems.remote(src, dst, peers.xp))
        fwd.append(sems.remote(other, other, peers.sib))

    def freed(i):
        for peer in ([peers.sib], [peers.yp, peers.zp], [peers.yp, peers.zp], [peers.xp])[i]:
            pl.semaphore_signal(free.at[i], inc=1, device_id=peer, device_id_type=MESH)

    def forward(s):
        xp[s]().wait_recv()
        fwd[s]().start()

    def early():
        pl.semaphore_wait(free.at[0], 1)
        for job in ends:
            job.start(0)

    def early_add():
        pl.semaphore_wait(free.at[1], 2)
        for job in ends:
            job.add0(0)
        for job in ends:
            job.send1(0)
    actions = merge(steps(a, '1add0y,1send1y,4add1y,4send2y,8add2y,8send3,10add1x,10send2x'), steps(b, '1add0y,1send1y,7add1y,7send2y,12add2y,12send3,14add1x,14send2x'),
                    steps(a, '2add0x,6send1x'), steps(b, '2add0x,7send1x'),
                    ticks('3,11,10,15,15', [functools.partial(freed, i) for i in range(2)] + [functools.partial(forward, i) for i in range(2)] + [early]))

    def begin():
        peers.barrier()
        for x in (1, 0):
            for job in jobs:
                job.start(x)

    def emit(s):
        dxb[s] = acc[...].T.astype(BF16)
        for k in range(SLOTS):
            @pl.when(s == k)
            def _(k=k):
                for c in (xp, sib, mine_dx):
                    c[k]().start()
    attn_step(sems, peers, x_ref, dy_hbm, w_hbm, *body, begin, lambda: at_ticks(actions, step), emit, early_add)

    @pl.when(step == SLOTS * SLOTS - 1)
    def _():
        with jax.named_scope('e1'):
            for job in ends:
                job.start(1)
        with jax.named_scope('e2'):
            a.add2(0)
        with jax.named_scope('e3'):
            freed(2)
        with jax.named_scope('e4'):
            a.add3()
        with jax.named_scope('e5'):
            freed(3)
        with jax.named_scope('e6'):
            for job in ends:
                job.add0(1)
        with jax.named_scope('e7'):
            a.out()
        with jax.named_scope('e8'):
            b.add2(0)
        with jax.named_scope('e9'):
            for job in ends:
                job.send1(1)
        with jax.named_scope('e10'):
            b.add3()
        with jax.named_scope('e11'):
            b.out()
        with jax.named_scope('e12'):
            pl.semaphore_wait(free.at[2], 2)
        with jax.named_scope('e13'):
            pl.semaphore_wait(free.at[3], 1)
        with jax.named_scope('e14'):
            for job in ends:
                job.add1(0)
        with jax.named_scope('e15'):
            forward(2)
        with jax.named_scope('e16'):
            for job in ends:
                job.add1(1)
                job.send2(1)
        with jax.named_scope('e17'):
            for job in ends:
                job.send2(0)
        with jax.named_scope('e18'):
            for job in ends:
                job.add2(1)
                job.send3()
        with jax.named_scope('e19'):
            for job in ends:
                job.add2(0)
        with jax.named_scope('e20'):
            forward(3)
        with jax.named_scope('e21'):
            for s in range(SLOTS):
                mine_dx[s]().wait()
                sib[s]().wait()
                xp[s]().wait_send()
        with jax.named_scope('e22'):
            for job in ends:
                job.add3()
                job.out()
        with jax.named_scope('e23'):
            for s in range(SLOTS):
                fwd[s]().wait()
        with jax.named_scope('e24'):
            for job in jobs + ends:
                job.finish()


def attn_specs(layer, x, w):
    slots, nw, d = w.shape
    seq = x.shape[2]
    seqs = x.shape[1] // slots
    tok = seqs * seq
    nqkv = nw * 3 // 4
    in_specs = [pl.BlockSpec((1, 1, seq, d), lambda s, j: (layer, lax.axis_index('tp') * seqs + s, 0, 0))] + [ANY] * 3
    scratch = [pltpu.VMEM((d, tok), BF16), pltpu.VMEM((slots, nw, d), BF16), pltpu.VMEM((2, d, seq), BF16), pltpu.VMEM((d, seq), F32), pltpu.VMEM((slots, 4, d // 4, nw), F32), pltpu.VMEM((nqkv, seq), BF16),
               pltpu.VMEM((nw - nqkv, seq), BF16), pltpu.VMEM((2, nw, seq), BF16), pltpu.VMEM((2, d // 3, seq), BF16)]
    scratch += [pltpu.VMEM((2, 4, d // 4, d), F32)] * 2 + scatter_bufs(d // 4, d) * 2
    red = jax.ShapeDtypeStruct((2, d // 4, d), F32)
    return (slots, seqs), in_specs, scratch, red, tok


def attn_first(layer, x, dy, w, partial, *weights):
    grid, in_specs, scratch, red, tok = attn_specs(layer, x, w)
    slots, nw, d = w.shape
    gathered = [jax.ShapeDtypeStruct((slots, d, d), BF16)] * 3
    return pl.pallas_call(
        functools.partial(attn_first_kernel, layer),
        out_shape=[jax.ShapeDtypeStruct((d, tok), BF16), jax.ShapeDtypeStruct((slots, 4, d // 4, nw), F32)] + gathered + [jax.ShapeDtypeStruct((2,) + red.shape, F32)],
        grid=grid,
        in_specs=in_specs + [ANY] * len(weights),
        out_specs=[ANY] * 6,
        scratch_shapes=scratch + [pltpu.VMEM((slots, d, tok // slots), BF16), pltpu.VMEM((d, d), BF16)] + SEMS,
        compiler_params=params(2, 2),
        name='attn_first',
    )(x, dy, w, partial, *weights)


def attn_last(layer, x, dy, w, partial):
    grid, in_specs, scratch, red, tok = attn_specs(layer, x, w)
    slots, nw, d = w.shape
    seq = x.shape[2]
    return pl.pallas_call(
        attn_last_kernel,
        out_shape=[jax.ShapeDtypeStruct((x.shape[1], seq, d), BF16), red, jax.ShapeDtypeStruct(red.shape[1:], F32)],
        grid=grid,
        in_specs=in_specs,
        out_specs=[ANY] * 3,
        scratch_shapes=scratch + [pltpu.VMEM((slots, seq, d), BF16), pltpu.SemaphoreType.REGULAR((4,))] + SEMS,
        compiler_params=params(3, 2),
        name='attn_last',
    )(x, dy, w, partial)


def finish_kernel(dxg, ra0, ra1, rm0, rm1, dx, g_qkv, g_out, g_down, g_up, buf, wide, mlp, tq, to, sems):
    n = dxg.shape[0]
    nq = tq.shape[1]
    count = [n]

    def copy(src, dst, i=None):
        if i is None:
            i = count[0]
            count[0] += 1
        return pltpu.make_async_copy(src, dst, sems.at[i])
    small = [copy(ra0, wide.at[0]), copy(ra1, wide.at[1]), copy(rm0, mlp.at[0]), copy(rm1, mlp.at[1])]
    first = count[0]
    for c in small:
        c.start()

    def load(i, carry):
        copy(dxg.at[i], buf.at[i], i).start()
        return carry
    lax.fori_loop(0, n, load, 0)
    for c in small:
        c.wait()
    out = [copy(mlp.at[k, j], g.at[k]) for j, g in enumerate((g_down, g_up)) for k in range(2)]
    for c in out:
        c.start()

    def move(i, carry):
        copy(dxg.at[i], buf.at[i], i).wait()
        copy(buf.at[i], dx.at[i], i).start()
        return carry
    lax.fori_loop(0, n, move, 0)
    for k in range(2):
        tq[k] = wide[k, :, :nq].T
        to[k] = wide[k, :, nq:].T
    last = [copy(tq, g_qkv), copy(to, g_out)]
    for c in last:
        c.start()

    def done(i, carry):
        copy(buf.at[i], dx.at[i], i).wait()
        return carry
    lax.fori_loop(0, n, done, 0)
    for c in out + last:
        c.wait()


def finish(nq, dxg, ra0, ra1, rm0, rm1):
    rows, d = ra0.shape
    shapes = [dxg.shape, (2, nq, rows), (2, d - nq, rows), (2, rows, d), (2, rows, d)]
    return pl.pallas_call(
        finish_kernel,
        out_shape=[jax.ShapeDtypeStruct(shapes[0], BF16)] + [jax.ShapeDtypeStruct(shape, F32) for shape in shapes[1:]],
        in_specs=[ANY] * 5,
        out_specs=[ANY] * 5,
        scratch_shapes=[pltpu.VMEM(dxg.shape, BF16), pltpu.VMEM((2, rows, d), F32), pltpu.VMEM((2,) + rm0.shape, F32), pltpu.VMEM(shapes[1], F32),
                        pltpu.VMEM(shapes[2], F32), pltpu.SemaphoreType.DMA((32,))],
        compiler_params=pltpu.CompilerParams(vmem_limit_bytes=VMEM_LIMIT),
        name='finish',
    )(dxg, ra0, ra1, rm0, rm1)


def solution(mesh):
    assert dict(mesh.shape) == {'dpy': 2, 'dpx': 2, 'tp': SLOTS}
    act_spec = P(None, DATA_AXES, None, None)

    def device_backward(x_saved, y_saved, dz_top, w_qkv, w_out, w_up, w_down):
        layers, d = w_up.shape[:2]
        assert layers == 2
        heads, hd = w_out.shape[1:3]
        n = 3 * heads * hd
        wq = w_qkv.transpose(0, 2, 3, 4, 1).reshape(layers, n, d)
        wo = w_out.reshape(layers, heads * hd, d)
        dy1, gm1, wa1 = mlp_first(1, y_saved, dz_top, w_up, w_down, wq, wo)
        dx1, ga1, w1_0, w2_0, wa0, half = attn_first(1, x_saved, dy1, wa1, gm1, w_up, w_down, wq, wo)
        dy0, gm0, ra1, rm1 = mlp_second(0, y_saved, dx1, w1_0, w2_0, ga1, half)
        d_input, rm0, ra0 = attn_last(0, x_saved, dy0, wa0, gm0)
        d_input, g_qkv, g_out, g_down, g_up = finish(n, d_input, ra0, ra1, rm0, rm1)
        g_qkv = g_qkv.reshape(layers, 3, heads, hd, d // 4).transpose(0, 4, 1, 2, 3)
        return d_input, g_qkv, g_out.reshape(layers, heads, hd, d // 4), g_up, g_down

    tp_last = P(None, None, None, 'tp', None), P(None, 'tp', None, None), P(None, None, 'tp'), P(None, 'tp', None)
    return jax.shard_map(device_backward, mesh=mesh,
                         in_specs=(act_spec, act_spec, P(DATA_AXES, None, None)) + tp_last,
                         out_specs=(P(DATA_AXES, None, None), P(None, DATA_AXES, None, 'tp', None), P(None, 'tp', None, DATA_AXES), P(None, DATA_AXES, 'tp'), P(None, ('tp', 'dpy', 'dpx'), None)),
                         check_vma=False)
```

```python
import functools
import math
import re

import jax
import jax.numpy as jnp
from jax import lax
from jax.experimental import pallas as pl
from jax.experimental.pallas import tpu as pltpu
from jax.sharding import PartitionSpec as P

DATA_AXES = ('dpy', 'dpx')
F32 = jnp.float32
BF16 = jnp.bfloat16
HEAD = 64
SLOTS = 4
LOOK_AHEAD = 3
PIECES = 8
BOTH = range(2)
NN = (((1,), (0,)), ((), ()))
NT = (((1,), (1,)), ((), ()))
VMEM_LIMIT = 66060288
MESH = pl.DeviceIdType.MESH
ANY = pl.BlockSpec(memory_space=pl.ANY)


def dot(a, b, dims):
    return lax.dot_general(a, b, dims, preferred_element_type=F32)


class Peers:
    def __init__(self):
        z, y, t = lax.axis_index('dpy'), lax.axis_index('dpx'), lax.axis_index('tp')
        self.z, self.y, self.t = z, y, t
        self.sib = (z, y, t + 1 - 2 * (t % 2))
        self.xp = (z, y, (t + 2) % 4)
        self.yp = (z, 1 - y, t)
        self.zp = (1 - z, y, t)

    def arrive(self):
        for peer in (self.sib, self.xp, self.yp, self.zp):
            pl.semaphore_signal(pltpu.get_barrier_semaphore(), inc=1, device_id=peer, device_id_type=MESH)

    def barrier(self):
        with jax.named_scope('entry'):
            pl.semaphore_wait(pltpu.get_barrier_semaphore(), 4)

    def rel(self, d):
        zr = self.z if d // 2 == 0 else 1 - self.z
        yr = self.y if d % 2 == 0 else 1 - self.y
        return zr * 2 + yr


class Sems:
    def __init__(self, send, recv, local):
        self.send, self.recv, self.local = send, recv, local
        self.n = self.m = 0

    def remote(self, src, dst, peer):
        i = self.n
        self.n += 1
        return lambda: pltpu.make_async_remote_copy(src_ref=src(), dst_ref=dst(), send_sem=self.send.at[i], recv_sem=self.recv.at[i],
                                                    device_id=peer, device_id_type=MESH)

    def copy(self, src, dst):
        i = self.m
        self.m += 1
        return lambda: pltpu.make_async_copy(src(), dst(), self.local.at[i])

    def copies(self, n, src, dst):
        first = self.m
        self.m += n
        return lambda i: pltpu.make_async_copy(src(i), dst(i), self.local.at[first + i])


def at_ticks(actions, tick, position=0, points=1):
    for k in sorted(actions):
        if k % points == position:
            @pl.when(tick == k)
            def _(k=k):
                with jax.named_scope('t%d' % k):
                    for action in actions[k]:
                        action()


class Scatter:
    def __init__(self, sems, peers, partial, mine, bufs, out, rows, load=True, half_out=None, part=None):
        r0, r1, r2, r3 = self.bufs = bufs
        self.mine, self.all = mine, pl.ds(*rows)
        first, count = part or rows
        h = count // 2
        self.part, self.lo, self.hi = pl.ds(first, count), pl.ds(first, h), pl.ds(first + h, h)
        self.half = half = pl.ds(first // 2, h)
        every, lo, hi = self.all, self.lo, self.hi
        self.load, self.c0, self.c1, self.c2 = [], [], [], []
        for x in BOTH:
            def near(k, part, x=x):
                return lambda: mine(x).at[k, part]

            def place(buf, *index):
                return lambda: buf.at[index]
            if load:
                self.load.append(sems.copy(lambda x=x: partial(2 * x).at[:, every], near(slice(None), every)))
            self.c0.append(sems.remote(lambda x=x: partial(2 * x + 1).at[:, every], place(r0, x, slice(None), every), peers.sib))
            self.c1.append([sems.remote(near(2 * k + 1, lo), place(r1, 0, x, k, half), peers.yp) for k in BOTH]
                           + [sems.remote(near(2 + k, hi), place(r1, 1, x, k, half), peers.zp) for k in BOTH])
            self.c2.append([sems.remote(near(2, lo), place(r2, 0, x, half), peers.zp), sems.remote(near(1, hi), place(r2, 1, x, half), peers.yp)])
        if half_out is None:
            self.c3 = sems.remote(lambda: mine(1).at[0, self.part], place(r3, self.part), peers.xp)
            self.store = [sems.copy(lambda: mine(0).at[0, every], out)]
        else:
            self.c3 = None
            self.store = [sems.copy(lambda x=x: mine(x).at[0, every], lambda x=x: half_out(x)) for x in BOTH]

    def start(self, x):
        self.c0[x]().start()
        if self.load:
            self.load[x]().start()

    def add0(self, x):
        if self.load:
            self.load[x]().wait()
        self.c0[x]().wait_recv()
        mine, r0 = self.mine(x), self.bufs[0].at[x]

        def body(k, carry):
            mine[k, self.all] = mine[k, self.all] + r0[k, self.all]
            return carry
        lax.fori_loop(0, 4, body, 0)

    def send1(self, x):
        for c in self.c1[x]:
            c().start()

    def add1(self, x):
        for c in self.c1[x]:
            c().wait_recv()
        mine, r1 = self.mine(x), self.bufs[1]

        def body(k, carry):
            mine[2 * k, self.lo] = mine[2 * k, self.lo] + r1[0, x, k, self.half]
            mine[k, self.hi] = mine[k, self.hi] + r1[1, x, k, self.half]
            return carry
        lax.fori_loop(0, 2, body, 0)

    def send2(self, x):
        for c in self.c2[x]:
            c().start()

    def add2(self, x):
        for c in self.c2[x]:
            c().wait_recv()
        mine, r2 = self.mine(x), self.bufs[2]
        mine[0, self.lo] = mine[0, self.lo] + r2[0, x, self.half]
        mine[0, self.hi] = mine[0, self.hi] + r2[1, x, self.half]

    def send3(self):
        self.c3().start()

    def add3(self):
        self.c3().wait_recv()
        mine = self.mine(0)
        mine[0, self.part] = (mine[0, self.part] + self.bufs[3][self.part]) * (1 / SLOTS)

    def out(self):
        for c in self.store:
            c().start()

    def finish(self):
        for c in self.c0 + sum(self.c1, []) + sum(self.c2, []) + ([self.c3] if self.c3 else []):
            c().wait_send()
        for c in self.store:
            c().wait()

    def both(self, name):
        for x in BOTH:
            getattr(self, name)(x)


class Across:
    def __init__(self, sems, peers, mine, bufs, rows, turn):
        self.rx, self.ra, self.rb = bufs
        mine_of, part = mine, pl.ds(*rows)
        self.mine, self.part = mine(0), part
        far, second = 1 + turn, 2 - turn
        self.near = (0, second)
        order = (peers.yp, peers.zp)
        self.go = [[sems.remote(lambda: mine_of(1).at[:, part], lambda: self.rx, peers.xp)],
                   [sems.remote(lambda k=k: self.mine.at[k, part], lambda i=i: self.ra.at[i], order[turn]) for i, k in enumerate((far, 3))],
                   [sems.remote(lambda: self.mine.at[second, part], lambda: self.rb, order[1 - turn])]]

    def send(self, i):
        for c in self.go[i]:
            c().start()

    def add(self, i):
        for c in self.go[i]:
            c().wait_recv()
        mine, part = self.mine, self.part
        if i == 0:
            for k in range(4):
                mine[k, part] = mine[k, part] + self.rx[k]
        elif i == 1:
            for n, k in enumerate(self.near):
                mine[k, part] = mine[k, part] + self.ra[n]
        else:
            mine[0, part] = (mine[0, part] + self.rb[:]) * (1 / SLOTS)

    def both(self, name):
        getattr(self, name[:-1])(int(name[-1]))

    def finish(self):
        for c in sum(self.go, []):
            c().wait_send()


def scatter_bufs(rows, d):
    return [pltpu.VMEM((2, 4, rows, d), F32), pltpu.VMEM((2, 2, 2, rows // 2, d), F32), pltpu.VMEM((2, 2, rows // 2, d), F32), pltpu.VMEM((rows, d), F32)]


def steps(job, plan):
    out = []
    for tick, name, half in re.findall('([0-9]+)([a-z]+[0-3]?)([xy]?)', plan):
        if half:
            action = functools.partial(getattr(job, name), int(half == 'y'))
        else:
            action = functools.partial(job.both, name) if name[-1] in '012' else getattr(job, name)
        out.append((int(tick), action))
    return out


def ticks(plan, actions):
    return list(zip(map(int, plan.split(',')), actions))


class Gather:
    def __init__(self, sems, peers, blocks):
        self.sib = [sems.remote(own, lambda dst=dst: dst(1), peers.sib) for own, dst in blocks]
        self.xp = [sems.remote(own, lambda dst=dst: dst(2), peers.xp) for own, dst in blocks]
        self.fwd = [sems.remote(lambda dst=dst: dst(2), lambda dst=dst: dst(3), peers.sib) for own, dst in blocks]

    def start(self, blocks):
        for i in blocks:
            self.sib[i]().start()
            self.xp[i]().start()

    def forward(self, i):
        self.xp[i]().wait_recv()
        self.fwd[i]().start()

    def forwards(self):
        return [functools.partial(self.forward, i) for i in range(len(self.fwd))]

    def finish(self):
        for i in range(len(self.sib)):
            self.sib[i]().wait_recv()
            self.fwd[i]().wait_recv()
            self.sib[i]().wait_send()
            self.xp[i]().wait_send()
            self.fwd[i]().wait_send()


class Bounce:
    def __init__(self, sems, items, buf):
        self.steps = []
        prev = None
        for own, dst, rows in items:
            ld = sems.copy(own, lambda rows=rows: buf.at[pl.ds(0, rows)])
            st = sems.copy(lambda rows=rows: buf.at[pl.ds(0, rows)], lambda dst=dst: dst(0))
            self.steps.append(functools.partial(self.load, prev, ld))
            self.steps.append(functools.partial(self.flip, ld, st))
            prev = st
        self.steps.append(lambda prev=prev: prev().wait())

    @staticmethod
    def load(prev, ld):
        if prev is not None:
            prev().wait()
        ld().start()

    @staticmethod
    def flip(ld, st):
        ld().wait()
        st().start()


def merge(*lists):
    actions = {}
    for pairs in lists:
        for k, action in pairs:
            actions.setdefault(k, []).append(action)
    return actions


SEMS = [pltpu.SemaphoreType.DMA((96,)), pltpu.SemaphoreType.DMA((96,)), pltpu.SemaphoreType.DMA((32,))]


def leading(*shape):
    return pl.BlockSpec((1,) + shape, lambda j, *_: (j,) + (0,) * len(shape))


def params(collective_id, axes):
    return pltpu.CompilerParams(vmem_limit_bytes=VMEM_LIMIT, dimension_semantics=('arbitrary',) * axes, collective_id=collective_id, has_side_effects=True)


def mlp_slot(slot, seqs, seq, w1, w2, w1t, yt, dz, acc, gt, dht, tick, arrive, emit):
    w1t[:] = w1[:].T

    def block(i, carry):
        tick(i)
        with jax.named_scope('arrive'):
            pl.when(slot == 0)(lambda: arrive(i))
        cols = pl.ds(pl.multiple_of(i * seq, seq), seq)
        h = dot(w1t[:], yt[:, cols], NN)
        dg = dot(w2[:], dz[:, cols], NN)
        c0 = math.sqrt(2 / math.pi)
        c1 = 0.044715 * c0
        h2 = h * h
        t = jnp.tanh(h * (c0 + c1 * h2))
        q = 0.5 * t + 0.5
        g = h * q
        dh = dg * (q + (g * (1.0 - t)) * (c0 + (3 * c1) * h2))
        gt[:, cols] = g.astype(BF16)
        dh = dh.astype(BF16)
        dht[:, cols] = dh
        acc[:, cols] += dot(w1[:], dh, NN)
        with jax.named_scope('memit'):
            pl.when(slot == SLOTS - 1)(lambda: emit(i))
        return carry
    lax.fori_loop(0, seqs, block, 0)


def tokens(i, seq):
    return pl.ds(pl.multiple_of(i * seq, seq), seq)


class MlpIo:
    def __init__(self, sems, peers, seqs, seq, loads, acc, dz, dyb, dy_hbm, gbuf, g_hbm):
        self.seqs, self.seq, self.peers = seqs, seq, peers
        self.loads, self.acc, self.dz, self.dyb, self.gbuf = loads, acc, dz, dyb, gbuf
        self.dy = sems.copies(seqs, lambda i: dyb.at[:, tokens(i, seq)], lambda i: dy_hbm.at[:, tokens(i, seq)])
        self.g = [sems.copy(lambda j=j: gbuf.at[j], lambda j=j: g_hbm.at[pl.program_id(0), j]) for j in BOTH]

    def start(self):
        for load, _ in self.loads:
            for i in range(self.seqs):
                load(i).start()

    def arrive(self, i):
        for load, use in self.loads:
            load(i).wait()
            use(i)
        cols = tokens(i, self.seq)
        self.acc[:, cols] = jnp.zeros((self.acc.shape[0], self.seq), F32)

    def emit(self, i):
        cols = tokens(i, self.seq)
        self.dyb[:, cols] = (self.dz[:, cols].astype(F32) + self.acc[:, cols]).astype(BF16)
        self.dy(i).start()

    def grads(self, j, a, b):
        pl.when(pl.program_id(0) > 0)(lambda: self.g[j]().wait())
        rows, width = self.gbuf.shape[-2:]
        split, half = width * 2 // 3, width // 2
        for lo, hi, c0, c1 in ((0, width, 0, split), (0, half, split, width), (half, width, split, width)):
            g = dot(a[lo:hi], b[c0:c1], NT)
            for k in range(g.shape[0] // rows):
                self.gbuf[j, self.peers.rel(lo // rows + k), :, c0:c1] = g[k * rows:(k + 1) * rows]
        self.g[j]().start()

    def finish(self):
        for i in range(self.seqs):
            self.dy(i).wait()
        for c in self.g:
            c().wait()


def mlp_rest(slot, actions, io, w1, w2, w1t, yt, gt, dht):
    seqs, seq, dz, acc = io.seqs, io.seq, io.dz, io.acc
    points = seqs + 2
    first = slot * points

    def tick(i):
        at_ticks({k: v for k, v in actions.items() if k % points < seqs}, first + i)
    mlp_slot(slot, seqs, seq, w1, w2, w1t, yt, dz, acc, gt, dht, tick, io.arrive, io.emit)
    at_ticks(actions, first + seqs, seqs, points)
    with jax.named_scope('dw2'):
        io.grads(0, gt, dz)
    at_ticks(actions, first + seqs + 1, seqs + 1, points)
    with jax.named_scope('dw1'):
        io.grads(1, yt, dht)


def attn_weights(layer, wq, wo, wa_g):
    nq, d = wq.shape[1:]
    return [(lambda: wq.at[layer], lambda j: wa_g.at[j, pl.ds(0, nq)], nq), (lambda: wo.at[layer], lambda j: wa_g.at[j, pl.ds(nq, d - nq)], d - nq)]


class Spread:
    def __init__(self, sems, peers, wb, pieces):
        rows = wb.shape[2] // pieces
        y = peers.y

        def piece(slot, m, k):
            return lambda: wb.at[slot, m, pl.ds(k * rows, rows)]
        every = range(pieces)
        self.sib = sems.remote(lambda: wb.at[0], lambda: wb.at[1], peers.sib)
        self.xp = [sems.remote(piece(0, y, k), piece(2, y, k), peers.xp) for k in every]
        self.fy, self.wy = [], []
        for k in every:
            self.fy.append(sems.remote(piece(2, y, k), piece(2, y, k), peers.yp))
            sems.n -= 1
            self.wy.append(sems.remote(piece(2, 1 - y, k), piece(2, 1 - y, k), peers.yp))
        self.fs = [sems.remote(piece(2, y, k), piece(3, y, k), peers.sib) for k in every]
        self.fs2 = [sems.remote(piece(2, 1 - y, k), piece(3, 1 - y, k), peers.sib) for k in every]

    def start(self):
        for c in self.xp + [self.sib]:
            c().start()

    def forward(self, k):
        self.xp[k]().wait_recv()
        self.fy[k]().start()
        self.fs[k]().start()

    def forward2(self, k):
        self.wy[k]().wait_recv()
        self.fs2[k]().start()

    def arrived(self):
        for c in self.fs + self.fs2:
            c().wait_recv()

    def finish(self):
        for c in [self.sib] + self.xp + self.fy + self.fs + self.fs2:
            c().wait_send()


def turned(src, dst, seq):
    def use(i):
        dst[:, tokens(i, seq)] = src[i].T
    return use


def mlp_first_kernel(layer, y, dz_in, wup, wdn, wq, wo, dy_hbm, g_hbm, wa_g, yb, dzb, yt, dzt, acc, w1t, gt, dht, wb, bounce, dyb, gbuf, *rest):
    slot = pl.program_id(0)
    seqs, seq = yb.shape[:2]
    peers, sems = Peers(), Sems(*rest)
    mine = peers.t * seqs
    loads = [(sems.copies(seqs, lambda i: y.at[layer, mine + i], lambda i: yb.at[i]), turned(yb, yt, seq)),
             (sems.copies(seqs, lambda i: dz_in.at[mine + i], lambda i: dzb.at[i]), turned(dzb, dzt, seq))]
    io = MlpIo(sems, peers, seqs, seq, loads, acc, dzt, dyb, dy_hbm, gbuf, g_hbm)
    own = [sems.copy(lambda w=w: w.at[layer], lambda m=m: wb.at[0, m]) for m, w in enumerate((wup, wdn))]
    blocks = attn_weights(layer, wq, wo, wa_g)
    gather = Gather(sems, peers, [r[:2] for r in blocks])
    hop = Bounce(sems, blocks, bounce)
    spread = Spread(sems, peers, wb, PIECES)

    @pl.when(slot == 0)
    def _():
        with jax.named_scope('e56'):
            for c in own:
                c().start()
        with jax.named_scope('e57'):
            io.start()
        with jax.named_scope('e58'):
            peers.arrive()
        with jax.named_scope('e59'):
            peers.barrier()
        with jax.named_scope('e60'):
            for c in own:
                c().wait()
        with jax.named_scope('e61'):
            spread.start()
        with jax.named_scope('e62'):
            gather.start(BOTH)

    @pl.when(slot == 1)
    def _():
        with jax.named_scope('e55'):
            spread.sib().wait_recv()

    @pl.when(slot == 2)
    def _():
        with jax.named_scope('e54'):
            for k in range(5, PIECES):
                spread.forward2(k)

    @pl.when(slot == 3)
    def _():
        with jax.named_scope('e53'):
            spread.arrived()
    every = range(PIECES)
    actions = merge([(14 + k, s) for k, s in enumerate(hop.steps)], ticks('2,3,4,5,7,8,9,10', [functools.partial(spread.forward, k) for k in every]),
                    ticks('7,8,9,10,11', [functools.partial(spread.forward2, k) for k in every]), ticks('21', gather.forwards()))
    mlp_rest(slot, actions, io, wb.at[slot, 0], wb.at[slot, 1], w1t, yt, gt, dht)

    @pl.when(slot == SLOTS - 1)
    def _():
        with jax.named_scope('e49'):
            gather.forward(1)
        with jax.named_scope('e50'):
            io.finish()
        with jax.named_scope('e51'):
            spread.finish()
        with jax.named_scope('e52'):
            gather.finish()


def mlp_first(layer, y, dz, wup, wdn, wq, wo):
    d, f = wup.shape[1:]
    seq = y.shape[2]
    seqs = y.shape[1] // SLOTS
    tok = seqs * seq
    return pl.pallas_call(
        functools.partial(mlp_first_kernel, layer),
        out_shape=(jax.ShapeDtypeStruct((d, tok), BF16), jax.ShapeDtypeStruct((SLOTS, 2, 4, d // 4, f), F32), jax.ShapeDtypeStruct((SLOTS, d, d), BF16)),
        grid=(SLOTS,),
        in_specs=[ANY] * 6,
        out_specs=[ANY] * 3,
        scratch_shapes=[pltpu.VMEM((seqs, seq, d), BF16)] * 2 + [pltpu.VMEM((d, tok), BF16)] * 2
        + [pltpu.VMEM((d, tok), F32), pltpu.VMEM((f, d), BF16), pltpu.VMEM((f, tok), BF16), pltpu.VMEM((f, tok), BF16), pltpu.VMEM((SLOTS, 2, d, f), BF16),
           pltpu.VMEM((d, d), BF16), pltpu.VMEM((d, tok), BF16), pltpu.VMEM((2, 4, d // 4, f), F32)] + SEMS,
        compiler_params=params(0, 1),
        name='mlp_first',
    )(y, dz, wup, wdn, wq, wo)


def mlp_second_kernel(layer, w1_ref, w2_ref, y, dz_in, partial, half, dy_hbm, g_hbm, red, red_half, yb, yt, dzt, acc, w1t, gt, dht, dyb, gbuf, mine, *rest):
    slot = pl.program_id(0)
    seqs, seq = yb.shape[:2]
    bufs, rest = rest[:4], rest[4:]
    peers, sems = Peers(), Sems(*rest[2:])
    place = peers.t * seqs
    loads = [(sems.copies(seqs, lambda i: y.at[layer, place + i], lambda i: yb.at[i]), turned(yb, yt, seq)),
             (sems.copies(seqs, lambda i: dz_in.at[:, tokens(i, seq)], lambda i: dzt.at[:, tokens(i, seq)]), lambda i: None)]
    io = MlpIo(sems, peers, seqs, seq, loads, acc, dzt, dyb, dy_hbm, gbuf, g_hbm)
    rows = mine.shape[2] // 2
    a, b = jobs = [Scatter(sems, peers, lambda s: partial.at[s], lambda x: mine.at[x], bufs, lambda j=j: red.at[pl.ds(j * rows, rows)], (j * rows, rows)) for j in BOTH]

    h0, h1 = rest[:2]
    mine_half = sems.copy(lambda: half.at[0], lambda: h0)
    x_half = sems.remote(lambda: half.at[1], lambda: h1, peers.xp)
    store_half = sems.copy(lambda: h0, lambda: red_half)

    def add_half():
        mine_half().wait()
        x_half().wait_recv()
        h0[:] = (h0[:] + h1[:]) * (1 / SLOTS)

    @pl.when(slot == 0)
    def _():
        with jax.named_scope('e43'):
            io.start()
        with jax.named_scope('e44'):
            peers.arrive()
        with jax.named_scope('e45'):
            peers.barrier()
        with jax.named_scope('e46'):
            for job in jobs:
                job.both('start')
        with jax.named_scope('e47'):
            x_half().start()
        with jax.named_scope('e48'):
            mine_half().start()
    actions = merge(ticks('17,18', [add_half, lambda: store_half().start()]),
                    steps(a, '3add0,3send1,9add1,9send2,17add2,17send3,21add3,22out'),
                    steps(b, '4add0,4send1,14add1,14send2,19add2,19send3,23add3'))
    mlp_rest(slot, actions, io, w1_ref.at[0], w2_ref.at[0], w1t, yt, gt, dht)

    @pl.when(slot == SLOTS - 1)
    def _():
        with jax.named_scope('e37'):
            b.out()
        with jax.named_scope('e38'):
            io.finish()
        with jax.named_scope('e39'):
            x_half().wait_send()
        with jax.named_scope('e40'):
            store_half().wait()
        with jax.named_scope('e41'):
            a.finish()
        with jax.named_scope('e42'):
            b.finish()


def mlp_second(layer, y, dz, w1, w2, partial, half):
    d, f = w1.shape[1:]
    seq = y.shape[2]
    seqs = y.shape[1] // SLOTS
    tok = seqs * seq
    return pl.pallas_call(
        functools.partial(mlp_second_kernel, layer),
        out_shape=(jax.ShapeDtypeStruct((d, tok), BF16), jax.ShapeDtypeStruct((SLOTS, 2, 4, d // 4, f), F32),
                   jax.ShapeDtypeStruct((d // 4, d), F32), jax.ShapeDtypeStruct(half.shape[1:], F32)),
        grid=(SLOTS,),
        in_specs=[leading(d, f), leading(f, d)] + [ANY] * 4,
        out_specs=[ANY] * 4,
        scratch_shapes=[pltpu.VMEM((seqs, seq, d), BF16), pltpu.VMEM((d, tok), BF16), pltpu.VMEM((d, tok), BF16), pltpu.VMEM((d, tok), F32), pltpu.VMEM((f, d), BF16),
                        pltpu.VMEM((f, tok), BF16), pltpu.VMEM((f, tok), BF16), pltpu.VMEM((d, tok), BF16),
                        pltpu.VMEM((2, 4, d // 4, f), F32), pltpu.VMEM((2, 4, d // 4, d), F32)]
        + scatter_bufs(d // 4, d) + [pltpu.VMEM(half.shape[1:], F32)] * 2 + SEMS,
        compiler_params=params(1, 1),
        name='mlp_second',
    )(w1, w2, y, dz, partial, half)


def attn_step(sems, peers, x_ref, dy_hbm, w_hbm, dy_ref, w_ref, xt, acc, gacc, qkv, do, b1, b2, begin, act, emit, ending=lambda: None):
    s, slot = pl.program_id(0), pl.program_id(1)
    step = s * SLOTS + slot
    last = SLOTS * SLOTS - 1
    before = jnp.maximum(step - 1, 0)
    seq, d = x_ref.shape[-2:]
    nqkv = qkv.shape[0]
    third = nqkv // 3
    split = d - b2.shape[1]
    rows = d // 4

    load_w = sems.copies(SLOTS, lambda i: w_hbm.at[i], lambda i: w_ref.at[i])
    load_dy = sems.copies(SLOTS, lambda i: dy_hbm.at[:, tokens(i, seq)], lambda i: dy_ref.at[:, tokens(i, seq)])

    @pl.when(step == 0)
    def _():
        for i in range(SLOTS):
            load_w(i).start()
            load_dy(i).start()
        peers.arrive()
        def clear(j, carry):
            gacc[j // 4, j % 4] = jnp.zeros(gacc.shape[2:], F32)
            b1[j % 2] = jnp.zeros(b1.shape[1:], BF16)
            b2[j % 2] = jnp.zeros(b2.shape[1:], BF16)
            return carry
        lax.fori_loop(0, SLOTS * 4, clear, 0)
        begin()
    act()
    with jax.named_scope('loadw'):
        pl.when(s == 0)(lambda: load_w(slot).wait())

    @pl.when(slot == 0)
    def _():
        with jax.named_scope('e35'):
            load_dy(s).wait()
        with jax.named_scope('e36'):
            xt[s % 2] = x_ref[0, 0].T

    def grads(n, par):
        ps, pj = n // SLOTS, n % SLOTS
        third_d = d // 3

        def weights(c):
            cols = slice(c * third_d, (c + 1) * third_d)
            g = dot(xt[ps % 2], b1[par, cols], NT)
            if c == 2:
                g = g + dot(dy_ref[:, tokens(ps, seq)], b2[par], NT)
            for k in range(4):
                r = peers.rel(k)
                gacc[pj, r, :, cols] = gacc[pj, r, :, cols] + g[k * rows:(k + 1) * rows]

        def inputs(c):
            part = slice(c * third_d, (c + 1) * third_d)
            acc[part] += dot(w_ref[pj, :, part].T, b1[par], NN)
        return [functools.partial(f, c) for c in range(3) for f in (weights, inputs)]
    with jax.named_scope("main"):
        x_t = xt[s % 2]
        dy_t = dy_ref[:, tokens(s, seq)]
        now = step % 2
        qkv[:] = dot(w_ref[slot, pl.ds(0, nqkv), :], x_t, NN).astype(BF16)
        do[:] = dot(w_ref[slot, pl.ds(nqkv, d - nqkv), :], dy_t, NN).astype(BF16)
        scale = HEAD ** -0.5
        exp_scale = scale * math.log2(math.e)
        qb = seq // 2
        units = [(h, slice(c * qb, (c + 1) * qb)) for h in range(third // HEAD) for c in BOTH]

        def scores(h, qc):
            q_rows, k_rows, v_rows = head_rows(h)
            return dot(qkv[k_rows, :].T, qkv[q_rows, qc], NN), dot(qkv[v_rows, :].T, do[q_rows, qc] * scale, NN)

        def head_rows(h):
            return [slice(i * third + h * HEAD, i * third + (h + 1) * HEAD) for i in range(3)]
        for piece in grads(before, 1 - step % 2):
            piece()
        ahead = [scores(*unit) for unit in units[:LOOK_AHEAD]]
        for n, (h, qc) in enumerate(units):
            sc, dp_t = ahead.pop(0)
            if n + LOOK_AHEAD < len(units):
                ahead.append(scores(*units[n + LOOK_AHEAD]))
            q_rows, k_rows, v_rows = head_rows(h)
            m = jnp.max(sc, axis=0, keepdims=True)
            e = jnp.exp2((sc - m) * exp_scale)
            inv = 1.0 / jnp.sum(e, axis=0, keepdims=True)
            rd = jnp.sum(e * dp_t, axis=0, keepdims=True) * inv
            p = e * inv
            p_bf = p.astype(BF16)
            ds = (p * (dp_t - rd)).astype(BF16)
            b2[now, pl.ds(b2.shape[1] - third + h * HEAD, HEAD), qc] = dot(qkv[v_rows, :], p_bf, NN).astype(BF16)
            b1[now, q_rows, qc] = dot(qkv[k_rows, :], ds, NN).astype(BF16)
            dv_c = dot(do[q_rows, qc], p_bf, NT)
            dk_c = dot(qkv[q_rows, qc], ds, NT)
            if n % 2 == 0:
                dv, dk = dv_c, dk_c
            else:
                b1[now, k_rows] = (dk + dk_c).astype(BF16)
                b1[now, v_rows] = (dv + dv_c).astype(BF16)

    @pl.when(slot == 0)
    def _():
        @pl.when(s > 0)
        def _():
            emit(s - 1)
        acc[:] = dy_ref[:, tokens(s, seq)].astype(F32)

    @pl.when(step == last)
    def _():
        with jax.named_scope('e32'):
            ending()
        with jax.named_scope('e33'):
            for piece in grads(last, last % 2):
                piece()
        with jax.named_scope('e34'):
            emit(s)


ATTN_IN = 3
ATTN_SCRATCH = 9
JOB_PLAN = '1add0,1send1,6add1,6send2,11add2', '3add0,3send1x,6send1y,9add1x,9send2x,14add1y,14send2y'


def attn_first_kernel(layer, x_ref, dy_hbm, w_hbm, partial, wup, wdn, wq, wo, dx_hbm, g_hbm, w1_g, w2_g, wa_g, half, *rest):
    body, rest = rest[:ATTN_SCRATCH], rest[ATTN_SCRATCH:]
    acc, gacc, mine, bounce = body[3], body[4], rest[:2], rest[-4]
    seq = x_ref.shape[-2]
    step = pl.program_id(0) * SLOTS + pl.program_id(1)
    peers, sems = Peers(), Sems(*rest[-3:])
    a, b = jobs = [Scatter(sems, peers, lambda s, j=j: partial.at[s, j], lambda x, j=j: mine[j].at[x], rest[2 + 4 * j:6 + 4 * j], None,
                           (0, half.shape[2]), half_out=lambda x, j=j: half.at[x, j]) for j in BOTH]
    blocks = [(lambda w=w: w.at[layer - 1], lambda j, g=g: g.at[j], wup.shape[1]) for w, g in ((wup, w1_g), (wdn, w2_g))] + attn_weights(layer - 1, wq, wo, wa_g)
    gather = Gather(sems, peers, [r[:2] for r in blocks])
    hop = Bounce(sems, blocks, bounce)
    stores = [sems.copy(lambda j=j: gacc.at[j], lambda j=j: g_hbm.at[j]) for j in range(SLOTS)]
    actions = merge(steps(a, JOB_PLAN[0]), steps(b, JOB_PLAN[1]), [(5 + k, s) for k, s in enumerate(hop.steps)],
                    ticks('6,11,15,15', gather.forwards()), ticks('14,15,12', [lambda c=c: c().start() for c in stores[:2]] + [a.out]))

    dxb = rest[-5]
    store_dx = sems.copies(SLOTS, lambda i: dxb.at[i], lambda i: dx_hbm.at[:, tokens(i, seq)])

    def begin():
        peers.barrier()
        for job in jobs:
            job.both('start')
        gather.start(range(len(blocks)))

    def emit(s):
        dxb[s] = acc[:].astype(BF16)
        store_dx(s).start()
    attn_step(sems, peers, x_ref, dy_hbm, w_hbm, *body, begin, lambda: at_ticks(actions, step), emit, lambda: stores[2]().start())

    @pl.when(step == SLOTS * SLOTS - 1)
    def _():
        with jax.named_scope('e25'):
            stores[3]().start()
        with jax.named_scope('e26'):
            b.both('add2')
        with jax.named_scope('e27'):
            gather.finish()
        with jax.named_scope('e28'):
            b.out()
        with jax.named_scope('e29'):
            for c in stores:
                c().wait()
        with jax.named_scope('e30'):
            for i in range(SLOTS):
                store_dx(i).wait()
        with jax.named_scope('e31'):
            for job in jobs:
                job.finish()


def attn_last_kernel(x_ref, dy_hbm, w_hbm, partial, dxg, red, red_last, *rest):
    body, rest = rest[:ATTN_SCRATCH], rest[ATTN_SCRATCH:]
    acc, gacc, mine, dxb, free = body[3], body[4], rest[:2], rest[-5], rest[-4]
    step = pl.program_id(0) * SLOTS + pl.program_id(1)
    seqs = pl.num_programs(0)
    peers, sems = Peers(), Sems(*rest[-3:])
    nred = red.shape[1]
    a, b = jobs = [Scatter(sems, peers, lambda s, j=j: partial.at[s, j], lambda x, j=j: mine[j].at[x], rest[2 + 4 * j:6 + 4 * j], lambda j=j: red.at[j],
                           (0, nred), part=(0, nred * 3 // 4)) for j in BOTH]
    rows = nred * 3 // 4, nred // 4
    across = [Across(sems, peers, lambda x, j=j: mine[j].at[x], [r.at[j] for r in rest[-8:-5]], rows, j) for j in BOTH]
    h = nred // 2
    ends = [Scatter(sems, peers, lambda s: gacc.at[s], lambda x: gacc.at[2 * x], rest[2:6], lambda j=j: red_last.at[pl.ds(j * h, h)], (j * h, h), load=False)
            for j in BOTH]
    t = peers.t
    t2 = (t + 2) % SLOTS
    sib, xp, fwd, mine_dx = [], [], [], []
    for s in range(SLOTS):
        def src(s=s):
            return dxb.at[s]

        def dst(s=s):
            return dxg.at[t * SLOTS + s]

        def other(s=s):
            return dxg.at[t2 * SLOTS + s]
        mine_dx.append(sems.copy(src, dst))
        sib.append(sems.remote(src, dst, peers.sib))
        xp.append(sems.remote(src, dst, peers.xp))
        fwd.append(sems.remote(other, other, peers.sib))

    def freed(i):
        for peer in ([peers.sib], [peers.yp, peers.zp], [peers.yp, peers.zp], [peers.xp])[i]:
            pl.semaphore_signal(free.at[i], inc=1, device_id=peer, device_id_type=MESH)

    def forward(s):
        xp[s]().wait_recv()
        fwd[s]().start()

    def early():
        pl.semaphore_wait(free.at[0], 1)
        for job in ends:
            job.start(0)

    def early_add():
        pl.semaphore_wait(free.at[1], 2)
        for job in ends:
            job.add0(0)
        for job in ends:
            job.send1(0)
    actions = merge(steps(a, '1add0y,1send1y,3add0x,4add1y,4send2y,7add2y,7send3,10add1x,10send2x'),
                    steps(b, '1add0y,1send1y,3add0x,6add1y,6send2y,9add2y,9send3,11add1x,11send2x'),
                    steps(across[0], '1send0,4add0,4send1,8add1,8send2,13add2'), steps(across[1], '1send0,7add0,7send1,10add1,10send2,13add2'),
                    steps(a, '4send1x'), steps(b, '6send1x'),
                    ticks('4,11,10,15,15', [functools.partial(freed, i) for i in BOTH] + [functools.partial(forward, i) for i in BOTH] + [early]))

    def begin():
        peers.barrier()
        for x in (1, 0):
            for job in jobs:
                job.start(x)

    def emit(s):
        dxb[s] = acc[:].T.astype(BF16)
        for k in range(SLOTS):
            @pl.when(s == k)
            def _(k=k):
                for c in (xp, sib, mine_dx):
                    c[k]().start()
    attn_step(sems, peers, x_ref, dy_hbm, w_hbm, *body, begin, lambda: at_ticks(actions, step), emit, early_add)

    @pl.when(step == SLOTS * SLOTS - 1)
    def _():
        with jax.named_scope('e1'):
            for job in ends:
                job.start(1)
        with jax.named_scope('e2'):
            a.add2(0)
        with jax.named_scope('e3'):
            freed(2)
        with jax.named_scope('e4'):
            a.add3()
        with jax.named_scope('e5'):
            freed(3)
        with jax.named_scope('e6'):
            for job in ends:
                job.add0(1)
        with jax.named_scope('e7'):
            a.out()
        with jax.named_scope('e8'):
            b.add2(0)
        with jax.named_scope('e9'):
            for job in ends:
                job.send1(1)
        with jax.named_scope('e10'):
            b.add3()
        with jax.named_scope('e11'):
            b.out()
        with jax.named_scope('e12'):
            pl.semaphore_wait(free.at[2], 2)
        with jax.named_scope('e13'):
            pl.semaphore_wait(free.at[3], 1)
        with jax.named_scope('e14'):
            for job in ends:
                job.add1(0)
        with jax.named_scope('e15'):
            forward(2)
        with jax.named_scope('e16'):
            for job in ends:
                job.add1(1)
                job.send2(1)
        with jax.named_scope('e17'):
            for job in ends:
                job.send2(0)
        with jax.named_scope('e18'):
            for job in ends:
                job.add2(1)
                job.send3()
        with jax.named_scope('e19'):
            for job in ends:
                job.add2(0)
        with jax.named_scope('e20'):
            forward(3)
        with jax.named_scope('e21'):
            for s in range(SLOTS):
                mine_dx[s]().wait()
                sib[s]().wait()
                xp[s]().wait_send()
        with jax.named_scope('e22'):
            for job in ends:
                job.add3()
                job.out()
        with jax.named_scope('e23'):
            for s in range(SLOTS):
                fwd[s]().wait()
        with jax.named_scope('e24'):
            for job in jobs + ends + across:
                job.finish()


def attn_specs(layer, x, w):
    slots, nw, d = w.shape
    seq = x.shape[2]
    seqs = x.shape[1] // slots
    tok = seqs * seq
    nqkv = nw * 3 // 4
    in_specs = [pl.BlockSpec((1, 1, seq, d), lambda s, j: (layer, lax.axis_index('tp') * seqs + s, 0, 0))] + [ANY] * 3
    scratch = [pltpu.VMEM((d, tok), BF16), pltpu.VMEM((slots, nw, d), BF16), pltpu.VMEM((2, d, seq), BF16), pltpu.VMEM((d, seq), F32), pltpu.VMEM((slots, 4, d // 4, nw), F32), pltpu.VMEM((nqkv, seq), BF16),
               pltpu.VMEM((nw - nqkv, seq), BF16), pltpu.VMEM((2, nw, seq), BF16), pltpu.VMEM((2, d // 3, seq), BF16)]
    scratch += [pltpu.VMEM((2, 4, d // 4, d), F32)] * 2 + scatter_bufs(d // 4, d) * 2
    red = jax.ShapeDtypeStruct((2, d // 4, d), F32)
    return (slots, seqs), in_specs, scratch, red, tok


def attn_first(layer, x, dy, w, partial, *weights):
    grid, in_specs, scratch, red, tok = attn_specs(layer, x, w)
    slots, nw, d = w.shape
    gathered = [jax.ShapeDtypeStruct((slots, d, d), BF16)] * 3
    return pl.pallas_call(
        functools.partial(attn_first_kernel, layer),
        out_shape=[jax.ShapeDtypeStruct((d, tok), BF16), jax.ShapeDtypeStruct((slots, 4, d // 4, nw), F32)] + gathered + [jax.ShapeDtypeStruct((2,) + red.shape, F32)],
        grid=grid,
        in_specs=in_specs + [ANY] * len(weights),
        out_specs=[ANY] * 6,
        scratch_shapes=scratch + [pltpu.VMEM((slots, d, tok // slots), BF16), pltpu.VMEM((d, d), BF16)] + SEMS,
        compiler_params=params(2, 2),
        name='attn_first',
    )(x, dy, w, partial, *weights)


def attn_last(layer, x, dy, w, partial):
    grid, in_specs, scratch, red, tok = attn_specs(layer, x, w)
    slots, nw, d = w.shape
    seq = x.shape[2]
    return pl.pallas_call(
        attn_last_kernel,
        out_shape=[jax.ShapeDtypeStruct((x.shape[1], seq, d), BF16), red, jax.ShapeDtypeStruct(red.shape[1:], F32)],
        grid=grid,
        in_specs=in_specs,
        out_specs=[ANY] * 3,
        scratch_shapes=scratch + [pltpu.VMEM((2, n, d // 16, d), F32) for n in (4, 2)] + [pltpu.VMEM((2, d // 16, d), F32), pltpu.VMEM((slots, seq, d), BF16),
                                                                                         pltpu.SemaphoreType.REGULAR((4,))] + SEMS,
        compiler_params=params(3, 2),
        name='attn_last',
    )(x, dy, w, partial)


def finish_kernel(dxg, ra0, ra1, rm0, rm1, dx, g_qkv, g_out, g_down, g_up, buf, wide, mlp, tq, to, sems):
    n = dxg.shape[0]
    nq = tq.shape[1]
    count = [n]

    def copy(src, dst, i=None):
        if i is None:
            i = count[0]
            count[0] += 1
        return pltpu.make_async_copy(src, dst, sems.at[i])
    small = [copy(ra0, wide.at[0]), copy(ra1, wide.at[1]), copy(rm0, mlp.at[0]), copy(rm1, mlp.at[1])]
    first = count[0]
    for c in small:
        c.start()

    def load(i, carry):
        copy(dxg.at[i], buf.at[i], i).start()
        return carry
    lax.fori_loop(0, n, load, 0)
    for c in small:
        c.wait()
    out = [copy(mlp.at[k, j], g.at[k]) for j, g in enumerate((g_down, g_up)) for k in BOTH]
    for c in out:
        c.start()

    def move(i, carry):
        copy(dxg.at[i], buf.at[i], i).wait()
        copy(buf.at[i], dx.at[i], i).start()
        return carry
    lax.fori_loop(0, n, move, 0)
    for k in BOTH:
        tq[k] = wide[k, :, :nq].T
        to[k] = wide[k, :, nq:].T
    last = [copy(tq, g_qkv), copy(to, g_out)]
    for c in last:
        c.start()

    def done(i, carry):
        copy(buf.at[i], dx.at[i], i).wait()
        return carry
    lax.fori_loop(0, n, done, 0)
    for c in out + last:
        c.wait()


def finish(nq, dxg, ra0, ra1, rm0, rm1):
    rows, d = ra0.shape
    shapes = [dxg.shape, (2, nq, rows), (2, d - nq, rows), (2, rows, d), (2, rows, d)]
    return pl.pallas_call(
        finish_kernel,
        out_shape=[jax.ShapeDtypeStruct(shapes[0], BF16)] + [jax.ShapeDtypeStruct(shape, F32) for shape in shapes[1:]],
        in_specs=[ANY] * 5,
        out_specs=[ANY] * 5,
        scratch_shapes=[pltpu.VMEM(dxg.shape, BF16), pltpu.VMEM((2, rows, d), F32), pltpu.VMEM((2,) + rm0.shape, F32), pltpu.VMEM(shapes[1], F32),
                        pltpu.VMEM(shapes[2], F32), pltpu.SemaphoreType.DMA((32,))],
        compiler_params=pltpu.CompilerParams(vmem_limit_bytes=VMEM_LIMIT),
        name='finish',
    )(dxg, ra0, ra1, rm0, rm1)


def solution(mesh):
    assert dict(mesh.shape) == {'dpy': 2, 'dpx': 2, 'tp': SLOTS}
    act_spec = P(None, DATA_AXES)

    def device_backward(x_saved, y_saved, dz_top, w_qkv, w_out, w_up, w_down):
        layers, d = w_up.shape[:2]
        assert layers == 2
        heads, hd = w_out.shape[1:3]
        n = 3 * heads * hd
        wq = w_qkv.transpose(0, 2, 3, 4, 1).reshape(layers, n, d)
        wo = w_out.reshape(layers, heads * hd, d)
        dy1, gm1, wa1 = mlp_first(1, y_saved, dz_top, w_up, w_down, wq, wo)
        dx1, ga1, w1_0, w2_0, wa0, half = attn_first(1, x_saved, dy1, wa1, gm1, w_up, w_down, wq, wo)
        dy0, gm0, ra1, rm1 = mlp_second(0, y_saved, dx1, w1_0, w2_0, ga1, half)
        d_input, rm0, ra0 = attn_last(0, x_saved, dy0, wa0, gm0)
        d_input, g_qkv, g_out, g_down, g_up = finish(n, d_input, ra0, ra1, rm0, rm1)
        g_qkv = g_qkv.reshape(layers, 3, heads, hd, d // 4).transpose(0, 4, 1, 2, 3)
        return d_input, g_qkv, g_out.reshape(layers, heads, hd, d // 4), g_up, g_down

    tp_last = P(None, None, None, 'tp'), P(None, 'tp'), P(None, None, 'tp'), P(None, 'tp')
    return jax.shard_map(device_backward, mesh=mesh,
                         in_specs=(act_spec, act_spec, P(DATA_AXES)) + tp_last,
                         out_specs=(P(DATA_AXES), P(None, DATA_AXES, None, 'tp'), P(None, 'tp', None, DATA_AXES), P(None, DATA_AXES, 'tp'), P(None, ('tp',) + DATA_AXES)),
                         check_vma=False)
```

```python
import functools
import math
import re

import jax
import jax.numpy as jnp
from jax import lax
from jax.experimental import pallas as pl
from jax.experimental.pallas import tpu as pltpu
from jax.sharding import PartitionSpec as P

DATA_AXES = ('dpy', 'dpx')
F32 = jnp.float32
BF16 = jnp.bfloat16
HEAD = 64
SLOTS = 4
LOOK_AHEAD = 3
PIECES = 8
BOTH = range(2)
NN = (((1,), (0,)), ((), ()))
NT = (((1,), (1,)), ((), ()))
VMEM_LIMIT = 66060288
MESH = pl.DeviceIdType.MESH
ANY = pl.BlockSpec(memory_space=pl.ANY)


def dot(a, b, dims):
    return lax.dot_general(a, b, dims, preferred_element_type=F32)


class Peers:
    def __init__(self):
        z, y, t = lax.axis_index('dpy'), lax.axis_index('dpx'), lax.axis_index('tp')
        self.z, self.y, self.t = z, y, t
        self.sib = (z, y, t + 1 - 2 * (t % 2))
        self.xp = (z, y, (t + 2) % 4)
        self.yp = (z, 1 - y, t)
        self.zp = (1 - z, y, t)

    def arrive(self):
        for peer in (self.sib, self.xp, self.yp, self.zp):
            pl.semaphore_signal(pltpu.get_barrier_semaphore(), inc=1, device_id=peer, device_id_type=MESH)

    def barrier(self):
        with jax.named_scope('entry'):
            pl.semaphore_wait(pltpu.get_barrier_semaphore(), 4)

    def rel(self, d):
        zr = self.z if d // 2 == 0 else 1 - self.z
        yr = self.y if d % 2 == 0 else 1 - self.y
        return zr * 2 + yr


class Sems:
    def __init__(self, send, recv, local):
        self.send, self.recv, self.local = send, recv, local
        self.n = self.m = 0

    def remote(self, src, dst, peer):
        i = self.n
        self.n += 1
        return lambda: pltpu.make_async_remote_copy(src_ref=src(), dst_ref=dst(), send_sem=self.send.at[i], recv_sem=self.recv.at[i],
                                                    device_id=peer, device_id_type=MESH)

    def copy(self, src, dst):
        i = self.m
        self.m += 1
        return lambda: pltpu.make_async_copy(src(), dst(), self.local.at[i])

    def copies(self, n, src, dst):
        first = self.m
        self.m += n
        return lambda i: pltpu.make_async_copy(src(i), dst(i), self.local.at[first + i])


def at_ticks(actions, tick, position=0, points=1):
    for k in sorted(actions):
        if k % points == position:
            @pl.when(tick == k)
            def _(k=k):
                with jax.named_scope('t%d' % k):
                    for action in actions[k]:
                        action()


class Scatter:
    def __init__(self, sems, peers, partial, mine, bufs, out, rows, load=True, half_out=None, part=None):
        r0, r1, r2, r3 = self.bufs = bufs
        self.mine, self.all = mine, pl.ds(*rows)
        first, count = part or rows
        h = count // 2
        self.part, self.lo, self.hi = pl.ds(first, count), pl.ds(first, h), pl.ds(first + h, h)
        self.half = half = pl.ds(first // 2, h)
        every, lo, hi = self.all, self.lo, self.hi
        self.load, self.c0, self.c1, self.c2 = [], [], [], []
        for x in BOTH:
            def near(k, part, x=x):
                return lambda: mine(x).at[k, part]

            def place(buf, *index):
                return lambda: buf.at[index]
            if load:
                self.load.append(sems.copy(lambda x=x: partial(2 * x).at[:, every], near(slice(None), every)))
            self.c0.append(sems.remote(lambda x=x: partial(2 * x + 1).at[:, every], place(r0, x, slice(None), every), peers.sib))
            self.c1.append([sems.remote(near(2 * k + 1, lo), place(r1, 0, x, k, half), peers.yp) for k in BOTH]
                           + [sems.remote(near(2 + k, hi), place(r1, 1, x, k, half), peers.zp) for k in BOTH])
            self.c2.append([sems.remote(near(2, lo), place(r2, 0, x, half), peers.zp), sems.remote(near(1, hi), place(r2, 1, x, half), peers.yp)])
        if half_out is None:
            self.c3 = sems.remote(lambda: mine(1).at[0, self.part], place(r3, self.part), peers.xp)
            self.store = [sems.copy(lambda: mine(0).at[0, every], out)]
        else:
            self.c3 = None
            self.store = [sems.copy(lambda x=x: mine(x).at[0, every], lambda x=x: half_out(x)) for x in BOTH]

    def start(self, x):
        self.c0[x]().start()
        if self.load:
            self.load[x]().start()

    def add0(self, x):
        if self.load:
            self.load[x]().wait()
        self.c0[x]().wait_recv()
        mine, r0 = self.mine(x), self.bufs[0].at[x]

        def body(k, carry):
            mine[k, self.all] = mine[k, self.all] + r0[k, self.all]
            return carry
        lax.fori_loop(0, 4, body, 0)

    def send1(self, x):
        for c in self.c1[x]:
            c().start()

    def add1(self, x):
        for c in self.c1[x]:
            c().wait_recv()
        mine, r1 = self.mine(x), self.bufs[1]

        def body(k, carry):
            mine[2 * k, self.lo] = mine[2 * k, self.lo] + r1[0, x, k, self.half]
            mine[k, self.hi] = mine[k, self.hi] + r1[1, x, k, self.half]
            return carry
        lax.fori_loop(0, 2, body, 0)

    def send2(self, x):
        for c in self.c2[x]:
            c().start()

    def add2(self, x):
        for c in self.c2[x]:
            c().wait_recv()
        mine, r2 = self.mine(x), self.bufs[2]
        mine[0, self.lo] = mine[0, self.lo] + r2[0, x, self.half]
        mine[0, self.hi] = mine[0, self.hi] + r2[1, x, self.half]

    def send3(self):
        self.c3().start()

    def add3(self):
        self.c3().wait_recv()
        mine = self.mine(0)
        mine[0, self.part] = (mine[0, self.part] + self.bufs[3][self.part]) * (1 / SLOTS)

    def out(self):
        for c in self.store:
            c().start()

    def finish(self):
        for c in self.c0 + sum(self.c1, []) + sum(self.c2, []) + ([self.c3] if self.c3 else []):
            c().wait_send()
        for c in self.store:
            c().wait()

    def both(self, name):
        for x in BOTH:
            getattr(self, name)(x)


class Across:
    def __init__(self, sems, peers, mine, bufs, rows, turn):
        self.rx, self.ra, self.rb = bufs
        mine_of, part = mine, pl.ds(*rows)
        self.mine, self.part = mine(0), part
        far, second = 1 + turn, 2 - turn
        self.near = (0, second)
        order = (peers.yp, peers.zp)
        self.go = [[sems.remote(lambda: mine_of(1).at[:, part], lambda: self.rx, peers.xp)],
                   [sems.remote(lambda k=k: self.mine.at[k, part], lambda i=i: self.ra.at[i], order[turn]) for i, k in enumerate((far, 3))],
                   [sems.remote(lambda: self.mine.at[second, part], lambda: self.rb, order[1 - turn])]]

    def send(self, i):
        for c in self.go[i]:
            c().start()

    def add(self, i):
        for c in self.go[i]:
            c().wait_recv()
        mine, part = self.mine, self.part
        if i == 0:
            for k in range(4):
                mine[k, part] = mine[k, part] + self.rx[k]
        elif i == 1:
            for n, k in enumerate(self.near):
                mine[k, part] = mine[k, part] + self.ra[n]
        else:
            mine[0, part] = (mine[0, part] + self.rb[:]) * (1 / SLOTS)

    def both(self, name):
        getattr(self, name[:-1])(int(name[-1]))

    def finish(self):
        for c in sum(self.go, []):
            c().wait_send()


def scatter_bufs(rows, d):
    return [pltpu.VMEM((2, 4, rows, d), F32), pltpu.VMEM((2, 2, 2, rows // 2, d), F32), pltpu.VMEM((2, 2, rows // 2, d), F32), pltpu.VMEM((rows, d), F32)]


def steps(job, plan):
    out = []
    for tick, name, half in re.findall('([0-9]+)([a-z]+[0-3]?)([xy]?)', plan):
        if half:
            action = functools.partial(getattr(job, name), int(half == 'y'))
        else:
            action = functools.partial(job.both, name) if name[-1] in '012' else getattr(job, name)
        out.append((int(tick), action))
    return out


def ticks(plan, actions):
    return list(zip(map(int, plan.split(',')), actions))


class Gather:
    def __init__(self, sems, peers, blocks):
        self.sib = [sems.remote(own, lambda dst=dst: dst(1), peers.sib) for own, dst in blocks]
        self.xp = [sems.remote(own, lambda dst=dst: dst(2), peers.xp) for own, dst in blocks]
        self.fwd = [sems.remote(lambda dst=dst: dst(2), lambda dst=dst: dst(3), peers.sib) for own, dst in blocks]

    def start(self, blocks):
        for i in blocks:
            self.sib[i]().start()
            self.xp[i]().start()

    def forward(self, i):
        self.xp[i]().wait_recv()
        self.fwd[i]().start()

    def forwards(self):
        return [functools.partial(self.forward, i) for i in range(len(self.fwd))]

    def finish(self):
        for i in range(len(self.sib)):
            self.sib[i]().wait_recv()
            self.fwd[i]().wait_recv()
            self.sib[i]().wait_send()
            self.xp[i]().wait_send()
            self.fwd[i]().wait_send()


class Bounce:
    def __init__(self, sems, items, buf):
        self.steps = []
        prev = None
        for own, dst, rows in items:
            ld = sems.copy(own, lambda rows=rows: buf.at[pl.ds(0, rows)])
            st = sems.copy(lambda rows=rows: buf.at[pl.ds(0, rows)], lambda dst=dst: dst(0))
            self.steps.append(functools.partial(self.load, prev, ld))
            self.steps.append(functools.partial(self.flip, ld, st))
            prev = st
        self.steps.append(lambda prev=prev: prev().wait())

    @staticmethod
    def load(prev, ld):
        if prev is not None:
            prev().wait()
        ld().start()

    @staticmethod
    def flip(ld, st):
        ld().wait()
        st().start()


def merge(*lists):
    actions = {}
    for pairs in lists:
        for k, action in pairs:
            actions.setdefault(k, []).append(action)
    return actions


SEMS = [pltpu.SemaphoreType.DMA((96,)), pltpu.SemaphoreType.DMA((96,)), pltpu.SemaphoreType.DMA((32,))]


def leading(*shape):
    return pl.BlockSpec((1,) + shape, lambda j, *_: (j,) + (0,) * len(shape))


def params(collective_id, axes):
    return pltpu.CompilerParams(vmem_limit_bytes=VMEM_LIMIT, dimension_semantics=('arbitrary',) * axes, collective_id=collective_id, has_side_effects=True)


def mlp_slot(slot, seqs, seq, w1, w2, w1t, yt, dz, acc, gt, dht, tick, arrive, emit):
    w1t[:] = w1[:].T

    def block(i, carry):
        tick(i)
        with jax.named_scope('arrive'):
            pl.when(slot == 0)(lambda: arrive(i))
        cols = pl.ds(pl.multiple_of(i * seq, seq), seq)
        h = dot(w1t[:], yt[:, cols], NN)
        dg = dot(w2[:], dz[:, cols], NN)
        c0 = math.sqrt(2 / math.pi)
        c1 = 0.044715 * c0
        h2 = h * h
        t = jnp.tanh(h * (c0 + c1 * h2))
        q = 0.5 * t + 0.5
        g = h * q
        dh = dg * (q + (g * (1.0 - t)) * (c0 + (3 * c1) * h2))
        gt[:, cols] = g.astype(BF16)
        dh = dh.astype(BF16)
        dht[:, cols] = dh
        acc[:, cols] += dot(w1[:], dh, NN)
        with jax.named_scope('memit'):
            pl.when(slot == SLOTS - 1)(lambda: emit(i))
        return carry
    lax.fori_loop(0, seqs, block, 0)


def tokens(i, seq):
    return pl.ds(pl.multiple_of(i * seq, seq), seq)


class MlpIo:
    def __init__(self, sems, peers, seqs, seq, loads, acc, dz, dyb, dy_hbm, gbuf, g_hbm):
        self.seqs, self.seq, self.peers = seqs, seq, peers
        self.loads, self.acc, self.dz, self.dyb, self.gbuf = loads, acc, dz, dyb, gbuf
        self.dy = sems.copies(seqs, lambda i: dyb.at[:, tokens(i, seq)], lambda i: dy_hbm.at[:, tokens(i, seq)])
        self.g = [sems.copy(lambda j=j: gbuf.at[j], lambda j=j: g_hbm.at[pl.program_id(0), j]) for j in BOTH]

    def start(self):
        for load, _ in self.loads:
            for i in range(self.seqs):
                load(i).start()

    def arrive(self, i):
        for load, use in self.loads:
            load(i).wait()
            use(i)
        cols = tokens(i, self.seq)
        self.acc[:, cols] = jnp.zeros((self.acc.shape[0], self.seq), F32)

    def emit(self, i):
        cols = tokens(i, self.seq)
        self.dyb[:, cols] = (self.dz[:, cols].astype(F32) + self.acc[:, cols]).astype(BF16)
        self.dy(i).start()

    def grads(self, j, a, b):
        pl.when(pl.program_id(0) > 0)(lambda: self.g[j]().wait())
        rows, width = self.gbuf.shape[-2:]
        split, half = width * 2 // 3, width // 2
        for lo, hi, c0, c1 in ((0, width, 0, split), (0, half, split, width), (half, width, split, width)):
            g = dot(a[lo:hi], b[c0:c1], NT)
            for k in range(g.shape[0] // rows):
                self.gbuf[j, self.peers.rel(lo // rows + k), :, c0:c1] = g[k * rows:(k + 1) * rows]
        self.g[j]().start()

    def finish(self):
        for i in range(self.seqs):
            self.dy(i).wait()
        for c in self.g:
            c().wait()


def mlp_rest(slot, actions, io, w1, w2, w1t, yt, gt, dht):
    seqs, seq, dz, acc = io.seqs, io.seq, io.dz, io.acc
    points = seqs + 2
    first = slot * points

    def tick(i):
        at_ticks({k: v for k, v in actions.items() if k % points < seqs}, first + i)
    mlp_slot(slot, seqs, seq, w1, w2, w1t, yt, dz, acc, gt, dht, tick, io.arrive, io.emit)
    at_ticks(actions, first + seqs, seqs, points)
    with jax.named_scope('dw2'):
        io.grads(0, gt, dz)
    at_ticks(actions, first + seqs + 1, seqs + 1, points)
    with jax.named_scope('dw1'):
        io.grads(1, yt, dht)


def attn_weights(layer, wq, wo, wa_g):
    nq, d = wq.shape[1:]
    return [(lambda: wq.at[layer], lambda j: wa_g.at[j, pl.ds(0, nq)], nq), (lambda: wo.at[layer], lambda j: wa_g.at[j, pl.ds(nq, d - nq)], d - nq)]


class Spread:
    def __init__(self, sems, peers, wb, pieces):
        rows = wb.shape[2] // pieces
        y = peers.y

        def piece(slot, m, k):
            return lambda: wb.at[slot, m, pl.ds(k * rows, rows)]
        every = range(pieces)
        self.sib = sems.remote(lambda: wb.at[0], lambda: wb.at[1], peers.sib)
        self.xp = [sems.remote(piece(0, y, k), piece(2, y, k), peers.xp) for k in every]
        self.fy, self.wy = [], []
        for k in every:
            self.fy.append(sems.remote(piece(2, y, k), piece(2, y, k), peers.yp))
            sems.n -= 1
            self.wy.append(sems.remote(piece(2, 1 - y, k), piece(2, 1 - y, k), peers.yp))
        self.fs = [sems.remote(piece(2, y, k), piece(3, y, k), peers.sib) for k in every]
        self.fs2 = [sems.remote(piece(2, 1 - y, k), piece(3, 1 - y, k), peers.sib) for k in every]

    def start(self):
        for c in self.xp + [self.sib]:
            c().start()

    def forward(self, k):
        self.xp[k]().wait_recv()
        self.fy[k]().start()
        self.fs[k]().start()

    def forward2(self, k):
        self.wy[k]().wait_recv()
        self.fs2[k]().start()

    def arrived(self):
        for c in self.fs + self.fs2:
            c().wait_recv()

    def finish(self):
        for c in [self.sib] + self.xp + self.fy + self.fs + self.fs2:
            c().wait_send()


def turned(src, dst, seq):
    def use(i):
        dst[:, tokens(i, seq)] = src[i].T
    return use


def mlp_first_kernel(layer, y, dz_in, wup, wdn, wq, wo, dy_hbm, g_hbm, wa_g, yb, dzb, yt, dzt, acc, w1t, gt, dht, wb, bounce, dyb, gbuf, *rest):
    slot = pl.program_id(0)
    seqs, seq = yb.shape[:2]
    peers, sems = Peers(), Sems(*rest)
    mine = peers.t * seqs
    loads = [(sems.copies(seqs, lambda i: y.at[layer, mine + i], lambda i: yb.at[i]), turned(yb, yt, seq)),
             (sems.copies(seqs, lambda i: dz_in.at[mine + i], lambda i: dzb.at[i]), turned(dzb, dzt, seq))]
    io = MlpIo(sems, peers, seqs, seq, loads, acc, dzt, dyb, dy_hbm, gbuf, g_hbm)
    own = [sems.copy(lambda w=w: w.at[layer], lambda m=m: wb.at[0, m]) for m, w in enumerate((wup, wdn))]
    blocks = attn_weights(layer, wq, wo, wa_g)
    gather = Gather(sems, peers, [r[:2] for r in blocks])
    hop = Bounce(sems, blocks, bounce)
    spread = Spread(sems, peers, wb, PIECES)

    @pl.when(slot == 0)
    def _():
        with jax.named_scope('e56'):
            for c in own:
                c().start()
        with jax.named_scope('e57'):
            io.start()
        with jax.named_scope('e58'):
            peers.arrive()
        with jax.named_scope('e59'):
            peers.barrier()
        with jax.named_scope('e60'):
            for c in own:
                c().wait()
        with jax.named_scope('e61'):
            spread.start()
        with jax.named_scope('e62'):
            gather.start(BOTH)

    @pl.when(slot == 1)
    def _():
        with jax.named_scope('e55'):
            spread.sib().wait_recv()

    @pl.when(slot == 2)
    def _():
        with jax.named_scope('e54'):
            for k in range(5, PIECES):
                spread.forward2(k)

    @pl.when(slot == 3)
    def _():
        with jax.named_scope('e53'):
            spread.arrived()
    every = range(PIECES)
    actions = merge([(14 + k, s) for k, s in enumerate(hop.steps)], ticks('2,3,4,5,7,8,9,10', [functools.partial(spread.forward, k) for k in every]),
                    ticks('7,8,9,10,11', [functools.partial(spread.forward2, k) for k in every]), ticks('21', gather.forwards()))
    mlp_rest(slot, actions, io, wb.at[slot, 0], wb.at[slot, 1], w1t, yt, gt, dht)

    @pl.when(slot == SLOTS - 1)
    def _():
        with jax.named_scope('e49'):
            gather.forward(1)
        with jax.named_scope('e50'):
            io.finish()
        with jax.named_scope('e51'):
            spread.finish()
        with jax.named_scope('e52'):
            gather.finish()


def mlp_first(layer, y, dz, wup, wdn, wq, wo):
    d, f = wup.shape[1:]
    seq = y.shape[2]
    seqs = y.shape[1] // SLOTS
    tok = seqs * seq
    return pl.pallas_call(
        functools.partial(mlp_first_kernel, layer),
        out_shape=(jax.ShapeDtypeStruct((d, tok), BF16), jax.ShapeDtypeStruct((SLOTS, 2, 4, d // 4, f), F32), jax.ShapeDtypeStruct((SLOTS, d, d), BF16)),
        grid=(SLOTS,),
        in_specs=[ANY] * 6,
        out_specs=[ANY] * 3,
        scratch_shapes=[pltpu.VMEM((seqs, seq, d), BF16)] * 2 + [pltpu.VMEM((d, tok), BF16)] * 2
        + [pltpu.VMEM((d, tok), F32), pltpu.VMEM((f, d), BF16), pltpu.VMEM((f, tok), BF16), pltpu.VMEM((f, tok), BF16), pltpu.VMEM((SLOTS, 2, d, f), BF16),
           pltpu.VMEM((d, d), BF16), pltpu.VMEM((d, tok), BF16), pltpu.VMEM((2, 4, d // 4, f), F32)] + SEMS,
        compiler_params=params(0, 1),
        name='mlp_first',
    )(y, dz, wup, wdn, wq, wo)


def mlp_second_kernel(layer, w1_ref, w2_ref, y, dz_in, partial, half, dy_hbm, g_hbm, red, red_half, yb, yt, dzt, acc, w1t, gt, dht, dyb, gbuf, mine, *rest):
    slot = pl.program_id(0)
    seqs, seq = yb.shape[:2]
    bufs, rest = rest[:4], rest[4:]
    peers, sems = Peers(), Sems(*rest[2:])
    place = peers.t * seqs
    loads = [(sems.copies(seqs, lambda i: y.at[layer, place + i], lambda i: yb.at[i]), turned(yb, yt, seq)),
             (sems.copies(seqs, lambda i: dz_in.at[:, tokens(i, seq)], lambda i: dzt.at[:, tokens(i, seq)]), lambda i: None)]
    io = MlpIo(sems, peers, seqs, seq, loads, acc, dzt, dyb, dy_hbm, gbuf, g_hbm)
    rows = mine.shape[2] // 2
    a, b = jobs = [Scatter(sems, peers, lambda s: partial.at[s], lambda x: mine.at[x], bufs, lambda j=j: red.at[pl.ds(j * rows, rows)], (j * rows, rows)) for j in BOTH]

    h0, h1 = rest[:2]
    mine_half = sems.copy(lambda: half.at[0], lambda: h0)
    x_half = sems.remote(lambda: half.at[1], lambda: h1, peers.xp)
    store_half = sems.copy(lambda: h0, lambda: red_half)

    def add_half():
        mine_half().wait()
        x_half().wait_recv()
        h0[:] = (h0[:] + h1[:]) * (1 / SLOTS)

    @pl.when(slot == 0)
    def _():
        with jax.named_scope('e43'):
            io.start()
        with jax.named_scope('e44'):
            peers.arrive()
        with jax.named_scope('e45'):
            peers.barrier()
        with jax.named_scope('e46'):
            for job in jobs:
                job.both('start')
        with jax.named_scope('e47'):
            x_half().start()
        with jax.named_scope('e48'):
            mine_half().start()
    actions = merge(ticks('17,18', [add_half, lambda: store_half().start()]),
                    steps(a, '3add0,3send1,9add1,9send2,17add2,17send3,21add3,22out'),
                    steps(b, '4add0,4send1,14add1,14send2,19add2,19send3,23add3'))
    mlp_rest(slot, actions, io, w1_ref.at[0], w2_ref.at[0], w1t, yt, gt, dht)

    @pl.when(slot == SLOTS - 1)
    def _():
        with jax.named_scope('e37'):
            b.out()
        with jax.named_scope('e38'):
            io.finish()
        with jax.named_scope('e39'):
            x_half().wait_send()
        with jax.named_scope('e40'):
            store_half().wait()
        with jax.named_scope('e41'):
            a.finish()
        with jax.named_scope('e42'):
            b.finish()


def mlp_second(layer, y, dz, w1, w2, partial, half):
    d, f = w1.shape[1:]
    seq = y.shape[2]
    seqs = y.shape[1] // SLOTS
    tok = seqs * seq
    return pl.pallas_call(
        functools.partial(mlp_second_kernel, layer),
        out_shape=(jax.ShapeDtypeStruct((d, tok), BF16), jax.ShapeDtypeStruct((SLOTS, 2, 4, d // 4, f), F32),
                   jax.ShapeDtypeStruct((d // 4, d), F32), jax.ShapeDtypeStruct(half.shape[1:], F32)),
        grid=(SLOTS,),
        in_specs=[leading(d, f), leading(f, d)] + [ANY] * 4,
        out_specs=[ANY] * 4,
        scratch_shapes=[pltpu.VMEM((seqs, seq, d), BF16), pltpu.VMEM((d, tok), BF16), pltpu.VMEM((d, tok), BF16), pltpu.VMEM((d, tok), F32), pltpu.VMEM((f, d), BF16),
                        pltpu.VMEM((f, tok), BF16), pltpu.VMEM((f, tok), BF16), pltpu.VMEM((d, tok), BF16),
                        pltpu.VMEM((2, 4, d // 4, f), F32), pltpu.VMEM((2, 4, d // 4, d), F32)]
        + scatter_bufs(d // 4, d) + [pltpu.VMEM(half.shape[1:], F32)] * 2 + SEMS,
        compiler_params=params(1, 1),
        name='mlp_second',
    )(w1, w2, y, dz, partial, half)


def attn_step(sems, peers, x_ref, dy_hbm, w_hbm, dy_ref, w_ref, xt, acc, gacc, qkv, do, b1, b2, begin, act, emit, ending=lambda: None):
    s, slot = pl.program_id(0), pl.program_id(1)
    step = s * SLOTS + slot
    last = SLOTS * SLOTS - 1
    before = jnp.maximum(step - 1, 0)
    seq, d = x_ref.shape[-2:]
    nqkv = qkv.shape[0]
    third = nqkv // 3
    split = d - b2.shape[1]
    rows = d // 4

    load_w = sems.copies(SLOTS, lambda i: w_hbm.at[i], lambda i: w_ref.at[i])
    load_dy = sems.copies(SLOTS, lambda i: dy_hbm.at[:, tokens(i, seq)], lambda i: dy_ref.at[:, tokens(i, seq)])

    @pl.when(step == 0)
    def _():
        for i in range(SLOTS):
            load_w(i).start()
            load_dy(i).start()
        peers.arrive()
        def clear(j, carry):
            gacc[j // 4, j % 4] = jnp.zeros(gacc.shape[2:], F32)
            b1[j % 2] = jnp.zeros(b1.shape[1:], BF16)
            b2[j % 2] = jnp.zeros(b2.shape[1:], BF16)
            return carry
        lax.fori_loop(0, SLOTS * 4, clear, 0)
        begin()
    act()
    with jax.named_scope('loadw'):
        pl.when(s == 0)(lambda: load_w(slot).wait())

    @pl.when(slot == 0)
    def _():
        with jax.named_scope('e35'):
            load_dy(s).wait()
        with jax.named_scope('e36'):
            xt[s % 2] = x_ref[0, 0].T

    def grads(n, par):
        ps, pj = n // SLOTS, n % SLOTS
        third_d = d // 3

        def weights(c):
            cols = slice(c * third_d, (c + 1) * third_d)
            g = dot(xt[ps % 2], b1[par, cols], NT)
            if c == 2:
                g = g + dot(dy_ref[:, tokens(ps, seq)], b2[par], NT)
            for k in range(4):
                r = peers.rel(k)
                gacc[pj, r, :, cols] = gacc[pj, r, :, cols] + g[k * rows:(k + 1) * rows]

        def inputs(c):
            part = slice(c * third_d, (c + 1) * third_d)
            acc[part] += dot(w_ref[pj, :, part].T, b1[par], NN)
        return [functools.partial(f, c) for c in range(3) for f in (weights, inputs)]
    with jax.named_scope("main"):
        x_t = xt[s % 2]
        dy_t = dy_ref[:, tokens(s, seq)]
        now = step % 2
        qkv[:] = dot(w_ref[slot, pl.ds(0, nqkv), :], x_t, NN).astype(BF16)
        do[:] = dot(w_ref[slot, pl.ds(nqkv, d - nqkv), :], dy_t, NN).astype(BF16)
        scale = HEAD ** -0.5
        exp_scale = scale * math.log2(math.e)
        qb = seq // 2
        units = [(h, slice(c * qb, (c + 1) * qb)) for h in range(third // HEAD) for c in BOTH]

        def scores(h, qc):
            q_rows, k_rows, v_rows = head_rows(h)
            return dot(qkv[k_rows, :].T, qkv[q_rows, qc], NN), dot(qkv[v_rows, :].T, do[q_rows, qc] * scale, NN)

        def head_rows(h):
            return [slice(i * third + h * HEAD, i * third + (h + 1) * HEAD) for i in range(3)]
        for piece in grads(before, 1 - step % 2):
            piece()
        ahead = [scores(*unit) for unit in units[:LOOK_AHEAD]]
        for n, (h, qc) in enumerate(units):
            sc, dp_t = ahead.pop(0)
            if n + LOOK_AHEAD < len(units):
                ahead.append(scores(*units[n + LOOK_AHEAD]))
            q_rows, k_rows, v_rows = head_rows(h)
            m = jnp.max(sc, axis=0, keepdims=True)
            e = jnp.exp2((sc - m) * exp_scale)
            inv = 1.0 / jnp.sum(e, axis=0, keepdims=True)
            rd = jnp.sum(e * dp_t, axis=0, keepdims=True) * inv
            p = e * inv
            p_bf = p.astype(BF16)
            ds = (p * (dp_t - rd)).astype(BF16)
            b2[now, pl.ds(b2.shape[1] - third + h * HEAD, HEAD), qc] = dot(qkv[v_rows, :], p_bf, NN).astype(BF16)
            b1[now, q_rows, qc] = dot(qkv[k_rows, :], ds, NN).astype(BF16)
            dv_c = dot(do[q_rows, qc], p_bf, NT)
            dk_c = dot(qkv[q_rows, qc], ds, NT)
            if n % 2 == 0:
                dv, dk = dv_c, dk_c
            else:
                b1[now, k_rows] = (dk + dk_c).astype(BF16)
                b1[now, v_rows] = (dv + dv_c).astype(BF16)

    @pl.when(slot == 0)
    def _():
        @pl.when(s > 0)
        def _():
            emit(s - 1)
        acc[:] = dy_ref[:, tokens(s, seq)].astype(F32)

    @pl.when(step == last)
    def _():
        with jax.named_scope('e32'):
            ending()
        with jax.named_scope('e33'):
            for piece in grads(last, last % 2):
                piece()
        with jax.named_scope('e34'):
            emit(s)


ATTN_IN = 3
ATTN_SCRATCH = 9
JOB_PLAN = '1add0x,1send1x,2add0y,2send1y,7add1,7send2,12add2', '3add0,3send1x,7send1y,9add1x,9send2x,14add1y,14send2y'


def attn_first_kernel(layer, x_ref, dy_hbm, w_hbm, partial, wup, wdn, wq, wo, dx_hbm, g_hbm, w1_g, w2_g, wa_g, half, *rest):
    body, rest = rest[:ATTN_SCRATCH], rest[ATTN_SCRATCH:]
    acc, gacc, mine, bounce = body[3], body[4], rest[:2], rest[-4]
    seq = x_ref.shape[-2]
    step = pl.program_id(0) * SLOTS + pl.program_id(1)
    peers, sems = Peers(), Sems(*rest[-3:])
    a, b = jobs = [Scatter(sems, peers, lambda s, j=j: partial.at[s, j], lambda x, j=j: mine[j].at[x], rest[2 + 4 * j:6 + 4 * j], None,
                           (0, half.shape[2]), half_out=lambda x, j=j: half.at[x, j]) for j in BOTH]
    blocks = [(lambda w=w: w.at[layer - 1], lambda j, g=g: g.at[j], wup.shape[1]) for w, g in ((wup, w1_g), (wdn, w2_g))] + attn_weights(layer - 1, wq, wo, wa_g)
    gather = Gather(sems, peers, [r[:2] for r in blocks])
    hop = Bounce(sems, blocks, bounce)
    stores = [sems.copy(lambda j=j: gacc.at[j], lambda j=j: g_hbm.at[j]) for j in range(SLOTS)]
    actions = merge(steps(a, JOB_PLAN[0]), steps(b, JOB_PLAN[1]), [(5 + k, s) for k, s in enumerate(hop.steps)],
                    ticks('6,11,15,15', gather.forwards()), ticks('14,15,13', [lambda c=c: c().start() for c in stores[:2]] + [a.out]))

    dxb = rest[-5]
    store_dx = sems.copies(SLOTS, lambda i: dxb.at[i], lambda i: dx_hbm.at[:, tokens(i, seq)])

    def begin():
        peers.barrier()
        for job in jobs:
            job.both('start')
        gather.start(range(len(blocks)))

    def emit(s):
        dxb[s] = acc[:].astype(BF16)
        store_dx(s).start()
    attn_step(sems, peers, x_ref, dy_hbm, w_hbm, *body, begin, lambda: at_ticks(actions, step), emit, lambda: stores[2]().start())

    @pl.when(step == SLOTS * SLOTS - 1)
    def _():
        with jax.named_scope('e25'):
            stores[3]().start()
        with jax.named_scope('e26'):
            b.both('add2')
        with jax.named_scope('e27'):
            gather.finish()
        with jax.named_scope('e28'):
            b.out()
        with jax.named_scope('e29'):
            for c in stores:
                c().wait()
        with jax.named_scope('e30'):
            for i in range(SLOTS):
                store_dx(i).wait()
        with jax.named_scope('e31'):
            for job in jobs:
                job.finish()


def attn_last_kernel(x_ref, dy_hbm, w_hbm, partial, dxg, red, red_last, *rest):
    body, rest = rest[:ATTN_SCRATCH], rest[ATTN_SCRATCH:]
    acc, gacc, mine, dxb, free = body[3], body[4], rest[:2], rest[-5], rest[-4]
    step = pl.program_id(0) * SLOTS + pl.program_id(1)
    seqs = pl.num_programs(0)
    peers, sems = Peers(), Sems(*rest[-3:])
    nred = red.shape[1]
    a, b = jobs = [Scatter(sems, peers, lambda s, j=j: partial.at[s, j], lambda x, j=j: mine[j].at[x], rest[2 + 4 * j:6 + 4 * j], lambda j=j: red.at[j],
                           (0, nred), part=(0, nred * 3 // 4)) for j in BOTH]
    rows = nred * 3 // 4, nred // 4
    across = [Across(sems, peers, lambda x, j=j: mine[j].at[x], [r.at[j] for r in rest[-8:-5]], rows, j) for j in BOTH]
    h = nred // 2
    ends = [Scatter(sems, peers, lambda s: gacc.at[s], lambda x: gacc.at[2 * x], rest[2:6], lambda j=j: red_last.at[pl.ds(j * h, h)], (j * h, h), load=False)
            for j in BOTH]
    t = peers.t
    t2 = (t + 2) % SLOTS
    sib, xp, fwd, mine_dx = [], [], [], []
    for s in range(SLOTS):
        def src(s=s):
            return dxb.at[s]

        def dst(s=s):
            return dxg.at[t * SLOTS + s]

        def other(s=s):
            return dxg.at[t2 * SLOTS + s]
        mine_dx.append(sems.copy(src, dst))
        sib.append(sems.remote(src, dst, peers.sib))
        xp.append(sems.remote(src, dst, peers.xp))
        fwd.append(sems.remote(other, other, peers.sib))

    def freed(i):
        for peer in ([peers.sib], [peers.yp, peers.zp], [peers.yp, peers.zp], [peers.xp])[i]:
            pl.semaphore_signal(free.at[i], inc=1, device_id=peer, device_id_type=MESH)

    def forward(s):
        xp[s]().wait_recv()
        fwd[s]().start()

    def early():
        pl.semaphore_wait(free.at[0], 1)
        for job in ends:
            job.start(0)

    def early_add():
        pl.semaphore_wait(free.at[1], 2)
        for job in ends:
            job.add0(0)
        for job in ends:
            job.send1(0)
    actions = merge(steps(a, '1add0y,1send1y,3add0x,4add1y,4send2y'), steps(b, '2add0y,2send1y,3add0x,6add1y,6send2y'),
                    steps(a, '7add2y,7send3,10add1x,10send2x'), steps(b, '10add2y,10send3,12add1x,12send2x'),
                    steps(across[0], '1send0,4add0,4send1,8add1,8send2,13add2'), steps(across[1], '2send0,7add0,7send1,13add1,13send2,15add2'),
                    steps(a, '4send1x'), steps(b, '6send1x'),
                    ticks('4,11,10,15,15', [functools.partial(freed, i) for i in BOTH] + [functools.partial(forward, i) for i in BOTH] + [early]))

    def begin():
        peers.barrier()
        for x in (1, 0):
            for job in jobs:
                job.start(x)

    def emit(s):
        dxb[s] = acc[:].T.astype(BF16)
        for k in range(SLOTS):
            @pl.when(s == k)
            def _(k=k):
                for c in (xp, sib, mine_dx):
                    c[k]().start()
    attn_step(sems, peers, x_ref, dy_hbm, w_hbm, *body, begin, lambda: at_ticks(actions, step), emit, early_add)

    @pl.when(step == SLOTS * SLOTS - 1)
    def _():
        with jax.named_scope('e1'):
            for job in ends:
                job.start(1)
        with jax.named_scope('e2'):
            a.add2(0)
        with jax.named_scope('e3'):
            freed(2)
        with jax.named_scope('e4'):
            a.add3()
        with jax.named_scope('e5'):
            freed(3)
        with jax.named_scope('e6'):
            for job in ends:
                job.add0(1)
        with jax.named_scope('e7'):
            a.out()
        with jax.named_scope('e8'):
            b.add2(0)
        with jax.named_scope('e9'):
            for job in ends:
                job.send1(1)
        with jax.named_scope('e10'):
            b.add3()
        with jax.named_scope('e11'):
            b.out()
        with jax.named_scope('e12'):
            pl.semaphore_wait(free.at[2], 2)
        with jax.named_scope('e13'):
            pl.semaphore_wait(free.at[3], 1)
        with jax.named_scope('e14'):
            for job in ends:
                job.add1(0)
        with jax.named_scope('e15'):
            forward(2)
        with jax.named_scope('e16'):
            for job in ends:
                job.add1(1)
                job.send2(1)
        with jax.named_scope('e17'):
            for job in ends:
                job.send2(0)
        with jax.named_scope('e18'):
            for job in ends:
                job.add2(1)
                job.send3()
        with jax.named_scope('e19'):
            for job in ends:
                job.add2(0)
        with jax.named_scope('e20'):
            forward(3)
        with jax.named_scope('e21'):
            for s in range(SLOTS):
                mine_dx[s]().wait()
                sib[s]().wait()
                xp[s]().wait_send()
        with jax.named_scope('e22'):
            for job in ends:
                job.add3()
                job.out()
        with jax.named_scope('e23'):
            for s in range(SLOTS):
                fwd[s]().wait()
        with jax.named_scope('e24'):
            for job in jobs + ends + across:
                job.finish()


def attn_specs(layer, x, w):
    slots, nw, d = w.shape
    seq = x.shape[2]
    seqs = x.shape[1] // slots
    tok = seqs * seq
    nqkv = nw * 3 // 4
    in_specs = [pl.BlockSpec((1, 1, seq, d), lambda s, j: (layer, lax.axis_index('tp') * seqs + s, 0, 0))] + [ANY] * 3
    scratch = [pltpu.VMEM((d, tok), BF16), pltpu.VMEM((slots, nw, d), BF16), pltpu.VMEM((2, d, seq), BF16), pltpu.VMEM((d, seq), F32), pltpu.VMEM((slots, 4, d // 4, nw), F32), pltpu.VMEM((nqkv, seq), BF16),
               pltpu.VMEM((nw - nqkv, seq), BF16), pltpu.VMEM((2, nw, seq), BF16), pltpu.VMEM((2, d // 3, seq), BF16)]
    scratch += [pltpu.VMEM((2, 4, d // 4, d), F32)] * 2 + scatter_bufs(d // 4, d) * 2
    red = jax.ShapeDtypeStruct((2, d // 4, d), F32)
    return (slots, seqs), in_specs, scratch, red, tok


def attn_first(layer, x, dy, w, partial, *weights):
    grid, in_specs, scratch, red, tok = attn_specs(layer, x, w)
    slots, nw, d = w.shape
    gathered = [jax.ShapeDtypeStruct((slots, d, d), BF16)] * 3
    return pl.pallas_call(
        functools.partial(attn_first_kernel, layer),
        out_shape=[jax.ShapeDtypeStruct((d, tok), BF16), jax.ShapeDtypeStruct((slots, 4, d // 4, nw), F32)] + gathered + [jax.ShapeDtypeStruct((2,) + red.shape, F32)],
        grid=grid,
        in_specs=in_specs + [ANY] * len(weights),
        out_specs=[ANY] * 6,
        scratch_shapes=scratch + [pltpu.VMEM((slots, d, tok // slots), BF16), pltpu.VMEM((d, d), BF16)] + SEMS,
        compiler_params=params(2, 2),
        name='attn_first',
    )(x, dy, w, partial, *weights)


def attn_last(layer, x, dy, w, partial):
    grid, in_specs, scratch, red, tok = attn_specs(layer, x, w)
    slots, nw, d = w.shape
    seq = x.shape[2]
    return pl.pallas_call(
        attn_last_kernel,
        out_shape=[jax.ShapeDtypeStruct((x.shape[1], seq, d), BF16), red, jax.ShapeDtypeStruct(red.shape[1:], F32)],
        grid=grid,
        in_specs=in_specs,
        out_specs=[ANY] * 3,
        scratch_shapes=scratch + [pltpu.VMEM((2, n, d // 16, d), F32) for n in (4, 2)] + [pltpu.VMEM((2, d // 16, d), F32), pltpu.VMEM((slots, seq, d), BF16),
                                                                                         pltpu.SemaphoreType.REGULAR((4,))] + SEMS,
        compiler_params=params(3, 2),
        name='attn_last',
    )(x, dy, w, partial)


def finish_kernel(dxg, ra0, ra1, rm0, rm1, dx, g_qkv, g_out, g_down, g_up, buf, wide, mlp, tq, to, sems):
    n = dxg.shape[0]
    nq = tq.shape[1]
    count = [n]

    def copy(src, dst, i=None):
        if i is None:
            i = count[0]
            count[0] += 1
        return pltpu.make_async_copy(src, dst, sems.at[i])
    small = [copy(ra0, wide.at[0]), copy(ra1, wide.at[1]), copy(rm0, mlp.at[0]), copy(rm1, mlp.at[1])]
    first = count[0]
    for c in small:
        c.start()

    def load(i, carry):
        copy(dxg.at[i], buf.at[i], i).start()
        return carry
    lax.fori_loop(0, n, load, 0)
    for c in small:
        c.wait()
    out = [copy(mlp.at[k, j], g.at[k]) for j, g in enumerate((g_down, g_up)) for k in BOTH]
    for c in out:
        c.start()

    def move(i, carry):
        copy(dxg.at[i], buf.at[i], i).wait()
        copy(buf.at[i], dx.at[i], i).start()
        return carry
    lax.fori_loop(0, n, move, 0)
    for k in BOTH:
        tq[k] = wide[k, :, :nq].T
        to[k] = wide[k, :, nq:].T
    last = [copy(tq, g_qkv), copy(to, g_out)]
    for c in last:
        c.start()

    def done(i, carry):
        copy(buf.at[i], dx.at[i], i).wait()
        return carry
    lax.fori_loop(0, n, done, 0)
    for c in out + last:
        c.wait()


def finish(nq, dxg, ra0, ra1, rm0, rm1):
    rows, d = ra0.shape
    shapes = [dxg.shape, (2, nq, rows), (2, d - nq, rows), (2, rows, d), (2, rows, d)]
    return pl.pallas_call(
        finish_kernel,
        out_shape=[jax.ShapeDtypeStruct(shapes[0], BF16)] + [jax.ShapeDtypeStruct(shape, F32) for shape in shapes[1:]],
        in_specs=[ANY] * 5,
        out_specs=[ANY] * 5,
        scratch_shapes=[pltpu.VMEM(dxg.shape, BF16), pltpu.VMEM((2, rows, d), F32), pltpu.VMEM((2,) + rm0.shape, F32), pltpu.VMEM(shapes[1], F32),
                        pltpu.VMEM(shapes[2], F32), pltpu.SemaphoreType.DMA((32,))],
        compiler_params=pltpu.CompilerParams(vmem_limit_bytes=VMEM_LIMIT),
        name='finish',
    )(dxg, ra0, ra1, rm0, rm1)


def solution(mesh):
    assert dict(mesh.shape) == {'dpy': 2, 'dpx': 2, 'tp': SLOTS}
    act_spec = P(None, DATA_AXES)

    def device_backward(x_saved, y_saved, dz_top, w_qkv, w_out, w_up, w_down):
        layers, d = w_up.shape[:2]
        assert layers == 2
        heads, hd = w_out.shape[1:3]
        n = 3 * heads * hd
        wq = w_qkv.transpose(0, 2, 3, 4, 1).reshape(layers, n, d)
        wo = w_out.reshape(layers, heads * hd, d)
        dy1, gm1, wa1 = mlp_first(1, y_saved, dz_top, w_up, w_down, wq, wo)
        dx1, ga1, w1_0, w2_0, wa0, half = attn_first(1, x_saved, dy1, wa1, gm1, w_up, w_down, wq, wo)
        dy0, gm0, ra1, rm1 = mlp_second(0, y_saved, dx1, w1_0, w2_0, ga1, half)
        d_input, rm0, ra0 = attn_last(0, x_saved, dy0, wa0, gm0)
        d_input, g_qkv, g_out, g_down, g_up = finish(n, d_input, ra0, ra1, rm0, rm1)
        g_qkv = g_qkv.reshape(layers, 3, heads, hd, d // 4).transpose(0, 4, 1, 2, 3)
        return d_input, g_qkv, g_out.reshape(layers, heads, hd, d // 4), g_up, g_down

    tp_last = P(None, None, None, 'tp'), P(None, 'tp'), P(None, None, 'tp'), P(None, 'tp')
    return jax.shard_map(device_backward, mesh=mesh,
                         in_specs=(act_spec, act_spec, P(DATA_AXES)) + tp_last,
                         out_specs=(P(DATA_AXES), P(None, DATA_AXES, None, 'tp'), P(None, 'tp', None, DATA_AXES), P(None, DATA_AXES, 'tp'), P(None, ('tp',) + DATA_AXES)),
                         check_vma=False)
```
